256 devices in a mesh: rep: 1, r: 32 (over y, z), s: 8 (over x, core).
Axes of the slice: x: 4, y: 4, z: 8, core: 2. Of those that a mesh axis runs over, the one named last changes fastest.
Arguments:
- x: bfloat16 [256, 2048, 896], P(('rep', 'r', 's'))
- dy: bfloat16 [256, 2048, 896], P(('rep', 'r', 's'))
- w_gate: bfloat16 [2, 896, 2560], P(None, 's')
- w_up: bfloat16 [2, 896, 2560], P(None, 's')
- w_down: bfloat16 [2, 2560, 896], P(None, 's')
Outputs:
- output 1: bfloat16 [256, 2048, 896], P(('rep', 'r', 's'))
- output 2: bfloat16 [2, 896, 2560], P('rep', 's')
- output 3: bfloat16 [2, 896, 2560], P('rep', 's')
- output 4: bfloat16 [2, 2560, 896], P('rep', 's')
All inputs are finite; a program needn't handle non-finite values.
Results may differ from the reference program's by a relative error of at most 0.018.
Values are sent between devices in bfloat16 or wider.
A program may use at most 768 MiB of HBM per device.

```python
import jax
import jax.numpy as jnp
from jax import lax

SEQUENCES = 256
TOKENS = 2048
D = 896
FF = 2560
LAYERS = 2
NAMES = ("w_gate", "w_up", "w_down")
SHAPES = {"w_gate": (LAYERS, D, FF), "w_up": (LAYERS, D, FF), "w_down": (LAYERS, FF, D)}


def bump(key, n, height):
    away = (jnp.arange(n, dtype=jnp.int32) - jax.random.randint(key, (), 0, n, jnp.int32)) % n
    return jnp.where(away < n // 8, height, 1.0)


def together(key, own, strength):
    shared = jax.random.normal(key, own.shape[1:], jnp.float32)
    return (own + strength * shared) * lax.rsqrt(1 + strength * strength)


def setup_inputs(seed: int = 0, part: int = 0) -> dict:
    kx, kdy, ka, kb, kz, kf, kh, kl, *kw = jax.random.split(jax.random.key(seed), 8 + len(NAMES))
    kx, kdy, ka, kb = (jax.random.fold_in(k, part) for k in (kx, kdy, ka, kb))
    shape = (SEQUENCES, TOKENS, D)
    much_x, much_dy = jax.random.uniform(kz, (2,), jnp.float32, 0.0, 1.0)
    layers = 2.0 ** jax.random.uniform(kl, (LAYERS, 1, 1), jnp.float32, -1.0, 1.0)
    x = together(ka, jax.random.normal(kx, shape, jnp.float32), much_x) * bump(kf, D, 4.0)
    dy = together(kb, jax.random.normal(kdy, shape, jnp.float32), much_dy)
    drawn = {"x": x.astype(jnp.bfloat16), "dy": (dy * (SEQUENCES * TOKENS) ** -0.5).astype(jnp.bfloat16)}
    for key, name in zip(kw, NAMES, strict=True):
        w = jax.random.normal(key, SHAPES[name], jnp.float32) * SHAPES[name][1] ** -0.5
        drawn[name] = (w * {"w_gate": 1.0, "w_up": bump(kh, FF, 4.0), "w_down": layers}[name]).astype(jnp.bfloat16)
    return drawn


def matmul(a, w):
    return jnp.dot(a, w, preferred_element_type=jnp.float32).astype(jnp.bfloat16)


def normed(h):
    wide = h.astype(jnp.float32)
    scale = lax.rsqrt(jnp.mean(wide**2, -1, keepdims=True) + 1e-6)
    return (wide * scale).astype(jnp.bfloat16)


def layer(h, w):
    a = normed(h)
    gate = jnp.dot(a, w["w_gate"], preferred_element_type=jnp.float32)
    up = jnp.dot(a, w["w_up"], preferred_element_type=jnp.float32)
    return h + matmul((jax.nn.silu(gate) * up).astype(jnp.bfloat16), w["w_down"])


def stack(weights, h):
    return lax.scan(lambda h, w: (layer(h, w), None), h, weights)[0]


def reference(x, dy, w_gate, w_up, w_down):
    weights = dict(zip(NAMES, (w_gate, w_up, w_down), strict=True))

    def take(so_far, sequence):
        h, by_y = sequence
        _, back = jax.vjp(stack, weights, h)
        by_weights, by_h = back(by_y)
        return jax.tree.map(lambda total, term: total + term.astype(jnp.float32), so_far, by_weights), by_h

    none_yet = {name: jnp.zeros(w.shape, jnp.float32) for name, w in weights.items()}
    by_weights, by_x = lax.scan(take, none_yet, (x, dy))
    return (by_x, *(by_weights[name].astype(jnp.bfloat16) for name in NAMES))
```

```python
import functools

import jax
import jax.numpy as jnp
from jax import lax
from jax.experimental import pallas as pl
from jax.experimental.pallas import tpu as pltpu
from jax.sharding import PartitionSpec as P

f32, bf16 = jnp.float32, jnp.bfloat16
MESH = pl.DeviceIdType.MESH
LANES = 128
X, CORES, Y = 4, 2, 4
HBM, VMEM, DMA = pl.ANY, pltpu.VMEM, pltpu.SemaphoreType.DMA


def dot(a, b, dims=((1,), (0,))):
    return lax.dot_general(a, b, (dims, ((), ())), preferred_element_type=f32)


def at(start, size, multiple=16):
    return pl.ds(pl.multiple_of(start, multiple) if not isinstance(start, int) else start, size)


class Sizes:
    chunk, rows = 512, 256

    def __init__(self, mesh, tokens, d, ff):
        self.R = mesh.shape["r"]
        self.Z = self.R // Y
        self.T, self.D, self.F = tokens, d, ff
        self.NB = ff // (X * LANES)
        self.FB = X * LANES
        self.h = d // (X * CORES)
        self.TC = min(self.chunk, tokens)
        self.T3 = min(self.rows, tokens)
        self.half = X * self.h
        self.U = 3 * self.half
        per = -(-self.U // self.R)
        self.PR = -(-per // 16) * 16
        self.active = self.U // self.PR
        assert self.active * self.PR == self.U and mesh.shape["s"] == X * CORES


class Here:
    def __init__(self, z):
        s, self.r = lax.axis_index("s"), lax.axis_index("r")
        self.x, self.c = lax.div(s, CORES), lax.rem(s, CORES)
        self.y, self.z, self.Z = lax.div(self.r, z.Z), lax.rem(self.r, z.Z), z.Z
        self.R = z.R

    def partner(self):
        return {"s": self.x * CORES + 1 - self.c}

    def along_x(self, k):
        return {"s": lax.rem(self.x + k, X) * CORES + self.c}

    def along_y(self, k):
        return {"r": lax.rem(self.y + k, Y) * self.Z + self.z}

    def along_r(self, k):
        return {"r": lax.rem(self.r + k, self.R)}


def remote(src, dst, sent, got, where):
    return pltpu.make_async_remote_copy(src_ref=src, dst_ref=dst, send_sem=sent, recv_sem=got, device_id=where, device_id_type=MESH)


def start(copies):
    for copy in copies:
        copy.start()


def wait(ref, sem):
    pltpu.make_async_copy(ref, ref, sem).wait()


def meet(peers):
    barrier = pltpu.get_barrier_semaphore()
    for peer in peers:
        pl.semaphore_signal(barrier, inc=1, device_id=peer, device_id_type=MESH)
    return lambda: pl.semaphore_wait(barrier, len(peers))


class Fetch:
    def __init__(self, z, here, shards, w, sems):
        self.z, self.here, self.shards, self.w = z, here, shards, w
        (
            self.local, self.local_d, self.pair, self.pair_sent, self.a_got, self.a_sent, self.b_got, self.b_sent, self.c_got, self.c_sent,
            self.d_got, self.d_sent, self.e_got, self.e_sent,
        ) = sems

    @staticmethod
    def scratch(z):
        return [DMA((z.NB,)), DMA, DMA, DMA] + [DMA((z.NB,)) for _ in range(10)]

    def rows(self, x):
        return at(x * (CORES * self.z.h) + self.here.c * self.z.h, self.z.h)

    def own(self, j):
        z, here = self.z, self.here
        return [
            pltpu.make_async_copy(shard.at[:, pl.ds((l * z.NB + j) * LANES, LANES)], w.at[j, self.rows(here.x), pl.ds(l * LANES, LANES)], self.local.at[j])
            for shard, w in zip(self.shards[:2], self.w[:2], strict=True)
            for l in range(X)
        ]

    def own_down(self):
        z, here = self.z, self.here
        local, away = [], []
        for k in range(z.NB):
            place = here.c * z.NB + k
            slot = self.w[2].at[lax.div(place, 2), at(here.x * LANES + lax.rem(place, 2) * 64, 64), :]
            src = self.shards[2].at[pl.ds(64 * k, 64), :]
            local.append(pltpu.make_async_copy(src, slot, self.local_d))
            away.append(remote(src, slot, self.pair_sent, self.pair, here.partner()))
        return local, away

    def a(self, j):
        here = self.here
        out = []
        for k in range(1, X):
            for w in self.w[:2]:
                slot = w.at[j, self.rows(here.x), at(here.y * LANES, LANES, LANES)]
                out.append(remote(slot, slot, self.a_sent.at[j], self.a_got.at[j], here.along_x(k)))
        return out

    def d(self, j):
        here = self.here
        slot = self.w[2].at[j, at(here.x * LANES + here.c * 64, 64), :]
        return [remote(slot, slot, self.d_sent.at[j], self.d_got.at[j], here.along_x(k)) for k in range(1, X)]

    def b(self, j):
        here = self.here
        out = []
        for m in range(1, X):
            for k in range(1, Y):
                for w in self.w[:2]:
                    slot = w.at[j, self.rows(lax.rem(here.x + m, X)), at(here.y * LANES, LANES, LANES)]
                    out.append(remote(slot, slot, self.b_sent.at[j], self.b_got.at[j], here.along_y(k)))
        return out

    def c(self, j):
        here = self.here
        return [
            remote(w.at[j, self.rows(x), :], w.at[j, self.rows(x), :], self.c_sent.at[j], self.c_got.at[j], here.partner())
            for w in self.w[:2]
            for x in range(X)
        ]

    def e(self, j):
        here = self.here
        out = []
        for m in range(1, X):
            slot = self.w[2].at[j, at(lax.rem(here.x + m, X) * LANES + here.c * 64, 64), :]
            out.append(remote(slot, slot, self.e_sent.at[j], self.e_got.at[j], here.partner()))
        return out

    def bytes_own(self, j):
        return self.w[0].at[j, pl.ds(0, 2 * self.z.h), :]

    def bytes_down(self):
        return self.w[2].at[0, pl.ds(0, 64 * self.z.NB), :]

    def bytes_a(self, j):
        return self.w[0].at[j, pl.ds(0, 6 * self.z.h), pl.ds(0, LANES)]

    def bytes_b(self, j):
        return self.w[0].at[j, pl.ds(0, 6 * self.z.h), pl.ds(0, 3 * LANES)]

    def bytes_d(self, j):
        return self.w[2].at[j, pl.ds(0, 192), :]

    def begin_local(self):
        for j in range(self.z.NB):
            start(self.own(j))
        start(self.own_down()[0])

    def start_a(self, j):
        wait(self.bytes_own(j), self.local.at[j])
        start(self.a(j))

    def begin(self):
        nb = self.z.NB
        start(self.own_down()[1])
        for j in range(min(2, nb)):
            self.start_a(j)
        wait(self.bytes_down(), self.local_d)
        wait(self.bytes_down(), self.pair)
        for j in range(nb):
            if j >= 2:
                self.start_a(j)
            start(self.d(j))

    def pass_b(self, j):
        wait(self.bytes_a(j), self.a_got.at[j])
        start(self.b(j))

    def pass_c(self, j):
        wait(self.bytes_b(j), self.b_got.at[j])
        start(self.c(j))
        wait(self.bytes_d(j), self.d_got.at[j])
        start(self.e(j))

    def ready(self, j):
        wait(self.w[0].at[j], self.c_got.at[j])
        wait(self.bytes_d(j), self.e_got.at[j])

    def head(self):
        self.pass_b(0)
        if self.z.NB > 1:
            self.pass_b(1)
        self.pass_c(0)

    def serve(self, j):
        pl.when(j + 2 < self.z.NB)(lambda: self.pass_b(j + 2))
        pl.when(j + 1 < self.z.NB)(lambda: self.pass_c(j + 1))
        self.ready(j)

    def end(self):
        wait(self.bytes_down(), self.pair_sent)

        def one(j, _):
            wait(self.bytes_a(j), self.a_sent.at[j])
            wait(self.bytes_b(j), self.b_sent.at[j])
            wait(self.w[0].at[j], self.c_sent.at[j])
            wait(self.bytes_d(j), self.d_sent.at[j])
            wait(self.bytes_d(j), self.e_sent.at[j])
            return 0

        lax.fori_loop(0, self.z.NB, one, 0)


def normed(wide):
    scale = lax.rsqrt(jnp.mean(wide * wide, -1, keepdims=True) + 1e-6)
    return (wide * scale).astype(bf16), scale


def forward_kernel(z, x_in, sg, su, sd, h_out, wg_out, wu_out, wd_out, a, acc, xs, wg, wu, wd, x_sem, out_sem, h_sem, *sems):
    here = Here(z)
    fetch = Fetch(z, here, (sg, su, sd), (wg, wu, wd), sems)
    met = meet([here.partner()] + [here.along_x(k) for k in range(1, X)] + [here.along_y(k) for k in range(1, Y)])
    fetch.begin_local()
    load = pltpu.make_async_copy(x_in, xs, x_sem)
    load.start()
    met()
    fetch.begin()
    load.wait()

    def prepare(i, _):
        rows = at(i * z.T3, z.T3)
        a[rows, :] = normed(xs[rows, :].astype(f32))[0]
        acc[rows, :] = jnp.zeros((z.T3, z.D), f32)
        return 0

    lax.fori_loop(0, z.T // z.T3, prepare, 0)
    fetch.head()

    held = ((wg, wg_out), (wu, wu_out), (wd, wd_out))

    def block(j, _):
        fetch.serve(j)
        start([pltpu.make_async_copy(v.at[j], o.at[j], out_sem.at[k]) for k, (v, o) in enumerate(held)])

        def chunk(i, _):
            rows = at(i * z.TC, z.TC)
            gate, up = dot(a[rows, :], wg[j]), dot(a[rows, :], wu[j])
            act = (gate * (1.0 / (1.0 + jnp.exp(-gate))) * up).astype(bf16)
            acc[rows, :] += dot(act, wd[j])
            return 0

        lax.fori_loop(0, z.T // z.TC, chunk, 0)
        return 0

    lax.fori_loop(0, z.NB, block, 0)

    def finish(i, _):
        rows = at(i * z.T3, z.T3)
        xs[rows, :] = xs[rows, :] + acc[rows, :].astype(bf16)
        return 0

    lax.fori_loop(0, z.T // z.T3, finish, 0)
    store = pltpu.make_async_copy(xs, h_out, h_sem)
    store.start()

    for k, (v, _) in enumerate(held):
        wait(v, out_sem.at[k])
    fetch.end()
    store.wait()


class Reduce:
    def __init__(self, z, here, units, stage, got_p, got_x1, got_x2, got_r, send_x1, send_x2, kept, send_r, send_a, fin, fin_pair, sems):
        self.z, self.here, self.units = z, here, units
        self.stage, self.got_p, self.got_x1, self.got_x2, self.got_r = stage, got_p, got_x1, got_x2, got_r
        self.send_x1, self.send_x2, self.kept, self.send_r, self.send_a = send_x1, send_x2, kept, send_r, send_a
        self.fin, self.fin_pair = fin, fin_pair
        self.p_sent, self.p_got, self.x1_sent, self.x1_got, self.x2_sent, self.x2_got, self.r_sent, self.r_got, self.a_sent, self.a_got, self.f_sent, self.f_got, self.own_done = sems

    @staticmethod
    def scratch(z, units):
        u = z.U
        return [
            VMEM((2, X, CORES, u, LANES), bf16),
            VMEM((units, X, u, LANES), bf16),
            VMEM((units, 2, u // 2, LANES), bf16),
            VMEM((units, 2, u, LANES), bf16),
            VMEM((units, z.R, z.PR, LANES), bf16),
            VMEM((u, LANES), bf16),
            VMEM((2, u, LANES), bf16),
            VMEM((u, LANES), f32),
            VMEM((u, LANES), bf16),
            VMEM((z.PR, LANES), bf16),
        ]

    @staticmethod
    def sems(units):
        return [DMA((units,)) for _ in range(10)] + [DMA, DMA, DMA]

    def peers(self):
        here = self.here
        return [here.partner(), here.along_x(1), here.along_x(X - 1)] + [here.along_r(k) for k in range(1, here.R)]

    def p(self, u):
        here = self.here
        return [remote(self.stage.at[lax.rem(u, 2), x, 1 - here.c], self.got_p.at[u, x], self.p_sent.at[u], self.p_got.at[u], here.partner()) for x in range(X)]

    def start_p(self, u):
        start(self.p(u))

    def both(self, u, x, rows):
        return self.stage[lax.rem(u, 2), x, self.here.c, rows, :].astype(f32) + self.got_p[u, x, rows, :].astype(f32)

    def over(self, work, begin=0, end=None):
        size = self.z.h
        end = self.z.U if end is None else end

        def one(i, _):
            work(at(begin + i * size, size))
            return 0

        lax.fori_loop(0, (end - begin) // size, one, 0)

    def x1(self, u):
        here, half = self.here, self.z.U // 2
        return [
            remote(self.send_x1.at[pl.ds(0, half), :], self.got_x1.at[u, 0], self.x1_sent.at[u], self.x1_got.at[u], here.along_x(1)),
            remote(self.send_x1.at[pl.ds(half, half), :], self.got_x1.at[u, 1], self.x1_sent.at[u], self.x1_got.at[u], here.along_x(X - 1)),
        ]

    def start_x1(self, u):
        wait(self.got_p.at[u], self.p_got.at[u])
        far = lax.rem(self.here.x + 2, X)

        def work(rows):
            self.send_x1[rows, :] = self.both(u, far, rows).astype(bf16)

        self.over(work)
        start(self.x1(u))

    def x2(self, u):
        here = self.here
        return [
            remote(self.send_x2.at[side], self.got_x2.at[u, side], self.x2_sent.at[u], self.x2_got.at[u], here.along_x((1, X - 1)[side]))
            for side in range(2)
        ]

    def start_x2(self, u):
        wait(self.got_x1.at[u], self.x1_got.at[u])
        wait(self.got_x1.at[u], self.x1_sent.at[u])
        half = self.z.U // 2
        right, left = lax.rem(self.here.x + 1, X), lax.rem(self.here.x + X - 1, X)

        def first(rows):
            self.send_x2[0, rows, :] = (self.both(u, right, rows) + self.got_x1[u, 0, rows, :].astype(f32)).astype(bf16)
            self.send_x2[1, rows, :] = self.both(u, left, rows).astype(bf16)

        def second(rows):
            there = at(rows.start - half, rows.size)
            self.send_x2[0, rows, :] = self.both(u, right, rows).astype(bf16)
            self.send_x2[1, rows, :] = (self.both(u, left, rows) + self.got_x1[u, 1, there, :].astype(f32)).astype(bf16)

        self.over(first, 0, half)
        self.over(second, half)
        start(self.x2(u))

    def share(self, p):
        return at(p * self.z.PR, self.z.PR)

    def is_active(self):
        return self.here.r < self.z.active

    def start_r(self, u):
        wait(self.got_x2.at[u], self.x2_got.at[u])
        wait(self.got_x2.at[u], self.x2_sent.at[u])
        wait(self.got_p.at[u], self.p_sent.at[u])

        def work(rows):
            total = self.both(u, self.here.x, rows) + self.got_x2[u, 0, rows, :].astype(f32) + self.got_x2[u, 1, rows, :].astype(f32)
            self.kept[rows, :] = total
            self.send_r[rows, :] = total.astype(bf16)

        self.over(work)

        def send(k, _):
            here, p = self.here, lax.rem(self.here.r + k, self.here.R)

            @pl.when(p < self.z.active)
            def _():
                remote(self.send_r.at[self.share(p), :], self.got_r.at[u, here.r], self.r_sent.at[u], self.r_got.at[u], here.along_r(k)).start()

            return 0

        lax.fori_loop(1, self.z.R, send, 0)

    def start_a(self, u):
        z, here = self.z, self.here

        @pl.when(jnp.logical_not(self.is_active()))
        def _():
            wait(self.got_r.at[u, pl.ds(0, z.active)], self.r_sent.at[u])

        @pl.when(self.is_active())
        def _():
            wait(self.got_r.at[u, pl.ds(0, z.active - 1)], self.r_sent.at[u])
            wait(self.got_r.at[u, pl.ds(0, z.R - 1)], self.r_got.at[u])
            total = self.kept[self.share(here.r), :]
            total = lax.fori_loop(1, z.R, lambda k, t: t + self.got_r[u, lax.rem(here.r + k, z.R)].astype(f32), total)
            pl.when(u > 0)(lambda: self.wait_a_sent(u - 1))
            self.send_a[...] = total.astype(bf16)
            pltpu.make_async_copy(self.send_a, self.fin.at[u, self.share(here.r), :], self.own_done).start()

            def send(k, _):
                remote(self.send_a, self.fin.at[u, self.share(here.r), :], self.a_sent.at[u], self.a_got.at[u], here.along_r(k)).start()
                return 0

            lax.fori_loop(1, z.R, send, 0)

    def wait_a_sent(self, u):
        wait(self.send_a, self.own_done)
        wait(self.got_r.at[u, pl.ds(0, self.z.R - 1)], self.a_sent.at[u])

    def end(self):
        z = self.z
        pl.when(self.is_active())(lambda: self.wait_a_sent(self.units - 1))

        def arrive(u, _):
            @pl.when(jnp.logical_not(self.is_active()))
            def _():
                wait(self.got_r.at[u, pl.ds(0, z.active)], self.a_got.at[u])

            @pl.when(self.is_active())
            def _():
                wait(self.got_r.at[u, pl.ds(0, z.active - 1)], self.a_got.at[u])

            self.f(u).start()
            return 0

        lax.fori_loop(0, self.units, arrive, 0)
        wait(self.fin_pair, self.f_sent)
        wait(self.fin_pair, self.f_got)

    def f(self, u):
        z = self.z
        return remote(self.fin.at[u, pl.ds(2 * z.half, z.half), :], self.fin_pair.at[u], self.f_sent, self.f_got, self.here.partner())


def backward_kernel(z, fetching, h_in, dh_in, w0, w1, w2, dx_out, fin, fin_pair, spill, dx_buf, h_buf, a, at_, dh, dht, wg, wu, wd, work, ld_sem, dh_sem, w_sem, sp_sem, s3_sem, o_sem, *rest):
    T, TC, T3, NB, FB, D = z.T, z.TC, z.T3, z.NB, z.FB, z.D
    here = Here(z)
    n_fetch = len(Fetch.scratch(z)) if fetching else 0
    fetch_sems, rest = rest[:n_fetch], rest[n_fetch:]
    reduce = Reduce(z, here, NB, *rest[:10], fin, fin_pair, rest[10:])
    peers = reduce.peers() + ([here.along_x(2)] if fetching else [])
    met = meet(peers)
    whole = pltpu.make_async_copy(dh_in, dh, dh_sem)
    whole.start()

    def load_h(i):
        return pltpu.make_async_copy(h_in.at[at(i * T3, T3), :], h_buf.at[lax.rem(i, 2)], ld_sem.at[lax.rem(i, 2)])

    load_h(0).start()
    if fetching:
        fetch = Fetch(z, here, (w0, w1, w2), (wg, wu, wd), fetch_sems)
        fetch.begin_local()
        met()
        fetch.begin()
    else:

        def loads(j):
            return [pltpu.make_async_copy(src.at[j], dst.at[j], w_sem.at[k, j]) for k, (src, dst) in enumerate(((w0, wg), (w1, wu), (w2, wd)))]

        for j in range(NB):
            start(loads(j))
    whole.wait()
    n3 = T // T3

    def prepare(i, _):
        rows = at(i * T3, T3, 128)
        pl.when(i + 1 < n3)(lambda: load_h(i + 1).start())
        load_h(i).wait()
        value = normed(h_buf[lax.rem(i, 2)].astype(f32))[0]
        a[rows, :] = value
        at_[:, rows] = value.T
        dht[:, rows] = dh[rows, :].T
        return 0

    lax.fori_loop(0, n3, prepare, 0)
    if fetching:
        fetch.head()
    else:
        met()

    def product(k, rows):
        return work.at[at(k * T + rows.start, rows.size), :]

    def spills(j):
        return [pltpu.make_async_copy(work.at[pl.ds((1 + k) * T, T), :], spill.at[k, j], sp_sem.at[k]) for k in range(2)]

    def spilled(j):
        for copy in spills(j):
            copy.wait()

    def block(j, _):
        if fetching:
            fetch.serve(j)
        else:
            for copy in loads(j):
                copy.wait()
        pl.when(j > 0)(lambda: spilled(j - 1))

        def chunk(i, _):
            rows = at(i * TC, TC)
            gate, up = dot(a[rows, :], wg[j]), dot(a[rows, :], wu[j])
            by_act = dot(dh[rows, :], wd[j], ((1,), (1,))).astype(bf16).astype(f32)
            sig = 1.0 / (1.0 + jnp.exp(-gate))
            silu = gate * sig
            product(0, rows)[...] = (silu * up).astype(bf16)
            product(1, rows)[...] = (by_act * up * (sig + silu * (1.0 - sig))).astype(bf16)
            product(2, rows)[...] = (by_act * silu).astype(bf16)
            return 0

        lax.fori_loop(0, T // TC, chunk, 0)
        start(spills(j))
        pl.when(j > 0)(lambda: reduce.start_x1(j - 1))
        pl.when(j > 1)(lambda: reduce.start_r(j - 2))

        stage, slot = reduce.stage, lax.rem(j, 2)
        m = CORES * z.h

        def rows_of(i, _):
            rows = at(i * m, m)
            gates = dot(at_[rows, :], work[pl.ds(T, T), :]).astype(bf16)
            ups = dot(at_[rows, :], work[pl.ds(2 * T, T), :]).astype(bf16)
            downs = dot(dht[rows, :], work[pl.ds(0, T), :]).astype(bf16)
            for l in range(X):
                lanes = slice(l * LANES, (l + 1) * LANES)
                for c in range(CORES):
                    part = slice(c * z.h, (c + 1) * z.h)
                    stage[slot, i, c, pl.ds(l * z.h, z.h), :] = gates[part, lanes]
                    stage[slot, i, c, pl.ds(z.half + l * z.h, z.h), :] = ups[part, lanes]
                stage[slot, l, lax.div(i, 2), at(2 * z.half + lax.rem(i, 2) * m, m), :] = downs[:, lanes]
            return 0

        lax.fori_loop(0, X, rows_of, 0)
        reduce.start_p(j)
        pl.when(j > 0)(lambda: reduce.start_x2(j - 1))
        pl.when(j > 1)(lambda: reduce.start_a(j - 2))
        return 0

    lax.fori_loop(0, NB, block, 0)
    spilled(NB - 1)

    def load_3(i):
        slot, rows = lax.rem(i, 2), at(i * T3, T3)
        out = [load_h(i)]
        for k in range(2):
            for j in range(NB):
                out.append(pltpu.make_async_copy(spill.at[k, j, rows, :], work.at[at(((slot * 2 + k) * NB + j) * T3, T3), :], s3_sem.at[slot]))
        return out

    def store_3(i):
        return pltpu.make_async_copy(dx_buf.at[lax.rem(i, 2)], dx_out.at[at(i * T3, T3), :], o_sem.at[lax.rem(i, 2)])

    start(load_3(0))
    steps = {1: [lambda: reduce.start_x1(NB - 1)], 3: [lambda: reduce.start_x2(NB - 1)], 6: [lambda: reduce.start_r(NB - 1)]}
    if NB > 1:
        steps.setdefault(0, []).append(lambda: reduce.start_r(NB - 2))
        steps.setdefault(2, []).append(lambda: reduce.start_a(NB - 2))
    last = []
    for i in sorted(steps):
        if i >= n3:
            last += steps.pop(i)

    def rows_back(i, _):
        slot, rows = lax.rem(i, 2), at(i * T3, T3)
        pl.when(i + 1 < n3)(lambda: start(load_3(i + 1)))
        load_h(i).wait()
        wait(work.at[at(slot * 2 * NB * T3, 2 * NB * T3), :], s3_sem.at[slot])
        pl.when(i > 1)(lambda: store_3(i - 2).wait())
        back = []
        for k, w in ((0, wg), (1, wu)):
            total = None
            for j in range(NB):
                part = dot(work[at(((slot * 2 + k) * NB + j) * T3, T3), :], w[j], ((1,), (1,)))
                total = part if total is None else total + part
            back.append(total.astype(bf16))
        by_a = (back[0] + back[1]).astype(f32)
        wide = h_buf[slot].astype(f32)
        square = jnp.mean(wide * wide, -1, keepdims=True) + 1e-6
        scale = lax.rsqrt(square)
        by_scale = jnp.sum(by_a * wide, -1, keepdims=True)
        by_square = by_scale * (-0.5 * scale / square) * (2.0 / D)
        dx_buf[slot] = dh[rows, :] + (by_a * scale + by_square * wide).astype(bf16)
        store_3(i).start()
        for when, todo in steps.items():

            def now(todo=todo):
                for do in todo:
                    do()

            pl.when(i == when)(now)
        return 0

    lax.fori_loop(0, n3, rows_back, 0)
    for do in last:
        do()
    reduce.start_a(NB - 1)
    reduce.end()
    if fetching:
        fetch.end()
    for i in range(max(0, n3 - 2), n3):
        store_3(i).wait()


def call(body, z, out, n_in, scratch, number):
    return pl.pallas_call(
        functools.partial(body, z),
        out_shape=out,
        in_specs=[pl.BlockSpec(memory_space=HBM)] * n_in,
        out_specs=[pl.BlockSpec(memory_space=HBM)] * len(out),
        scratch_shapes=scratch,
        compiler_params=pltpu.CompilerParams(collective_id=number, has_side_effects=True, vmem_limit_bytes=66_900_000),
    )


def forward(z, x, shards):
    S = jax.ShapeDtypeStruct
    wide, tall = (z.NB, z.D, z.FB), (z.NB, z.FB, z.D)
    scratch = [VMEM((z.T, z.D), bf16), VMEM((z.T, z.D), f32), VMEM((z.T, z.D), bf16), VMEM(wide, bf16), VMEM(wide, bf16), VMEM(tall, bf16)]
    out = [S((z.T, z.D), bf16), S(wide, bf16), S(wide, bf16), S(tall, bf16)]
    h, *w = call(forward_kernel, z, out, 4, scratch + [DMA, DMA((3,)), DMA] + Fetch.scratch(z), 0)(x, *shards)
    return h, w


def backward(z, h, dh, w, fetching, number):
    S = jax.ShapeDtypeStruct
    wide, tall = (z.NB, z.D, z.FB), (z.NB, z.FB, z.D)
    tokens = (z.T, z.D)
    scratch = [VMEM((2, z.T3, z.D), bf16), VMEM((2, z.T3, z.D), bf16)]
    scratch += [VMEM(tokens, bf16), VMEM(tokens[::-1], bf16), VMEM(tokens, bf16), VMEM(tokens[::-1], bf16)]
    scratch += [VMEM(wide, bf16), VMEM(wide, bf16), VMEM(tall, bf16), VMEM((max(3 * z.T, 4 * z.NB * z.T3), z.FB), bf16)]
    scratch += [DMA((2,)), DMA, DMA((3, z.NB)), DMA((2,)), DMA((2,)), DMA((2,))]
    if fetching:
        scratch += Fetch.scratch(z)
    scratch += Reduce.scratch(z, z.NB) + Reduce.sems(z.NB)
    out = [S(tokens, bf16), S((z.NB, z.U, LANES), bf16), S((z.NB, z.half, LANES), bf16), S((2, z.NB, z.T, z.FB), bf16)]

    def body(z, *refs):
        backward_kernel(z, fetching, *refs)

    dx, fin, fin_pair, _ = call(body, z, out, 5, scratch, number)(h, dh, *w)
    return dx, fin, fin_pair


def blocks_of(z, fin, fin_pair):
    c = lax.rem(lax.axis_index("s"), CORES)

    def wide(part):
        return part.reshape(z.NB, X, z.h, LANES).transpose(2, 1, 0, 3).reshape(z.h, z.F)

    mine, other = fin[:, 2 * z.half :], fin_pair
    low, high = jnp.where(c == 0, mine, other), jnp.where(c == 0, other, mine)
    down = jnp.concatenate([low, high], 1).transpose(0, 2, 1).reshape(z.NB * LANES, z.D)
    down = lax.dynamic_slice(down, (c * (z.NB * 64), 0), (z.NB * 64, z.D))
    return wide(fin[:, : z.half]), wide(fin[:, z.half : 2 * z.half]), down


def solution(mesh):
    def step(x, dy, *weights):
        z = Sizes(mesh, x.shape[1], x.shape[2], weights[0].shape[2])
        h, w = forward(z, x[0], [v[0] for v in weights])
        dh, *one = backward(z, h, dy[0], [v[1] for v in weights], True, 1)
        dx, *zero = backward(z, x[0], dh, w, False, 2)
        grads = zip(blocks_of(z, *zero), blocks_of(z, *one), strict=True)
        return (dx[None], *(jnp.stack(pair) for pair in grads))

    states, cut = P(("rep", "r", "s"), None, None), P(None, "s", None)
    return jax.shard_map(
        step,
        mesh=mesh,
        in_specs=(states, states) + (cut,) * 3,
        out_specs=(states,) + (P("rep", "s", None),) * 3,
        check_vma=False,
    )
```

```python
import functools

import jax
import jax.numpy as jnp
from jax import lax
from jax.experimental import pallas as pl
from jax.experimental.pallas import tpu as pltpu
from jax.sharding import PartitionSpec as P

f32, bf16 = jnp.float32, jnp.bfloat16
MESH = pl.DeviceIdType.MESH
LANES = 128
X, CORES, Y = 4, 2, 4
HBM, VMEM, DMA = pl.ANY, pltpu.VMEM, pltpu.SemaphoreType.DMA


def dot(a, b, dims=((1,), (0,))):
    return lax.dot_general(a, b, (dims, ((), ())), preferred_element_type=f32)


def at(start, size, multiple=16):
    return pl.ds(pl.multiple_of(start, multiple) if not isinstance(start, int) else start, size)


class Sizes:
    chunk, rows = 1024, 256

    def __init__(self, mesh, tokens, d, ff):
        self.R = mesh.shape["r"]
        self.Z = self.R // Y
        self.T, self.D, self.F = tokens, d, ff
        self.NB = ff // (X * LANES)
        self.FB = X * LANES
        self.h = d // (X * CORES)
        self.TC = min(self.chunk, tokens)
        self.T3 = min(self.rows, tokens)
        self.U = 3 * X * self.h
        self.S = self.U // Y
        self.active = self.h // 16
        assert self.h % 16 == 0 and self.active <= self.Z and mesh.shape["s"] == X * CORES

    def piece(self, y, z, matrix):
        return pl.ds(y * self.S + z * 48 + matrix * 16, 16)


class Here:
    def __init__(self, z):
        s, self.r = lax.axis_index("s"), lax.axis_index("r")
        self.x, self.c = lax.div(s, CORES), lax.rem(s, CORES)
        self.y, self.z, self.Z = lax.div(self.r, z.Z), lax.rem(self.r, z.Z), z.Z
        self.R = z.R

    def partner(self):
        return {"s": self.x * CORES + 1 - self.c}

    def along_x(self, k):
        return {"s": lax.rem(self.x + k, X) * CORES + self.c}

    def along_y(self, k):
        return {"r": lax.rem(self.y + k, Y) * self.Z + self.z}

    def along_z(self, k):
        return {"r": self.y * self.Z + lax.rem(self.z + k, self.Z)}


def remote(src, dst, sent, got, where):
    return pltpu.make_async_remote_copy(src_ref=src, dst_ref=dst, send_sem=sent, recv_sem=got, device_id=where, device_id_type=MESH)


def start(copies):
    for copy in copies:
        copy.start()


def wait(ref, sem):
    pltpu.make_async_copy(ref, ref, sem).wait()


def meet(peers):
    barrier = pltpu.get_barrier_semaphore()
    for peer in peers:
        pl.semaphore_signal(barrier, inc=1, device_id=peer, device_id_type=MESH)
    return lambda: pl.semaphore_wait(barrier, len(peers))


class Fetch:
    PHASES = ("a1", "a2", "b1", "b2", "c", "d1", "d2", "e")

    def __init__(self, z, here, shards, w, sems):
        self.z, self.here, self.shards, self.w = z, here, shards, w
        self.local, self.local_d, self.pair, self.pair_sent = sems[:4]
        self.got = dict(zip(self.PHASES, sems[4::2], strict=True))
        self.sent = dict(zip(self.PHASES, sems[5::2], strict=True))

    @classmethod
    def scratch(cls, z):
        return [DMA((z.NB,)), DMA, DMA, DMA] + [DMA((z.NB,)) for _ in range(2 * len(cls.PHASES))]

    def peers(self):
        here = self.here
        return [here.partner()] + [here.along_x(k) for k in range(1, X)] + [here.along_y(k) for k in range(1, Y)]

    def own(self, j):
        z, here = self.z, self.here
        for shard, w in zip(self.shards[:2], self.w[:2], strict=True):
            for l in range(X):
                slot = w.at[j, self.rows(here.x), pl.ds(l * LANES, LANES)]
                pltpu.make_async_copy(shard.at[:, at((l * z.NB + j) * LANES, LANES, LANES)], slot, self.local.at[j]).start()

    def own_down(self, k):
        z, here = self.z, self.here
        place = here.c * z.NB + k
        return self.shards[2].at[pl.ds(64 * k, 64), :], self.w[2].at[lax.div(place, 2), at(here.x * LANES + lax.rem(place, 2) * 64, 64), :]

    def rows(self, x):
        return at(x * (CORES * self.z.h) + self.here.c * self.z.h, self.z.h)

    def lanes(self, y):
        return at(y * LANES, LANES, LANES)

    def down(self, x, begin=0, size=64):
        return at(x * LANES + self.here.c * 64 + begin, size)

    def send(self, phase, j, w, rows, lanes, where):
        slot = self.w[w].at[j, rows, lanes]
        remote(slot, slot, self.sent[phase].at[j], self.got[phase].at[j], where).start()

    def begin_local(self):
        for j in range(self.z.NB):
            self.own(j)
        for k in range(self.z.NB):
            pltpu.make_async_copy(*self.own_down(k), self.local_d).start()

    def start_a1(self, j, first=False):
        here = self.here
        wait(self.w[0].at[j, pl.ds(0, 2 * self.z.h), :], self.local.at[j])
        for k in (1, 3, 2) if first else (1, 3):
            for w in range(2):
                self.send("a1", j, w, self.rows(here.x), self.lanes(here.y), here.along_x(k))

    def start_d1(self, j, first=False):
        here = self.here
        for k in (1, 3, 2) if first else (1, 3):
            self.send("d1", j, 2, self.down(here.x), slice(None), here.along_x(k))

    def start_2(self, j):
        here = self.here
        left, right = lax.rem(here.x + 3, X), lax.rem(here.x + 1, X)
        wait(self.pieces(j, 4), self.got["a1"].at[j])
        self.send("a2", j, 0, self.rows(left), self.lanes(here.y), here.along_x(1))
        self.send("a2", j, 1, self.rows(right), self.lanes(here.y), here.along_x(3))
        wait(self.halves(j, 2), self.got["d1"].at[j])
        self.send("d2", j, 2, self.down(left, 0, 32), slice(None), here.along_x(1))
        self.send("d2", j, 2, self.down(right, 32, 32), slice(None), here.along_x(3))

    def start_b1(self, j, first=False):
        here = self.here
        if first:
            wait(self.pieces(j, 6), self.got["a1"].at[j])
        else:
            wait(self.pieces(j, 2), self.got["a2"].at[j])
        for k in (1, 3, 2) if first else (1, 3):
            for m in range(1, X):
                for w in range(2):
                    self.send("b1", j, w, self.rows(lax.rem(here.x + m, X)), self.lanes(here.y), here.along_y(k))

    def start_b2(self, j):
        here = self.here
        wait(self.pieces(j, 12), self.got["b1"].at[j])
        for m in range(1, X):
            rows = self.rows(lax.rem(here.x + m, X))
            self.send("b2", j, 0, rows, self.lanes(lax.rem(here.y + 3, Y)), here.along_y(1))
            self.send("b2", j, 1, rows, self.lanes(lax.rem(here.y + 1, Y)), here.along_y(3))

    def start_c(self, j, first=False):
        here = self.here
        if first:
            wait(self.pieces(j, 18), self.got["b1"].at[j])
        else:
            wait(self.pieces(j, 6), self.got["b2"].at[j])
        for w in range(2):
            for x in range(X):
                self.send("c", j, w, self.rows(x), slice(None), here.partner())
        if first:
            wait(self.halves(j, 3), self.got["d1"].at[j])
        else:
            wait(self.halves(j, 1), self.got["d2"].at[j])
        for m in range(1, X):
            self.send("e", j, 2, self.down(lax.rem(here.x + m, X)), slice(None), here.partner())

    def pieces(self, j, n):
        return self.w[0].at[j, pl.ds(0, min(n, 6) * self.z.h), pl.ds(0, max(n // 6, 1) * LANES)]

    def halves(self, j, n):
        return self.w[2].at[j, pl.ds(0, 64 * n), :]

    def begin(self):
        nb = self.z.NB
        for k in range(nb):
            src, slot = self.own_down(k)
            remote(src, slot, self.pair_sent, self.pair, self.here.partner()).start()
        self.start_a1(0, True)
        if nb > 1:
            self.start_a1(1)
        wait(self.halves(0, nb), self.local_d)
        wait(self.halves(0, nb), self.pair)
        self.start_d1(0, True)
        if nb > 1:
            self.start_d1(1)

    def head(self):
        nb = self.z.NB
        self.start_b1(0, True)
        if nb > 1:
            self.start_2(1)
        if nb > 2:
            self.start_a1(2)
            self.start_d1(2)
        self.start_c(0, True)
        if nb > 1:
            self.start_b1(1)

    def serve_a(self, j):
        nb = self.z.NB
        pl.when(j + 1 < nb)(lambda: self.start_b2(j + 1))
        pl.when(j + 2 < nb)(lambda: self.start_2(j + 2))
        wait(self.w[0].at[j], self.got["c"].at[j])
        wait(self.halves(j, 3), self.got["e"].at[j])

    def serve_b(self, j):
        nb = self.z.NB
        pl.when(j + 1 < nb)(lambda: self.start_c(j + 1))
        pl.when(j + 2 < nb)(lambda: self.start_b1(j + 2))

        @pl.when(j + 3 < nb)
        def _():
            self.start_a1(j + 3)
            self.start_d1(j + 3)

    def end(self):
        wait(self.halves(0, self.z.NB), self.pair_sent)

        def drain(j, first):
            wait(self.pieces(j, 6 if first else 4), self.sent["a1"].at[j])
            wait(self.pieces(j, 18 if first else 12), self.sent["b1"].at[j])
            wait(self.halves(j, 3 if first else 2), self.sent["d1"].at[j])
            if not first:
                wait(self.pieces(j, 2), self.sent["a2"].at[j])
                wait(self.pieces(j, 6), self.sent["b2"].at[j])
                wait(self.halves(j, 1), self.sent["d2"].at[j])
            wait(self.w[0].at[j], self.sent["c"].at[j])
            wait(self.halves(j, 3), self.sent["e"].at[j])
            return 0

        drain(0, True)
        lax.fori_loop(1, self.z.NB, lambda j, _: drain(j, False), 0)


def normed(wide):
    scale = lax.rsqrt(jnp.mean(wide * wide, -1, keepdims=True) + 1e-6)
    return (wide * scale).astype(bf16), scale


def forward_kernel(z, x_in, sg, su, sd, h_out, wg_out, wu_out, wd_out, a, acc, xs, act, wg, wu, wd, x_sem, out_sem, h_sem, *sems):
    here = Here(z)
    fetch = Fetch(z, here, (sg.at[0], su.at[0], sd.at[0]), (wg, wu, wd), sems)
    met = meet(fetch.peers())
    fetch.begin_local()
    load = pltpu.make_async_copy(x_in, xs, x_sem)
    load.start()
    met()
    fetch.begin()
    load.wait()

    def prepare(i, _):
        rows = at(i * z.T3, z.T3)
        a[rows, :] = normed(xs[rows, :].astype(f32))[0]
        acc[rows, :] = jnp.zeros((z.T3, z.D), f32)
        return 0

    lax.fori_loop(0, z.T // z.T3, prepare, 0)
    fetch.head()
    held = ((wg, wg_out), (wu, wu_out), (wd, wd_out))
    n = z.T // z.TC

    def block(j, _):
        fetch.serve_a(j)
        start([pltpu.make_async_copy(v.at[j], o.at[j], out_sem.at[k]) for k, (v, o) in enumerate(held)])

        def chunk(i, _):
            pl.when(i == n // 2)(lambda: fetch.serve_b(j))
            rows = at(i * z.TC, z.TC)
            for half in range(2):
                cols = slice(half * z.FB // 2, (half + 1) * z.FB // 2)
                gate, up = dot(a[rows, :], wg[j, :, cols]), dot(a[rows, :], wu[j, :, cols])
                act[:, cols] = (gate * (1.0 / (1.0 + jnp.exp(-gate))) * up).astype(bf16)
            acc[rows, :] += dot(act[...], wd[j])
            return 0

        lax.fori_loop(0, n, chunk, 0)
        return 0

    lax.fori_loop(0, z.NB, block, 0)

    def finish(i, _):
        rows = at(i * z.T3, z.T3)
        xs[rows, :] = xs[rows, :] + acc[rows, :].astype(bf16)
        return 0

    lax.fori_loop(0, z.T // z.T3, finish, 0)
    store = pltpu.make_async_copy(xs, h_out, h_sem)
    store.start()
    for k, (v, _) in enumerate(held):
        wait(v, out_sem.at[k])
    fetch.end()
    store.wait()


class Reduce:
    PHASES = ("p", "x1", "x2", "y", "z", "az", "ay", "f")

    def __init__(self, z, here, units, fin_out, pair_out, refs):
        self.z, self.here, self.units, self.fin_out, self.pair_out = z, here, units, fin_out, pair_out
        (self.stage, self.got_p, self.got_x1, self.got_x2, self.got_y, self.got_z) = refs[:6]
        (self.send_x1, self.send_x2, self.send_y, self.send_z, self.kept_y, self.kept_z, self.fin) = refs[6:13]
        self.got = dict(zip(self.PHASES, refs[13:29:2], strict=True))
        self.sent = dict(zip(self.PHASES, refs[14:29:2], strict=True))
        self.out_sem = refs[29]

    @classmethod
    def scratch(cls, z, units):
        u, s = z.U, z.S
        data = [(2, X, CORES, u), (3, X, u), (2, 2, u // 2), (2, 2, u), (2, Y, s), (units, z.Z, 48), (u,), (2, u), (u,), (s,)]
        return (
            [VMEM((*shape, LANES), bf16) for shape in data]
            + [VMEM((s, LANES), f32), VMEM((s, LANES), f32), VMEM((units, u, LANES), bf16)]
            + [DMA((units,)) for _ in range(2 * len(cls.PHASES))]
            + [DMA((units,))]
        )

    def peers(self):
        here = self.here
        return (
            [here.partner(), here.along_x(1), here.along_x(3)] + [here.along_y(k) for k in range(1, Y)] + [here.along_z(k) for k in range(1, here.Z)]
        )

    def send(self, phase, u, src, dst, where):
        remote(src, dst, self.sent[phase].at[u], self.got[phase].at[u], where).start()

    def over(self, work, begin, end):
        size = self.z.h

        def one(i, _):
            work(at(begin + i * size, size))
            return 0

        lax.fori_loop(0, (end - begin) // size, one, 0)

    def start_p(self, u):
        here = self.here
        for x in range(X):
            self.send("p", u, self.stage.at[lax.rem(u, 2), x, 1 - here.c], self.got_p.at[lax.rem(u, 3), x], here.partner())

    def both(self, u, x, rows):
        return self.stage[lax.rem(u, 2), x, self.here.c, rows, :].astype(f32) + self.got_p[lax.rem(u, 3), x, rows, :].astype(f32)

    def start_x1(self, u):
        here, half, slot = self.here, self.z.U // 2, lax.rem(u, 2)
        wait(self.got_p.at[lax.rem(u, 3)], self.got["p"].at[u])
        far = lax.rem(here.x + 2, X)

        def work(rows):
            self.send_x1[rows, :] = self.both(u, far, rows).astype(bf16)

        self.over(work, 0, self.z.U)
        for side in range(2):
            self.send("x1", u, self.send_x1.at[pl.ds(side * half, half), :], self.got_x1.at[slot, side], here.along_x((1, 3)[side]))

    def start_x2(self, u):
        here, half, slot = self.here, self.z.U // 2, lax.rem(u, 2)
        wait(self.got_x1.at[slot], self.got["x1"].at[u])
        wait(self.got_x1.at[slot], self.sent["x1"].at[u])
        right, left = lax.rem(here.x + 1, X), lax.rem(here.x + 3, X)

        def first(rows):
            self.send_x2[0, rows, :] = (self.both(u, right, rows) + self.got_x1[slot, 0, rows, :].astype(f32)).astype(bf16)
            self.send_x2[1, rows, :] = self.both(u, left, rows).astype(bf16)

        def second(rows):
            there = at(rows.start - half, rows.size)
            self.send_x2[0, rows, :] = self.both(u, right, rows).astype(bf16)
            self.send_x2[1, rows, :] = (self.both(u, left, rows) + self.got_x1[slot, 1, there, :].astype(f32)).astype(bf16)

        self.over(first, 0, half)
        self.over(second, half, self.z.U)
        for side in range(2):
            self.send("x2", u, self.send_x2.at[side], self.got_x2.at[slot, side], here.along_x((1, 3)[side]))

    def start_y(self, u):
        z, here, slot = self.z, self.here, lax.rem(u, 2)
        wait(self.got_x2.at[slot], self.got["x2"].at[u])
        wait(self.got_x2.at[slot], self.sent["x2"].at[u])
        wait(self.got_p.at[lax.rem(u, 3)], self.sent["p"].at[u])

        def total(rows):
            return self.both(u, here.x, rows) + self.got_x2[slot, 0, rows, :].astype(f32) + self.got_x2[slot, 1, rows, :].astype(f32)

        def work(rows):
            self.send_y[rows, :] = total(rows).astype(bf16)

        def own(rows):
            self.kept_y[rows, :] = total(at(here.y * z.S + rows.start, rows.size))

        self.over(work, 0, z.U)
        self.over(own, 0, z.S)
        for k in (1, 3, 2):
            self.send("y", u, self.send_y.at[at(lax.rem(here.y + k, Y) * z.S, z.S), :], self.got_y.at[slot, here.y], here.along_y(k))

    def start_z(self, u):
        z, here, slot = self.z, self.here, lax.rem(u, 2)
        wait(self.got_y.at[slot, pl.ds(0, Y - 1)], self.got["y"].at[u])
        wait(self.got_y.at[slot, pl.ds(0, Y - 1)], self.sent["y"].at[u])

        def work(rows):
            total = self.kept_y[rows, :]
            for k in range(1, Y):
                total += self.got_y[slot, lax.rem(here.y + k, Y), rows, :].astype(f32)
            self.kept_z[rows, :] = total
            self.send_z[rows, :] = total.astype(bf16)

        self.over(work, 0, z.S)
        for k in range(1, z.Z):
            to = lax.rem(here.z + k, z.Z)
            pl.when(to < z.active)(lambda k=k, to=to: self.send("z", u, self.send_z.at[at(to * 48, 48), :], self.got_z.at[u, here.z], here.along_z(k)))

    def if_active(self, yes, no):
        pl.when(self.here.z < self.z.active)(yes)
        pl.when(self.here.z >= self.z.active)(no)

    def pieces(self, u, n):
        return self.fin.at[u, pl.ds(0, 48 * n), :]

    def wait_pieces(self, u, n, sem):
        if n:
            wait(self.pieces(u, n), sem.at[u])

    def start_az(self, u):
        z, here = self.z, self.here

        def yes():
            self.wait_pieces(u, z.active - 1, self.sent["z"])
            self.wait_pieces(u, z.Z - 1, self.got["z"])
            total = self.kept_z[at(here.z * 48, 48), :]
            for k in range(1, z.Z):
                total += self.got_z[u, lax.rem(here.z + k, z.Z)].astype(f32)
            mine = at(here.y * z.S + here.z * 48, 48)
            self.fin[u, mine, :] = total.astype(bf16)
            for k in range(1, z.Z):
                self.send("az", u, self.fin.at[u, mine, :], self.fin.at[u, mine, :], here.along_z(k))

        self.if_active(yes, lambda: self.wait_pieces(u, z.active, self.sent["z"]))

    def start_ay(self, u):
        z, here = self.z, self.here
        self.if_active(lambda: self.wait_pieces(u, z.active - 1, self.got["az"]), lambda: self.wait_pieces(u, z.active, self.got["az"]))
        share = self.fin.at[u, at(here.y * z.S, z.S), :]
        for k in (1, 3, 2):
            self.send("ay", u, share, share, here.along_y(k))

    def start_f(self, u):
        wait(self.fin.at[u, pl.ds(0, (Y - 1) * self.z.S), :], self.got["ay"].at[u])
        self.send("f", u, self.fin.at[u], self.pair_out.at[u], self.here.partner())
        pltpu.make_async_copy(self.fin.at[u], self.fin_out.at[u], self.out_sem.at[u]).start()

    def end(self):
        z = self.z

        def one(u, _):
            self.if_active(lambda: self.wait_pieces(u, z.Z - 1, self.sent["az"]), lambda: None)
            wait(self.fin.at[u, pl.ds(0, (Y - 1) * z.S), :], self.sent["ay"].at[u])
            wait(self.fin.at[u], self.sent["f"].at[u])
            wait(self.fin.at[u], self.got["f"].at[u])
            wait(self.fin.at[u], self.out_sem.at[u])
            return 0

        lax.fori_loop(0, self.units, one, 0)


def backward_kernel(z, first, *refs):
    T, TC, T3, NB, FB, D = z.T, z.TC, z.T3, z.NB, z.FB, z.D
    here = Here(z)
    refs = list(refs)

    def take(n):
        out, refs[:] = refs[:n], refs[n:]
        return out

    h_in, dh_in, w0, w1, w2 = take(5)
    left_in = None if first else take(1)[0]
    dx_out, fin_out, pair_out, spill = take(4)
    left_out = take(1)[0] if first else None
    dx_buf, h_buf, a, a_t, dh, dh_t, wg, wu, wd, work = take(10)
    ld_sem, dh_sem, w_sem, sp_sem, s3_sem, o_sem, left_sem = take(7)
    fetch = Fetch(z, here, (w0.at[1], w1.at[1], w2.at[1]), (wg, wu, wd), take(len(Fetch.scratch(z)))) if first else None
    base = 0 if first else 1
    units = NB - 1 if first else NB + 1
    reduce = Reduce(z, here, units, fin_out, pair_out, refs)
    met = meet(reduce.peers() + ([here.along_x(2)] if first else []))
    whole = pltpu.make_async_copy(dh_in, dh, dh_sem)
    whole.start()

    def load_h(i):
        return pltpu.make_async_copy(h_in.at[at(i * T3, T3), :], h_buf.at[lax.rem(i, 2)], ld_sem.at[lax.rem(i, 2)])

    load_h(0).start()

    def loads(j):
        return [pltpu.make_async_copy(src.at[j], dst.at[j], w_sem.at[k, j]) for k, (src, dst) in enumerate(((w0, wg), (w1, wu), (w2, wd)))]

    if first:
        fetch.begin_local()
        met()
        fetch.begin()
    else:
        left = pltpu.make_async_copy(left_in, reduce.stage.at[0], left_sem)
        left.start()
        for j in range(NB):
            start(loads(j))
    whole.wait()
    n3 = T // T3

    def prepare(i, _):
        rows = at(i * T3, T3, 128)
        pl.when(i + 1 < n3)(lambda: load_h(i + 1).start())
        load_h(i).wait()
        value = normed(h_buf[lax.rem(i, 2)].astype(f32))[0]
        a[rows, :] = value
        a_t[:, rows] = value.T
        dh_t[:, rows] = dh[rows, :].T
        return 0

    if not first:
        met()
        left.wait()
        reduce.start_p(0)
    lax.fori_loop(0, n3, prepare, 0)
    if first:
        fetch.head()

    def product(k, rows, cols):
        return work.at[at(k * T + rows.start, rows.size), cols]

    def spills(j):
        return [pltpu.make_async_copy(work.at[pl.ds((1 + k) * T, T), :], spill.at[k, j], sp_sem.at[k]) for k in range(2)]

    def spilled(j):
        for copy in spills(j):
            copy.wait()

    def step(name, u):
        do = getattr(reduce, "start_" + name)
        if isinstance(u, int):
            if 0 <= u < units:
                do(u)
        else:
            pl.when(jnp.logical_and(u >= 0, u < units))(lambda: do(u))

    def halfway(i, n, before, after):
        if n == 1:
            before()
            after()
        else:
            pl.when(i == 0)(before)
            pl.when(i == n // 2)(after)

    def block(j, _):
        u = j + base - 1
        if first:
            fetch.serve_a(j)
        else:
            for copy in loads(j):
                copy.wait()
        pl.when(j > 0)(lambda: spilled(j - 1))

        def chunk(i, _):
            def before():
                step("ay", u - 3)
                step("z", u - 2)

            halfway(i, T // TC, before, lambda: step("x1", u))
            rows = at(i * TC, TC)
            for half in range(2):
                cols = slice(half * FB // 2, (half + 1) * FB // 2)
                gate, up = dot(a[rows, :], wg[j, :, cols]), dot(a[rows, :], wu[j, :, cols])
                by_act = dot(dh[rows, :], wd[j, cols, :], ((1,), (1,))).astype(bf16).astype(f32)
                sig = 1.0 / (1.0 + jnp.exp(-gate))
                silu = gate * sig
                product(0, rows, cols)[...] = (silu * up).astype(bf16)
                product(1, rows, cols)[...] = (by_act * up * (sig + silu * (1.0 - sig))).astype(bf16)
                product(2, rows, cols)[...] = (by_act * silu).astype(bf16)
            return 0

        lax.fori_loop(0, T // TC, chunk, 0)
        start(spills(j))
        stage, slot, m = reduce.stage, lax.rem(j + base, 2), D // 2

        def rows_of(i, _):
            def before():
                if first:
                    fetch.serve_b(j)
                step("y", u - 1)
                step("az", u - 2)

            halfway(i, 2, before, lambda: step("x2", u))
            rows = at(i * m, m)
            gates = dot(a_t[rows, :], work[pl.ds(T, T), :]).astype(bf16)
            ups = dot(a_t[rows, :], work[pl.ds(2 * T, T), :]).astype(bf16)
            downs = dot(dh_t[rows, :], work[pl.ds(0, T), :]).astype(bf16)
            for y in range(Y):
                lanes = slice(y * LANES, (y + 1) * LANES)
                for p in range(z.active):
                    for x in range(X // 2):
                        for c in range(CORES):
                            part = slice((x * CORES + c) * z.h + p * 16, (x * CORES + c) * z.h + (p + 1) * 16)
                            stage[slot, i * (X // 2) + x, c, z.piece(y, p, 0), :] = gates[part, lanes]
                            stage[slot, i * (X // 2) + x, c, z.piece(y, p, 1), :] = ups[part, lanes]
                    for x in range(X):
                        stage[slot, x, i, z.piece(y, p, 2), :] = downs[y * z.h + p * 16 : y * z.h + (p + 1) * 16, x * LANES : (x + 1) * LANES]
            return 0

        lax.fori_loop(0, 2, rows_of, 0)
        step("p", j + base)
        return 0

    lax.fori_loop(0, NB, block, 0)
    if first:
        left = pltpu.make_async_copy(reduce.stage.at[(NB - 1) % 2], left_out, left_sem)
        left.start()
    spilled(NB - 1)

    def load_3(i):
        slot, rows = lax.rem(i, 2), at(i * T3, T3)
        out = [load_h(i)]
        for k in range(2):
            for j in range(NB):
                out.append(pltpu.make_async_copy(spill.at[k, j, rows, :], work.at[at(((slot * 2 + k) * NB + j) * T3, T3), :], s3_sem.at[slot]))
        return out

    def store_3(i):
        return pltpu.make_async_copy(dx_buf.at[lax.rem(i, 2)], dx_out.at[at(i * T3, T3), :], o_sem.at[lax.rem(i, 2)])

    start(load_3(0))
    u = NB + base - 1
    todo = {
        0: [("ay", u - 3), ("z", u - 2)],
        1: [("x1", u), ("az", u - 2)],
        2: [("y", u - 1)],
        3: [("x2", u), ("ay", u - 2)],
        4: [("z", u - 1)],
        5: [("az", u - 1), ("f", 0)],
        6: [("y", u), ("ay", u - 1)],
        7: [("f", v) for v in range(1, u - 1)],
    }

    def rows_back(i, _):
        slot, rows = lax.rem(i, 2), at(i * T3, T3)
        pl.when(i + 1 < n3)(lambda: start(load_3(i + 1)))
        for when, steps in todo.items():

            def now(steps=steps):
                for each in steps:
                    step(*each)

            pl.when(i == when)(now)
        load_h(i).wait()
        wait(work.at[at(slot * 2 * NB * T3, 2 * NB * T3), :], s3_sem.at[slot])
        pl.when(i > 1)(lambda: store_3(i - 2).wait())
        back = []
        for k, w in ((0, wg), (1, wu)):
            total = None
            for j in range(NB):
                part = dot(work[at(((slot * 2 + k) * NB + j) * T3, T3), :], w[j], ((1,), (1,)))
                total = part if total is None else total + part
            back.append(total.astype(bf16))
        by_a = (back[0] + back[1]).astype(f32)
        wide = h_buf[slot].astype(f32)
        square = jnp.mean(wide * wide, -1, keepdims=True) + 1e-6
        scale = lax.rsqrt(square)
        by_scale = jnp.sum(by_a * wide, -1, keepdims=True)
        by_square = by_scale * (-0.5 * scale / square) * (2.0 / D)
        dx_buf[slot] = dh[rows, :] + (by_a * scale + by_square * wide).astype(bf16)
        store_3(i).start()
        return 0

    lax.fori_loop(0, n3, rows_back, 0)
    assert n3 > max(todo)
    step("f", u - 1)
    for name in ("z", "az", "ay", "f"):
        step(name, u)
    reduce.end()
    if first:
        fetch.end()
        left.wait()
    for i in range(max(0, n3 - 2), n3):
        store_3(i).wait()


def call(body, out, n_in, scratch, number):
    return pl.pallas_call(
        body,
        out_shape=out,
        in_specs=[pl.BlockSpec(memory_space=HBM)] * n_in,
        out_specs=[pl.BlockSpec(memory_space=HBM)] * len(out),
        scratch_shapes=scratch,
        compiler_params=pltpu.CompilerParams(collective_id=number, has_side_effects=True, vmem_limit_bytes=66_900_000),
    )


def forward(z, x, shards):
    S = jax.ShapeDtypeStruct
    wide, tall, tokens = (z.NB, z.D, z.FB), (z.NB, z.FB, z.D), (z.T, z.D)
    scratch = [VMEM(tokens, bf16), VMEM(tokens, f32), VMEM(tokens, bf16), VMEM((z.TC, z.FB), bf16), VMEM(wide, bf16), VMEM(wide, bf16), VMEM(tall, bf16)]
    scratch += [DMA, DMA((3,)), DMA] + Fetch.scratch(z)
    out = [S(tokens, bf16), S(wide, bf16), S(wide, bf16), S(tall, bf16)]
    h, *w = call(functools.partial(forward_kernel, z), out, 4, scratch, 0)(x, *shards)
    return h, w


def backward(z, h, dh, w, left):
    S = jax.ShapeDtypeStruct
    first = left is None
    wide, tall, tokens = (z.NB, z.D, z.FB), (z.NB, z.FB, z.D), (z.T, z.D)
    units = z.NB - 1 if first else z.NB + 1
    scratch = [VMEM((2, z.T3, z.D), bf16), VMEM((2, z.T3, z.D), bf16)]
    scratch += [VMEM(tokens, bf16), VMEM(tokens[::-1], bf16), VMEM(tokens, bf16), VMEM(tokens[::-1], bf16)]
    scratch += [VMEM(wide, bf16), VMEM(wide, bf16), VMEM(tall, bf16), VMEM((max(3 * z.T, 4 * z.NB * z.T3), z.FB), bf16)]
    scratch += [DMA((2,)), DMA, DMA((3, z.NB)), DMA((2,)), DMA((2,)), DMA((2,)), DMA]
    if first:
        scratch += Fetch.scratch(z)
    scratch += Reduce.scratch(z, units)
    out = [S(tokens, bf16), S((units, z.U, LANES), bf16), S((units, z.U, LANES), bf16), S((2, z.NB, z.T, z.FB), bf16)]
    if first:
        out.append(S((X, CORES, z.U, LANES), bf16))
    args = (h, dh, *w) if first else (h, dh, *w, left)
    dx, fin, pair, _, *left = call(functools.partial(backward_kernel, z, first), out, len(args), scratch, 1 if first else 2)(*args)
    return dx, fin, pair, left


def gradients(z, fin, pair):
    c = lax.rem(lax.axis_index("s"), CORES)
    fin, pair = (v.reshape(2, z.NB, Y, z.active, 3, 16, LANES)[::-1] for v in (fin, pair))

    def wide(matrix):
        return fin[:, :, :, :, matrix].transpose(0, 3, 4, 2, 1, 5).reshape(2, z.h, z.F)

    mine, other = fin[:, :, :, :, 2], pair[:, :, :, :, 2]
    low, high = jnp.where(c == 0, mine, other), jnp.where(c == 0, other, mine)
    down = jnp.stack([low, high], 1)
    down = down.transpose(0, 2, 6, 1, 3, 4, 5).reshape(2, z.NB * LANES, z.D)
    return wide(0), wide(1), lax.dynamic_slice(down, (0, c * (z.NB * 64), 0), (2, z.NB * 64, z.D))


def solution(mesh):
    def step(x, dy, *weights):
        z = Sizes(mesh, x.shape[1], x.shape[2], weights[0].shape[2])
        h, w = forward(z, x[0], weights)
        dh, fin_1, pair_1, left = backward(z, h, dy[0], weights, None)
        dx, fin_0, pair_0, _ = backward(z, x[0], dh, w, left[0])
        return (dx[None], *gradients(z, jnp.concatenate([fin_1, fin_0]), jnp.concatenate([pair_1, pair_0])))

    states, cut = P(("rep", "r", "s"), None, None), P(None, "s", None)
    return jax.shard_map(
        step,
        mesh=mesh,
        in_specs=(states, states) + (cut,) * 3,
        out_specs=(states,) + (P("rep", "s", None),) * 3,
        check_vma=False,
    )
```

```python
import functools

import jax
import jax.numpy as jnp
from jax import lax
from jax.experimental import pallas as pl
from jax.experimental.pallas import tpu as pltpu
from jax.sharding import PartitionSpec as P

f32, bf16 = jnp.float32, jnp.bfloat16
MESH = pl.DeviceIdType.MESH
LANES = 128
X, CORES, Y = 4, 2, 4
HBM, VMEM, DMA = pl.ANY, pltpu.VMEM, pltpu.SemaphoreType.DMA


def dot(a, b, dims=((1,), (0,))):
    return lax.dot_general(a, b, (dims, ((), ())), preferred_element_type=f32)


def at(start, size, multiple=16):
    return pl.ds(pl.multiple_of(start, multiple) if not isinstance(start, int) else start, size)


class Sizes:
    chunk, piece, rows = 1024, 512, 256

    def __init__(self, mesh, tokens, d, ff):
        self.R = mesh.shape["r"]
        self.Z = self.R // Y
        self.T, self.D, self.F = tokens, d, ff
        self.NB = ff // (X * LANES)
        self.FB = X * LANES
        self.h = d // (X * CORES)
        self.TC = min(self.chunk, tokens)
        self.T3 = min(self.rows, tokens)
        self.TS = min(self.piece, tokens)
        self.unit = (Y, 3, self.h, LANES)
        self.active = self.h // 16
        assert self.h % 16 == 0 and self.active <= self.Z and mesh.shape["s"] == X * CORES


class Here:
    def __init__(self, z):
        s, self.r = lax.axis_index("s"), lax.axis_index("r")
        self.x, self.c = lax.div(s, CORES), lax.rem(s, CORES)
        self.y, self.z, self.Z = lax.div(self.r, z.Z), lax.rem(self.r, z.Z), z.Z
        self.R = z.R

    def partner(self):
        return {"s": self.x * CORES + 1 - self.c}

    def along_x(self, k):
        return {"s": lax.rem(self.x + k, X) * CORES + self.c}

    def along_y(self, k):
        return {"r": lax.rem(self.y + k, Y) * self.Z + self.z}

    def along_z(self, k):
        return {"r": self.y * self.Z + lax.rem(self.z + k, self.Z)}


def remote(src, dst, sent, got, where):
    return pltpu.make_async_remote_copy(src_ref=src, dst_ref=dst, send_sem=sent, recv_sem=got, device_id=where, device_id_type=MESH)


def start(copies):
    for copy in copies:
        copy.start()


def wait(ref, sem):
    pltpu.make_async_copy(ref, ref, sem).wait()


def meet(peers):
    barrier = pltpu.get_barrier_semaphore()
    for peer in peers:
        pl.semaphore_signal(barrier, inc=1, device_id=peer, device_id_type=MESH)
    return lambda: pl.semaphore_wait(barrier, len(peers))


class Fetch:
    PHASES = ("a1", "a2", "b1", "b2", "c", "d1", "d2", "e")

    def __init__(self, z, here, shards, w, sems):
        self.z, self.here, self.shards, self.w = z, here, shards, w
        self.local, self.local_d, self.pair, self.pair_sent = sems[:4]
        self.got = dict(zip(self.PHASES, sems[4::2], strict=True))
        self.sent = dict(zip(self.PHASES, sems[5::2], strict=True))

    @classmethod
    def scratch(cls, z):
        return [DMA((z.NB,)), DMA, DMA, DMA] + [DMA((z.NB,)) for _ in range(2 * len(cls.PHASES))]

    def peers(self):
        here = self.here
        return [here.partner()] + [here.along_x(k) for k in (1, 3)] + [here.along_y(k) for k in (1, 3)]

    def own(self, j):
        z, here = self.z, self.here
        for shard, w in zip(self.shards[:2], self.w[:2], strict=True):
            for l in range(X):
                slot = w.at[j, self.rows(here.x), pl.ds(l * LANES, LANES)]
                pltpu.make_async_copy(shard.at[:, at((l * z.NB + j) * LANES, LANES, LANES)], slot, self.local.at[j]).start()

    def own_down(self, k):
        z, here = self.z, self.here
        place = here.c * z.NB + k
        return self.shards[2].at[pl.ds(64 * k, 64), :], self.w[2].at[lax.div(place, 2), at(here.x * LANES + lax.rem(place, 2) * 64, 64), :]

    def rows(self, x):
        return at(x * (CORES * self.z.h) + self.here.c * self.z.h, self.z.h)

    def lanes(self, y):
        return at(y * LANES, LANES, LANES)

    def down(self, x, begin=0, size=64):
        return at(x * LANES + self.here.c * 64 + begin, size)

    def send(self, phase, j, w, rows, lanes, where):
        slot = self.w[w].at[j, rows, lanes]
        remote(slot, slot, self.sent[phase].at[j], self.got[phase].at[j], where).start()

    def begin_local(self):
        for j in range(self.z.NB):
            self.own(j)
        for k in range(self.z.NB):
            pltpu.make_async_copy(*self.own_down(k), self.local_d).start()

    def start_a1(self, j, first=False):
        here = self.here
        wait(self.w[0].at[j, pl.ds(0, 2 * self.z.h), :], self.local.at[j])
        for k in (1, 3):
            for w in range(2):
                self.send("a1", j, w, self.rows(here.x), slice(None) if first else self.lanes(here.y), here.along_x(k))

    def start_d1(self, j):
        for k in (1, 3):
            self.send("d1", j, 2, self.down(self.here.x), slice(None), self.here.along_x(k))

    def start_a2(self, j, first=False):
        here = self.here
        wait(self.pieces(j, 16 if first else 4), self.got["a1"].at[j])
        lanes = slice(None) if first else self.lanes(here.y)
        self.send("a2", j, 0, self.rows(lax.rem(here.x + 3, X)), lanes, here.along_x(1))
        self.send("a2", j, 1, self.rows(lax.rem(here.x + 1, X)), lanes, here.along_x(3))

    def start_d2(self, j):
        here = self.here
        wait(self.halves(j, 2), self.got["d1"].at[j])
        self.send("d2", j, 2, self.down(lax.rem(here.x + 3, X), 0, 32), slice(None), here.along_x(1))
        self.send("d2", j, 2, self.down(lax.rem(here.x + 1, X), 32, 32), slice(None), here.along_x(3))

    def start_b1(self, j):
        here = self.here
        wait(self.pieces(j, 2), self.got["a2"].at[j])
        for k in (1, 3):
            for m in range(1, X):
                for w in range(2):
                    self.send("b1", j, w, self.rows(lax.rem(here.x + m, X)), self.lanes(here.y), here.along_y(k))

    def start_b2(self, j):
        here = self.here
        wait(self.pieces(j, 12), self.got["b1"].at[j])
        for m in range(1, X):
            rows = self.rows(lax.rem(here.x + m, X))
            self.send("b2", j, 0, rows, self.lanes(lax.rem(here.y + 3, Y)), here.along_y(1))
            self.send("b2", j, 1, rows, self.lanes(lax.rem(here.y + 1, Y)), here.along_y(3))

    def start_c(self, j, first=False):
        if first:
            wait(self.pieces(j, 8), self.got["a2"].at[j])
        else:
            wait(self.pieces(j, 6), self.got["b2"].at[j])
        for w in range(2):
            for x in range(X):
                self.send("c", j, w, self.rows(x), slice(None), self.here.partner())

    def start_e(self, j):
        wait(self.halves(j, 1), self.got["d2"].at[j])
        for m in range(1, X):
            self.send("e", j, 2, self.down(lax.rem(self.here.x + m, X)), slice(None), self.here.partner())

    def pieces(self, j, n):
        rows, lanes = {2: (2, 1), 4: (4, 1), 6: (6, 1), 8: (8, 1), 12: (6, 2), 16: (8, 2)}[n]
        return self.w[0].at[j, pl.ds(0, rows * self.z.h), pl.ds(0, lanes * LANES)]

    def halves(self, j, n):
        return self.w[2].at[j, pl.ds(0, 64 * n), :]

    def begin(self):
        nb = self.z.NB
        for k in range(nb):
            src, slot = self.own_down(k)
            remote(src, slot, self.pair_sent, self.pair, self.here.partner()).start()
        if nb > 1:
            self.start_a1(1)
        self.start_a1(0, True)
        wait(self.halves(0, nb), self.local_d)
        wait(self.halves(0, nb), self.pair)
        self.start_d1(0)

    def head(self):
        nb = self.z.NB
        if nb > 1:
            self.start_a2(1)
        self.start_a2(0, True)
        if nb > 1:
            self.start_b1(1)
        self.start_d2(0)
        if nb > 1:
            self.start_d1(1)
        if nb > 2:
            self.start_a1(2)
        self.start_c(0, True)
        self.start_e(0)

    def serve_a(self, j):
        nb = self.z.NB

        @pl.when(j + 1 < nb)
        def _():
            self.start_b2(j + 1)
            self.start_d2(j + 1)

        pl.when(j + 2 < nb)(lambda: self.start_a2(j + 2))
        wait(self.w[0].at[j], self.got["c"].at[j])
        wait(self.halves(j, 3), self.got["e"].at[j])

    def serve_b(self, j):
        nb = self.z.NB

        @pl.when(j + 1 < nb)
        def _():
            self.start_c(j + 1)
            self.start_e(j + 1)

        @pl.when(j + 2 < nb)
        def _():
            self.start_b1(j + 2)
            self.start_d1(j + 2)

        pl.when(j + 3 < nb)(lambda: self.start_a1(j + 3))

    def end(self):
        wait(self.halves(0, self.z.NB), self.pair_sent)

        def drain(j, first):
            wait(self.pieces(j, 16 if first else 4), self.sent["a1"].at[j])
            wait(self.pieces(j, 8 if first else 2), self.sent["a2"].at[j])
            if not first:
                wait(self.pieces(j, 12), self.sent["b1"].at[j])
                wait(self.pieces(j, 6), self.sent["b2"].at[j])
            wait(self.halves(j, 2), self.sent["d1"].at[j])
            wait(self.halves(j, 1), self.sent["d2"].at[j])
            wait(self.w[0].at[j], self.sent["c"].at[j])
            wait(self.halves(j, 3), self.sent["e"].at[j])
            return 0

        drain(0, True)
        lax.fori_loop(1, self.z.NB, lambda j, _: drain(j, False), 0)


def normed(wide):
    scale = lax.rsqrt(jnp.mean(wide * wide, -1, keepdims=True) + 1e-6)
    return (wide * scale).astype(bf16), scale


def forward_kernel(z, x_in, sg, su, sd, h_out, wg_out, wu_out, wd_out, by_up_out, by_gate_out, act_out, a, acc, xs, act, by_up, by_gate, wg, wu, wd, x_sem, out_sem, h_sem, keep_sem, *sems):
    here = Here(z)
    fetch = Fetch(z, here, (sg.at[0], su.at[0], sd.at[0]), (wg, wu, wd), sems)
    met = meet(fetch.peers())
    fetch.begin_local()
    load = pltpu.make_async_copy(x_in, xs, x_sem)
    load.start()
    met()
    fetch.begin()
    load.wait()

    def prepare(i, _):
        rows = at(i * z.T3, z.T3)
        a[rows, :] = normed(xs[rows, :].astype(f32))[0]
        acc[rows, :] = jnp.zeros((z.T3, z.D), f32)
        return 0

    lax.fori_loop(0, z.T // z.T3, prepare, 0)
    fetch.head()
    held = ((wg, wg_out), (wu, wu_out), (wd, wd_out))
    n = z.T // z.TC

    def keep(j, i):
        slot = lax.rem(i, 2)
        return [
            pltpu.make_async_copy(v.at[slot], o.at[j, at(i * z.TC, z.TC), :], keep_sem.at[k, slot])
            for k, (v, o) in enumerate(((act, act_out), (by_up, by_up_out), (by_gate, by_gate_out)))
        ]

    def kept(j, i):
        for copy in keep(j, i):
            copy.wait()

    def block(j, _):
        fetch.serve_a(j)
        start([pltpu.make_async_copy(v.at[j], o.at[j], out_sem.at[k]) for k, (v, o) in enumerate(held)])

        def chunk(i, _):
            pl.when(i == n // 2)(lambda: fetch.serve_b(j))
            pl.when(j * n + i > 1)(lambda: kept(j, i))
            rows, slot = at(i * z.TC, z.TC), lax.rem(i, 2)
            for half in range(2):
                cols = slice(half * z.FB // 2, (half + 1) * z.FB // 2)
                gate, up = dot(a[rows, :], wg[j, :, cols]), dot(a[rows, :], wu[j, :, cols])
                sig = 1.0 / (1.0 + jnp.exp(-gate))
                silu = gate * sig
                act[slot, :, cols] = (silu * up).astype(bf16)
                by_up[slot, :, cols] = silu
                by_gate[slot, :, cols] = up * (sig + silu * (1.0 - sig))
            acc[rows, :] += dot(act[slot], wd[j])
            start(keep(j, i))
            return 0

        lax.fori_loop(0, n, chunk, 0)
        return 0

    lax.fori_loop(0, z.NB, block, 0)

    def finish(i, _):
        rows = at(i * z.T3, z.T3)
        xs[rows, :] = xs[rows, :] + acc[rows, :].astype(bf16)
        return 0

    lax.fori_loop(0, z.T // z.T3, finish, 0)
    store = pltpu.make_async_copy(xs, h_out, h_sem)
    store.start()
    for i in range(2):
        kept(z.NB - 1, n - 2 + i)
    for k, (v, _) in enumerate(held):
        wait(v, out_sem.at[k])
    fetch.end()
    store.wait()


class Reduce:
    PHASES = ("p", "x1", "x2", "y", "z", "az", "ay", "f")

    def __init__(self, z, here, units, layer_first, outs, refs):
        self.z, self.here, self.units, self.layer_first, self.outs = z, here, units, layer_first, outs
        (self.stage, self.got_p, self.got_x1, self.got_x2, self.got_y, self.got_z) = refs[:6]
        (self.send_x1, self.send_x2, self.send_y, self.send_z, self.kept_y, self.kept_z, self.fin, self.down, self.turned) = refs[6:15]
        self.got = dict(zip(self.PHASES, refs[15:31:2], strict=True))
        self.sent = dict(zip(self.PHASES, refs[16:31:2], strict=True))
        self.out_sem, self.turned_sem = refs[31:33]

    @classmethod
    def scratch(cls, z, units):
        unit, share = z.unit, z.unit[1:]
        data = [(2, X, CORES, *unit), (3, X, *unit), (2, 2, Y // 2, *share), (2, 2, *unit), (2, *unit), (units, z.Z, 3, 16, LANES)]
        data += [unit, (2, *unit), unit, share]
        return (
            [VMEM(shape, bf16) for shape in data]
            + [VMEM(share, f32), VMEM(share, f32), VMEM((units, *unit), bf16), VMEM((units, CORES, Y, z.h, LANES), bf16), VMEM((2, LANES, z.D), bf16)]
            + [DMA((units,)) for _ in range(2 * len(cls.PHASES))]
            + [DMA((2, units)), DMA((2, 2))]
        )

    def peers(self):
        here = self.here
        return (
            [here.partner(), here.along_x(1), here.along_x(3)] + [here.along_y(k) for k in range(1, Y)] + [here.along_z(k) for k in range(1, here.Z)]
        )

    def send(self, phase, u, src, dst, where):
        remote(src, dst, self.sent[phase].at[u], self.got[phase].at[u], where).start()

    def over(self, work, begin=0, end=Y):
        def one(i, _):
            work(lax.div(i, 3), lax.rem(i, 3))
            return 0

        lax.fori_loop(begin * 3, end * 3, one, 0)

    def start_p(self, u):
        here = self.here
        for x in range(X):
            self.send("p", u, self.stage.at[lax.rem(u, 2), x, 1 - here.c], self.got_p.at[lax.rem(u, 3), x], here.partner())

    def both(self, u, x, y, m):
        return self.stage[lax.rem(u, 2), x, self.here.c, y, m].astype(f32) + self.got_p[lax.rem(u, 3), x, y, m].astype(f32)

    def start_x1(self, u):
        here, half, slot = self.here, Y // 2, lax.rem(u, 2)
        wait(self.got_p.at[lax.rem(u, 3)], self.got["p"].at[u])
        far = lax.rem(here.x + 2, X)

        def work(y, m):
            self.send_x1[y, m] = self.both(u, far, y, m).astype(bf16)

        self.over(work)
        for side in range(2):
            self.send("x1", u, self.send_x1.at[pl.ds(side * half, half)], self.got_x1.at[slot, side], here.along_x((1, 3)[side]))

    def start_x2(self, u):
        here, half, slot = self.here, Y // 2, lax.rem(u, 2)
        wait(self.got_x1.at[slot], self.got["x1"].at[u])
        wait(self.got_x1.at[slot], self.sent["x1"].at[u])
        right, left = lax.rem(here.x + 1, X), lax.rem(here.x + 3, X)

        def first(y, m):
            self.send_x2[0, y, m] = (self.both(u, right, y, m) + self.got_x1[slot, 0, y, m].astype(f32)).astype(bf16)
            self.send_x2[1, y, m] = self.both(u, left, y, m).astype(bf16)

        def second(y, m):
            self.send_x2[0, y, m] = self.both(u, right, y, m).astype(bf16)
            self.send_x2[1, y, m] = (self.both(u, left, y, m) + self.got_x1[slot, 1, y - half, m].astype(f32)).astype(bf16)

        self.over(first, 0, half)
        self.over(second, half, Y)
        for side in range(2):
            self.send("x2", u, self.send_x2.at[side], self.got_x2.at[slot, side], here.along_x((1, 3)[side]))

    def start_y(self, u):
        here, slot = self.here, lax.rem(u, 2)
        wait(self.got_x2.at[slot], self.got["x2"].at[u])
        wait(self.got_x2.at[slot], self.sent["x2"].at[u])
        wait(self.got_p.at[lax.rem(u, 3)], self.sent["p"].at[u])

        def total(y, m):
            return self.both(u, here.x, y, m) + self.got_x2[slot, 0, y, m].astype(f32) + self.got_x2[slot, 1, y, m].astype(f32)

        def work(y, m):
            self.send_y[y, m] = total(y, m).astype(bf16)

        def own(_, m):
            self.kept_y[m] = total(here.y, m)

        self.over(work)
        self.over(own, 0, 1)
        for k in (1, 3, 2):
            self.send("y", u, self.send_y.at[lax.rem(here.y + k, Y)], self.got_y.at[slot, here.y], here.along_y(k))

    def start_z(self, u):
        z, here, slot = self.z, self.here, lax.rem(u, 2)
        wait(self.got_y.at[slot, pl.ds(0, Y - 1)], self.got["y"].at[u])
        wait(self.got_y.at[slot, pl.ds(0, Y - 1)], self.sent["y"].at[u])

        def work(_, m):
            total = self.kept_y[m]
            for k in range(1, Y):
                total += self.got_y[slot, lax.rem(here.y + k, Y), m].astype(f32)
            self.kept_z[m] = total
            self.send_z[m] = total.astype(bf16)

        self.over(work, 0, 1)

        def send(k, _):
            to = lax.rem(here.z + k, z.Z)
            pl.when(to < z.active)(lambda: self.send("z", u, self.send_z.at[:, at(to * 16, 16), :], self.got_z.at[u, here.z], here.along_z(k)))
            return 0

        lax.fori_loop(1, z.Z, send, 0)

    def if_active(self, yes, no):
        pl.when(self.here.z < self.z.active)(yes)
        pl.when(self.here.z >= self.z.active)(no)

    def wait_pieces(self, u, n, sem):
        if n:
            wait(self.got_z.at[u, pl.ds(0, n)], sem.at[u])

    def start_az(self, u):
        z, here = self.z, self.here

        def yes():
            self.wait_pieces(u, z.active - 1, self.sent["z"])
            self.wait_pieces(u, z.Z - 1, self.got["z"])
            rows = at(here.z * 16, 16)
            total = self.kept_z[:, rows, :]
            for k in range(1, z.Z):
                total += self.got_z[u, lax.rem(here.z + k, z.Z)].astype(f32)
            self.fin[u, here.y, :, rows, :] = total.astype(bf16)
            mine = self.fin.at[u, here.y, :, rows, :]

            def send(k, _):
                self.send("az", u, mine, mine, here.along_z(k))
                return 0

            lax.fori_loop(1, z.Z, send, 0)

        self.if_active(yes, lambda: self.wait_pieces(u, z.active, self.sent["z"]))

    def start_ay(self, u):
        z, here = self.z, self.here
        self.if_active(lambda: self.wait_pieces(u, z.active - 1, self.got["az"]), lambda: self.wait_pieces(u, z.active, self.got["az"]))
        share = self.fin.at[u, here.y]
        for k in (1, 3, 2):
            self.send("ay", u, share, share, here.along_y(k))

    def place(self, u):
        nb = self.z.NB
        return (1, u) if self.layer_first else (1 - lax.div(u + nb - 1, nb), lax.rem(u + nb - 1, nb))

    def start_f(self, u):
        z, c = self.z, self.here.c
        layer, j = self.place(u)
        wait(self.fin.at[u, pl.ds(0, Y - 1)], self.got["ay"].at[u])
        for m in range(2):
            for y in range(Y):
                out = self.outs[m].at[layer, :, at((y * z.NB + j) * LANES, LANES, LANES)]
                pltpu.make_async_copy(self.fin.at[u, y, m], out, self.out_sem.at[m, u]).start()
        self.down[u, c] = self.fin[u, :, 2]
        self.send("f", u, self.fin.at[u, :, 2], self.down.at[u, c], self.here.partner())

    def finish(self, u):
        z, c = self.z, self.here.c
        layer, j = self.place(u)
        wait(self.down.at[u, 0], self.got["f"].at[u])
        slot = lax.rem(u, 2)
        pl.when(u > 1)(lambda: self.turned_out(u - 2, "wait"))
        self.turned[slot] = self.down[u].reshape(z.D, LANES).T
        self.turned_out(u, "start")

    def turned_out(self, u, what):
        z, c = self.z, self.here.c
        layer, j = self.place(u)
        for half in range(2):
            row = 2 * j + half

            @pl.when(lax.div(row, z.NB) == c)
            def _(half=half, row=row):
                out = self.outs[2].at[layer, at(lax.rem(row, z.NB) * 64, 64), :]
                getattr(pltpu.make_async_copy(self.turned.at[lax.rem(u, 2), pl.ds(half * 64, 64), :], out, self.turned_sem.at[lax.rem(u, 2), half]), what)()

    def end(self):
        z = self.z

        def one(u, _):
            self.if_active(lambda: self.wait_pieces(u, z.Z - 1, self.sent["az"]), lambda: None)
            wait(self.fin.at[u, pl.ds(0, Y - 1)], self.sent["ay"].at[u])
            wait(self.down.at[u, 0], self.sent["f"].at[u])
            for m in range(2):
                wait(self.down.at[u, 0], self.out_sem.at[m, u])
            return 0

        lax.fori_loop(0, self.units, one, 0)
        for u in range(max(0, self.units - 2), self.units):
            self.turned_out(u, "wait")


def backward_kernel(z, first, *refs):
    T, TC, T3, NB, FB, D = z.T, z.TC, z.T3, z.NB, z.FB, z.D
    here = Here(z)
    refs = list(refs)

    def take(n):
        out, refs[:] = refs[:n], refs[n:]
        return out

    h_in, dh_in, w0, w1, w2 = take(5)
    if not first:
        left_in, by_up_in, by_gate_in, act_in = take(4)
        take(3)
    dx_out, *outs = take(4)
    spill = take(1)[0]
    left_out = take(1)[0] if first else None
    dx_buf, h_buf, a_t, dh, dh_t, wg, wu, wd, work = take(9)
    ld_sem, dh_sem, w_sem, sp_sem, s3_sem, o_sem, left_sem = take(7)
    if first:
        a = take(1)[0]
    else:
        saved, saved_sem, act_sem = take(3)
    fetch = Fetch(z, here, (w0.at[1], w1.at[1], w2.at[1]), (wg, wu, wd), take(len(Fetch.scratch(z)))) if first else None
    base = 0 if first else 1
    units = NB - 1 if first else NB + 1
    reduce = Reduce(z, here, units, first, outs, refs)
    met = meet(reduce.peers())
    whole = pltpu.make_async_copy(dh_in, dh, dh_sem)
    whole.start()

    def load_h(i):
        return pltpu.make_async_copy(h_in.at[at(i * T3, T3), :], h_buf.at[lax.rem(i, 2)], ld_sem.at[lax.rem(i, 2)])

    load_h(0).start()

    def loads(j):
        return [pltpu.make_async_copy(src.at[j], dst.at[j], w_sem.at[k, j]) for k, (src, dst) in enumerate(((w0, wg), (w1, wu), (w2, wd)))]

    TS, slots = z.TS, 3

    def load_saved(q):
        j, rows, slot = lax.div(q, T // TS), at(lax.rem(q, T // TS) * TS, TS), lax.rem(q, slots)
        return [pltpu.make_async_copy(v.at[j, rows, :], saved.at[slot, k], saved_sem.at[k, slot]) for k, v in enumerate((by_up_in, by_gate_in))]

    def load_act(j):
        return pltpu.make_async_copy(act_in.at[j], work.at[pl.ds(0, T), :], act_sem)

    if first:
        fetch.begin_local()
        met()
        fetch.begin()
    else:
        left = pltpu.make_async_copy(left_in, reduce.stage.at[0], left_sem)
        left.start()
        for j in range(NB):
            start(loads(j)[2:])
        for q in range(2):
            start(load_saved(q))
        for j in range(NB):
            start(loads(j)[:2])
    whole.wait()
    n3 = T // T3

    def prepare(i, _):
        rows = at(i * T3, T3, 128)
        pl.when(i + 1 < n3)(lambda: load_h(i + 1).start())
        load_h(i).wait()
        value = normed(h_buf[lax.rem(i, 2)].astype(f32))[0]
        if first:
            a[rows, :] = value
        a_t[:, rows] = value.T
        dh_t[:, rows] = dh[rows, :].T
        return 0

    if not first:
        met()
        left.wait()
        reduce.start_p(0)
    lax.fori_loop(0, n3, prepare, 0)
    if first:
        fetch.head()

    def product(k, rows, cols):
        return work.at[at(k * T + rows.start, rows.size), cols]

    def spills(j):
        return [pltpu.make_async_copy(work.at[pl.ds((1 + k) * T, T), :], spill.at[k, j], sp_sem.at[k]) for k in range(2)]

    def spilled(j):
        for copy in spills(j):
            copy.wait()

    def step(name, u):
        do = getattr(reduce, "start_" + name)
        if isinstance(u, int):
            if 0 <= u < units:
                do(u)
        else:
            pl.when(jnp.logical_and(u >= 0, u < units))(lambda: do(u))

    def halfway(i, n, before, after):
        if n == 1:
            before()
            after()
        else:
            pl.when(i == 0)(before)
            pl.when(i == n // 2)(after)

    def block(j, _):
        u = j + base - 1
        if first:
            fetch.serve_a(j)
        else:
            load_act(j).start()
            loads(j)[2].wait()
        pl.when(j > 0)(lambda: spilled(j - 1))

        def before():
            step("ay", u - 3)
            step("z", u - 2)

        def piece(i, _):
            halfway(i, T // TS, before, lambda: step("x1", u))
            q, rows = j * (T // TS) + i, at(i * TS, TS)
            pl.when(q + 2 < NB * (T // TS))(lambda: start(load_saved(q + 2)))
            for copy in load_saved(q):
                copy.wait()
            by_act = dot(dh[rows, :], wd[j], ((1,), (1,))).astype(bf16).astype(f32)
            slot = lax.rem(q, slots)
            product(1, rows, slice(None))[...] = (by_act * saved[slot, 1]).astype(bf16)
            product(2, rows, slice(None))[...] = (by_act * saved[slot, 0]).astype(bf16)
            return 0

        def chunk(i, _):
            halfway(i, T // TC, before, lambda: step("x1", u))
            rows = at(i * TC, TC)
            for half in range(2):
                cols = slice(half * FB // 2, (half + 1) * FB // 2)
                gate, up = dot(a[rows, :], wg[j, :, cols]), dot(a[rows, :], wu[j, :, cols])
                by_act = dot(dh[rows, :], wd[j, cols, :], ((1,), (1,))).astype(bf16).astype(f32)
                sig = 1.0 / (1.0 + jnp.exp(-gate))
                silu = gate * sig
                product(0, rows, cols)[...] = (silu * up).astype(bf16)
                product(1, rows, cols)[...] = (by_act * up * (sig + silu * (1.0 - sig))).astype(bf16)
                product(2, rows, cols)[...] = (by_act * silu).astype(bf16)
            return 0

        if first:
            lax.fori_loop(0, T // TC, chunk, 0)
        else:
            lax.fori_loop(0, T // TS, piece, 0)
            load_act(j).wait()
        start(spills(j))
        stage, slot, m = reduce.stage, lax.rem(j + base, 2), D // 2

        def rows_of(i, _):
            def before():
                if first:
                    fetch.serve_b(j)
                step("y", u - 1)
                step("az", u - 2)

            halfway(i, 2, before, lambda: step("x2", u))
            rows = at(i * m, m)
            gates = dot(a_t[rows, :], work[pl.ds(T, T), :]).astype(bf16)
            ups = dot(a_t[rows, :], work[pl.ds(2 * T, T), :]).astype(bf16)
            downs = dot(dh_t[rows, :], work[pl.ds(0, T), :]).astype(bf16)
            for y in range(Y):
                lanes = slice(y * LANES, (y + 1) * LANES)
                for x in range(X // 2):
                    for c in range(CORES):
                        part = slice((x * CORES + c) * z.h, (x * CORES + c + 1) * z.h)
                        stage[slot, i * (X // 2) + x, c, y, 0] = gates[part, lanes]
                        stage[slot, i * (X // 2) + x, c, y, 1] = ups[part, lanes]
                for x in range(X):
                    stage[slot, x, i, y, 2] = downs[y * z.h : (y + 1) * z.h, x * LANES : (x + 1) * LANES]
            return 0

        lax.fori_loop(0, 2, rows_of, 0)
        step("p", j + base)
        return 0

    lax.fori_loop(0, NB, block, 0)
    if first:
        left = pltpu.make_async_copy(reduce.stage.at[(NB - 1) % 2], left_out, left_sem)
        left.start()
    spilled(NB - 1)

    def load_3(i):
        slot, rows = lax.rem(i, 2), at(i * T3, T3)
        out = [load_h(i)]
        for k in range(2):
            for j in range(NB):
                out.append(pltpu.make_async_copy(spill.at[k, j, rows, :], work.at[at(((slot * 2 + k) * NB + j) * T3, T3), :], s3_sem.at[slot]))
        return out

    def store_3(i):
        return pltpu.make_async_copy(dx_buf.at[lax.rem(i, 2)], dx_out.at[at(i * T3, T3), :], o_sem.at[lax.rem(i, 2)])

    start(load_3(0))
    u = NB + base - 1
    todo = {
        0: [("ay", u - 3), ("z", u - 2)],
        1: [("x1", u), ("az", u - 2)],
        2: [("y", u - 1)],
        3: [("x2", u), ("ay", u - 2)],
        4: [("z", u - 1)],
        5: [("az", u - 1)],
        6: [("y", u), ("ay", u - 1)],
    }

    def complete(i, _):
        reduce.start_f(i)
        return 0

    def turn(i, _):
        reduce.finish(i)
        return 0

    def rows_back(i, _):
        slot, rows = lax.rem(i, 2), at(i * T3, T3)
        pl.when(i + 1 < n3)(lambda: start(load_3(i + 1)))
        for when, steps in todo.items():

            def now(steps=steps):
                for each in steps:
                    step(*each)

            pl.when(i == when)(now)

        @pl.when(i == 6)
        def _():
            lax.fori_loop(0, u - 1, complete, 0)

        @pl.when(i == 7)
        def _():
            lax.fori_loop(0, u - 1, turn, 0)

        if not first:

            @pl.when(i == 0)
            def _():
                for j in range(NB):
                    for copy in loads(j)[:2]:
                        copy.wait()

        load_h(i).wait()
        wait(work.at[at(slot * 2 * NB * T3, 2 * NB * T3), :], s3_sem.at[slot])
        pl.when(i > 1)(lambda: store_3(i - 2).wait())
        back = []
        for k, w in ((0, wg), (1, wu)):
            total = None
            for j in range(NB):
                part = dot(work[at(((slot * 2 + k) * NB + j) * T3, T3), :], w[j], ((1,), (1,)))
                total = part if total is None else total + part
            back.append(total.astype(bf16))
        by_a = (back[0] + back[1]).astype(f32)
        wide = h_buf[slot].astype(f32)
        square = jnp.mean(wide * wide, -1, keepdims=True) + 1e-6
        scale = lax.rsqrt(square)
        by_scale = jnp.sum(by_a * wide, -1, keepdims=True)
        by_square = by_scale * (-0.5 * scale / square) * (2.0 / D)
        dx_buf[slot] = dh[rows, :] + (by_a * scale + by_square * wide).astype(bf16)
        store_3(i).start()
        return 0

    lax.fori_loop(0, n3, rows_back, 0)
    assert n3 == 8
    for name in ("z", "az"):
        step(name, u)
    reduce.start_f(u - 1)
    step("ay", u)
    reduce.finish(u - 1)
    if u < units:
        reduce.start_f(u)
        reduce.finish(u)
    reduce.end()
    if first:
        fetch.end()
        left.wait()
    for i in range(max(0, n3 - 2), n3):
        store_3(i).wait()


def call(body, out, n_in, scratch, number, aliases=()):
    return pl.pallas_call(
        body,
        out_shape=out,
        in_specs=[pl.BlockSpec(memory_space=HBM)] * n_in,
        out_specs=[pl.BlockSpec(memory_space=HBM)] * len(out),
        scratch_shapes=scratch,
        input_output_aliases=dict(aliases),
        compiler_params=pltpu.CompilerParams(collective_id=number, has_side_effects=True, vmem_limit_bytes=66_900_000),
    )


def forward(z, x, shards):
    S = jax.ShapeDtypeStruct
    wide, tall, tokens, hidden, piece = (z.NB, z.D, z.FB), (z.NB, z.FB, z.D), (z.T, z.D), (z.NB, z.T, z.FB), (2, z.TC, z.FB)
    scratch = [VMEM(tokens, bf16), VMEM(tokens, f32), VMEM(tokens, bf16), VMEM(piece, bf16), VMEM(piece, f32), VMEM(piece, f32)]
    scratch += [VMEM(wide, bf16), VMEM(wide, bf16), VMEM(tall, bf16), DMA, DMA((3,)), DMA, DMA((3, 2))] + Fetch.scratch(z)
    out = [S(tokens, bf16), S(wide, bf16), S(wide, bf16), S(tall, bf16), S(hidden, f32), S(hidden, f32), S(hidden, bf16)]
    h, wg, wu, wd, *kept = call(functools.partial(forward_kernel, z), out, 4, scratch, 0)(x, *shards)
    return h, (wg, wu, wd), kept


def backward(z, h, dh, w, more):
    S = jax.ShapeDtypeStruct
    first = not more
    wide, tall, tokens = (z.NB, z.D, z.FB), (z.NB, z.FB, z.D), (z.T, z.D)
    units = z.NB - 1 if first else z.NB + 1
    scratch = [VMEM((2, z.T3, z.D), bf16), VMEM((2, z.T3, z.D), bf16)]
    scratch += [VMEM(tokens[::-1], bf16), VMEM(tokens, bf16), VMEM(tokens[::-1], bf16)]
    scratch += [VMEM(wide, bf16), VMEM(wide, bf16), VMEM(tall, bf16), VMEM((max(3 * z.T, 4 * z.NB * z.T3), z.FB), bf16)]
    scratch += [DMA((2,)), DMA, DMA((3, z.NB)), DMA((2,)), DMA((2,)), DMA((2,)), DMA]
    if first:
        scratch += [VMEM(tokens, bf16)] + Fetch.scratch(z)
    else:
        scratch += [VMEM((3, 2, z.TS, z.FB), f32), DMA((2, 3)), DMA]
    scratch += Reduce.scratch(z, units)
    grads = [S((2, z.h, z.F), bf16), S((2, z.h, z.F), bf16), S((2, z.F // (X * CORES), z.D), bf16)]
    out = [S(tokens, bf16), *grads, S((2, z.NB, z.T, z.FB), bf16)]
    if first:
        out.append(S((X, CORES, *z.unit), bf16))
    args = (h, dh, *w, *more)
    aliases = {} if first else {len(args) - 3 + i: 1 + i for i in range(3)}
    dx, g, u, d, _, *left = call(functools.partial(backward_kernel, z, first), out, len(args), scratch, 1 if first else 2, aliases)(*args)
    return dx, (g, u, d), left


def solution(mesh):
    def step(x, dy, *weights):
        z = Sizes(mesh, x.shape[1], x.shape[2], weights[0].shape[2])
        h, w, kept = forward(z, x[0], weights)
        dh, grads, left = backward(z, h, dy[0], weights, ())
        dx, grads, _ = backward(z, x[0], dh, w, (*left, kept[0], kept[1], kept[2], *grads))
        return dx[None], *grads

    states, cut = P(("rep", "r", "s"), None, None), P(None, "s", None)
    return jax.shard_map(
        step,
        mesh=mesh,
        in_specs=(states, states) + (cut,) * 3,
        out_specs=(states,) + (P("rep", "s", None),) * 3,
        check_vma=False,
    )
```

```python
import functools

import jax
import jax.numpy as jnp
from jax import lax
from jax.experimental import pallas as pl
from jax.experimental.pallas import tpu as pltpu
from jax.sharding import PartitionSpec as P

f32, bf16 = jnp.float32, jnp.bfloat16
MESH = pl.DeviceIdType.MESH
LANES = 128
X, CORES, Y = 4, 2, 4
HBM, VMEM, DMA = pl.ANY, pltpu.VMEM, pltpu.SemaphoreType.DMA


def dot(a, b, dims=((1,), (0,))):
    return lax.dot_general(a, b, (dims, ((), ())), preferred_element_type=f32)


def at(start, size, multiple=16):
    return pl.ds(pl.multiple_of(start, multiple) if not isinstance(start, int) else start, size)


ALL = slice(None)
LEFT, RIGHT, FAR = 3, 1, 2
SIDES = (RIGHT, LEFT)


def loop(begin, end, body):
    def one(i, carry):
        body(i)
        return carry

    lax.fori_loop(begin, end, one, 0)


def odd(i):
    return lax.rem(i, 2)


class Sizes:
    chunk, piece, rows = 1024, 512, 256

    def __init__(self, mesh, tokens, d, ff):
        self.R = mesh.shape["r"]
        self.Z = self.R // Y
        self.T, self.D, self.F = tokens, d, ff
        self.NB = ff // (X * LANES)
        self.FB = X * LANES
        self.h = d // (X * CORES)
        self.TC = min(self.chunk, tokens)
        self.T3 = min(self.rows, tokens)
        self.TS = min(self.piece, tokens)
        self.unit = (Y, 3, self.h, LANES)
        self.active = self.h // 16
        self.halves = (slice(0, self.FB // 2), slice(self.FB // 2, self.FB))
        self.early = self.NB // 2
        assert self.h % 16 == 0 and self.active <= self.Z and mesh.shape["s"] == X * CORES


class Here:
    def __init__(self, z):
        s, self.r = lax.axis_index("s"), lax.axis_index("r")
        self.x, self.c = lax.div(s, CORES), lax.rem(s, CORES)
        self.y, self.z, self.Z = lax.div(self.r, z.Z), lax.rem(self.r, z.Z), z.Z
        self.R = z.R

    def partner(self):
        return {"s": self.x * CORES + 1 - self.c}

    def along_x(self, k):
        return {"s": lax.rem(self.x + k, X) * CORES + self.c}

    def along_y(self, k):
        return {"r": lax.rem(self.y + k, Y) * self.Z + self.z}

    def right(self):
        return lax.rem(self.x + RIGHT, X)

    def left(self):
        return lax.rem(self.x + LEFT, X)

    def along_z(self, k):
        return {"r": self.y * self.Z + lax.rem(self.z + k, self.Z)}


def remote(src, dst, sent, got, where):
    return pltpu.make_async_remote_copy(src_ref=src, dst_ref=dst, send_sem=sent, recv_sem=got, device_id=where, device_id_type=MESH)


def start(copies):
    for copy in copies:
        copy.start()


def wait(ref, sem):
    pltpu.make_async_copy(ref, ref, sem).wait()


def meet(peers):
    barrier = pltpu.get_barrier_semaphore()
    for peer in peers:
        pl.semaphore_signal(barrier, inc=1, device_id=peer, device_id_type=MESH)
    return lambda: pl.semaphore_wait(barrier, len(peers))


class Fetch:
    PHASES = ("a1", "a2", "b1", "b2", "c", "d1", "d2", "e")

    def __init__(self, z, here, shards, w, sems, begin, end):
        self.z, self.here, self.shards, self.w, self.first, self.last = z, here, shards, w, begin, end
        self.local, self.local_d, self.pair, self.pair_sent = sems[:4]
        self.got = dict(zip(self.PHASES, sems[4::2], strict=True))
        self.sent = dict(zip(self.PHASES, sems[5::2], strict=True))
        self.parts = [[k for k in range(z.NB) if begin <= (c * z.NB + k) // 2 < end] for c in range(CORES)]

    @classmethod
    def scratch(cls, z):
        return [DMA((z.NB,)), DMA, DMA, DMA] + [DMA((z.NB,)) for _ in range(2 * len(cls.PHASES))]

    def peers(self):
        here = self.here
        return [here.partner()] + [here.along_x(k) for k in SIDES] + [here.along_y(k) for k in SIDES]

    def own(self, j):
        z, here = self.z, self.here
        for shard, w in zip(self.shards[:2], self.w[:2], strict=True):
            for l in range(X):
                slot = w.at[j, self.rows(here.x), pl.ds(l * LANES, LANES)]
                pltpu.make_async_copy(shard.at[:, at((l * z.NB + j) * LANES, LANES, LANES)], slot, self.local.at[j]).start()

    def each_core(self, do):
        for c in range(CORES):
            pl.when(self.here.c == c)(lambda c=c: do(self.parts[c], self.parts[1 - c]))

    def part(self, k):
        z, here = self.z, self.here
        place = here.c * z.NB + k
        return self.shards[2].at[pl.ds(64 * k, 64), :], self.w[2].at[lax.div(place, 2), at(here.x * LANES + odd(place) * 64, 64), :]

    def rows(self, x):
        return at(x * (CORES * self.z.h) + self.here.c * self.z.h, self.z.h)

    def lanes(self, y):
        return at(y * LANES, LANES, LANES)

    def down(self, x, begin=0, size=64):
        return at(x * LANES + self.here.c * 64 + begin, size)

    def send(self, phase, j, w, rows, lanes, where):
        slot = self.w[w].at[j, rows, lanes]
        remote(slot, slot, self.sent[phase].at[j], self.got[phase].at[j], where).start()

    def begin_local(self):
        for j in range(self.first, self.last):
            self.own(j)

        def do(mine, _):
            for k in mine:
                pltpu.make_async_copy(*self.part(k), self.local_d).start()

        self.each_core(do)

    def begin_pair(self):
        def do(mine, _):
            for k in mine:
                src, slot = self.part(k)
                remote(src, slot, self.pair_sent, self.pair, self.here.partner()).start()

        self.each_core(do)

    def wait_parts(self, n, sem):
        if n:
            wait(self.halves(0, n), sem)

    def end_pair(self):
        def do(mine, other):
            self.wait_parts(len(mine), self.local_d)
            self.wait_parts(len(other), self.pair)

        self.each_core(do)

    def start_a1(self, j, alone=False):
        here = self.here
        wait(self.pieces(j, 8), self.local.at[j])
        for k in SIDES:
            for w in range(2):
                self.send("a1", j, w, self.rows(here.x), ALL if alone else self.lanes(here.y), here.along_x(k))

    def start_d1(self, j):
        for k in SIDES:
            self.send("d1", j, 2, self.down(self.here.x), ALL, self.here.along_x(k))

    def start_a2(self, j, alone=False):
        here = self.here
        wait(self.pieces(j, 16 if alone else 4), self.got["a1"].at[j])
        lanes = ALL if alone else self.lanes(here.y)
        self.send("a2", j, 0, self.rows(here.left()), lanes, here.along_x(RIGHT))
        self.send("a2", j, 1, self.rows(here.right()), lanes, here.along_x(LEFT))

    def start_d2(self, j):
        here = self.here
        wait(self.halves(j, 2), self.got["d1"].at[j])
        self.send("d2", j, 2, self.down(here.left(), 0, 32), ALL, here.along_x(RIGHT))
        self.send("d2", j, 2, self.down(here.right(), 32, 32), ALL, here.along_x(LEFT))

    def start_b1(self, j):
        here = self.here
        wait(self.pieces(j, 2), self.got["a2"].at[j])
        for k in SIDES:
            for m in range(1, X):
                for w in range(2):
                    self.send("b1", j, w, self.rows(lax.rem(here.x + m, X)), self.lanes(here.y), here.along_y(k))

    def start_b2(self, j):
        here = self.here
        wait(self.pieces(j, 12), self.got["b1"].at[j])
        for m in range(1, X):
            rows = self.rows(lax.rem(here.x + m, X))
            self.send("b2", j, 0, rows, self.lanes(lax.rem(here.y + LEFT, Y)), here.along_y(RIGHT))
            self.send("b2", j, 1, rows, self.lanes(lax.rem(here.y + RIGHT, Y)), here.along_y(LEFT))

    def start_c(self, j, alone=False):
        if alone:
            wait(self.pieces(j, 8), self.got["a2"].at[j])
        else:
            wait(self.pieces(j, 6), self.got["b2"].at[j])
        for w in range(2):
            for x in range(X):
                self.send("c", j, w, self.rows(x), ALL, self.here.partner())

    def start_e(self, j):
        wait(self.halves(j, 1), self.got["d2"].at[j])
        for m in range(1, X):
            self.send("e", j, 2, self.down(lax.rem(self.here.x + m, X)), ALL, self.here.partner())

    def pieces(self, j, n):
        high = 6 if n % 6 == 0 else min(n, 8)
        return self.w[0].at[j, pl.ds(0, high * self.z.h), pl.ds(0, n // high * LANES)]

    def halves(self, j, n):
        return self.w[2].at[j, pl.ds(0, 64 * n), :]

    def ready(self, j):
        wait(self.w[0].at[j], self.got["c"].at[j])
        wait(self.halves(j, 3), self.got["e"].at[j])

    def serve_a(self, j):
        @self.if_mine(j + 1)
        def _():
            self.start_b2(j + 1)
            self.start_d2(j + 1)

        @self.if_mine(j + 2)
        def _():
            self.start_b1(j + 2)
            self.start_d1(j + 2)

        self.if_mine(j + 3)(lambda: self.start_a1(j + 3))

    def serve_b(self, j):
        @self.if_mine(j + 1)
        def _():
            self.start_c(j + 1)
            self.start_e(j + 1)

        self.if_mine(j + 3)(lambda: self.start_a2(j + 3))

    def if_mine(self, j):
        return pl.when(jnp.logical_and(j >= self.first, j < self.last))

    def end(self, alone):
        self.each_core(lambda mine, _: self.wait_parts(len(mine), self.pair_sent))

        def drain(j, alone=False):
            wait(self.pieces(j, 16 if alone else 4), self.sent["a1"].at[j])
            wait(self.pieces(j, 8 if alone else 2), self.sent["a2"].at[j])
            if not alone:
                wait(self.pieces(j, 12), self.sent["b1"].at[j])
                wait(self.pieces(j, 6), self.sent["b2"].at[j])
            wait(self.halves(j, 2), self.sent["d1"].at[j])
            wait(self.halves(j, 1), self.sent["d2"].at[j])
            wait(self.w[0].at[j], self.sent["c"].at[j])
            wait(self.halves(j, 3), self.sent["e"].at[j])

        for j in alone:
            drain(j, True)
        loop(self.first + len(alone), self.last, drain)


def normed(wide):
    scale = lax.rsqrt(jnp.mean(wide * wide, -1, keepdims=True) + 1e-6)
    return (wide * scale).astype(bf16), scale


def forward_kernel(z, *refs):
    refs = list(refs)

    def take(n):
        out, refs[:] = refs[:n], refs[n:]
        return out

    x_in, *shards = take(4)
    h_out, *w_out = take(4)
    kept_out, next_out = take(3), take(3)
    a, acc, xs = take(3)
    parts, w, w_next = take(3), take(3), take(3)
    act, by_up, by_gate = parts
    x_sem, out_sem, next_sem, h_sem, keep_sem = take(5)
    n_sems = len(Fetch.scratch(z))
    here = Here(z)
    fetch = Fetch(z, here, [v.at[0] for v in shards], w, take(n_sems), 0, z.NB)
    later = Fetch(z, here, [v.at[1] for v in shards], w_next, take(n_sems), 0, z.early)
    early = range(z.early)
    met = meet(fetch.peers())
    fetch.begin_local()
    load = pltpu.make_async_copy(x_in, xs, x_sem)
    load.start()
    met()
    fetch.begin_pair()
    fetch.start_a1(1)
    fetch.start_a1(0, True)
    fetch.end_pair()
    fetch.start_d1(0)
    fetch.start_d1(1)
    fetch.start_a1(2)
    load.wait()

    def prepare(i):
        rows = at(i * z.T3, z.T3)
        a[rows, :] = normed(xs[rows, :].astype(f32))[0]
        acc[rows, :] = jnp.zeros((z.T3, z.D), f32)

    loop(0, z.T // z.T3, prepare)
    fetch.start_a2(1)
    fetch.start_a2(0, True)
    fetch.start_b1(1)
    fetch.start_d2(0)
    fetch.start_c(0, True)
    fetch.start_e(0)
    fetch.start_a2(2)
    n = z.T // z.TC

    def keep(j, i):
        slot = odd(i)
        return [pltpu.make_async_copy(v.at[slot], o.at[j, at(i * z.TC, z.TC), :], keep_sem.at[k, slot]) for k, (v, o) in enumerate(zip(parts, kept_out, strict=True))]

    def kept(j, i):
        for copy in keep(j, i):
            copy.wait()

    def prefetch(j):
        @pl.when(j == 0)
        def _():
            later.begin_local()
            later.begin_pair()

        @pl.when(j == 1)
        def _():
            later.end_pair()
            later.start_a1(0, True)
            later.start_d1(0)

        @pl.when(j == 2)
        def _():
            later.start_a2(0, True)
            later.start_d2(0)
            for e in early[1:]:
                later.start_a1(e, True)
                later.start_d1(e)

        @pl.when(j == 3)
        def _():
            later.start_c(0, True)
            later.start_e(0)
            for e in early[1:]:
                later.start_a2(e, True)
                later.start_d2(e)

        @pl.when(j == 4)
        def _():
            for e in early[1:]:
                later.start_c(e, True)
                later.start_e(e)

    def block(j):
        fetch.serve_a(j)
        fetch.ready(j)
        start([pltpu.make_async_copy(v.at[j], o.at[j], out_sem.at[k]) for k, (v, o) in enumerate(zip(w, w_out, strict=True))])

        def chunk(i):
            @pl.when(i == n // 2)
            def _():
                fetch.serve_b(j)
                prefetch(j)

            pl.when(j * n + i > 1)(lambda: kept(j, i))
            rows, slot = at(i * z.TC, z.TC), odd(i)
            for cols in z.halves:
                gate, up = dot(a[rows, :], w[0][j, :, cols]), dot(a[rows, :], w[1][j, :, cols])
                sig = 1.0 / (1.0 + jnp.exp(-gate))
                silu = gate * sig
                act[slot, :, cols] = (silu * up).astype(bf16)
                by_up[slot, :, cols] = silu
                by_gate[slot, :, cols] = up * (sig + silu * (1.0 - sig))
            acc[rows, :] += dot(act[slot], w[2][j])
            start(keep(j, i))

        loop(0, n, chunk)

    loop(0, z.NB, block)

    def finish(i):
        rows = at(i * z.T3, z.T3)
        xs[rows, :] = xs[rows, :] + acc[rows, :].astype(bf16)

    loop(0, z.T // z.T3, finish)
    store = pltpu.make_async_copy(xs, h_out, h_sem)
    store.start()
    for e in early:
        later.ready(e)
    handed = [pltpu.make_async_copy(v, o, next_sem.at[k]) for k, (v, o) in enumerate(zip(w_next, next_out, strict=True))]
    start(handed)
    for i in range(2):
        kept(z.NB - 1, n - 2 + i)
    for k, v in enumerate(w):
        wait(v, out_sem.at[k])
    fetch.end((0,))
    later.end(early)
    store.wait()
    for copy in handed:
        copy.wait()


class Reduce:
    PHASES = ("p", "x1", "x2", "y", "z", "az", "ay", "f")

    def __init__(self, z, here, units, layer_first, outs, refs):
        self.z, self.here, self.units, self.layer_first, self.outs = z, here, units, layer_first, outs
        (self.stage, self.got_p, self.got_x1, self.got_x2, self.got_y, self.got_z, self.send_x1, self.send_x2, self.send_y, self.send_z, *refs) = refs
        (self.kept_x, self.kept_y, self.kept_z, self.fin, self.down, self.turned, self.out_sem, self.turned_sem, *refs) = refs
        self.got = dict(zip(self.PHASES, refs[::2], strict=True))
        self.sent = dict(zip(self.PHASES, refs[1::2], strict=True))

    @classmethod
    def scratch(cls, z, units):
        unit, share = z.unit, z.unit[1:]
        data = [(2, X, CORES, *unit), (3, X, *unit), (2, 2, Y // 2, *share), (2, 2, *unit), (2, *unit), (units, z.Z, 3, 16, LANES)]
        data += [unit, (2, 2, *unit), unit, share]
        wide = [(2, *unit), share, share]
        return (
            [VMEM(shape, bf16) for shape in data]
            + [VMEM(shape, f32) for shape in wide]
            + [VMEM((units, *unit), bf16), VMEM((units, CORES, Y, z.h, LANES), bf16), VMEM((2, LANES, z.D), bf16)]
            + [DMA((2, units)), DMA((2, 2))]
            + [DMA((units,)) for _ in range(2 * len(cls.PHASES))]
        )

    def peers(self):
        here = self.here
        return (
            [here.partner()] + [here.along_x(k) for k in SIDES] + [here.along_y(k) for k in range(1, Y)] + [here.along_z(k) for k in range(1, here.Z)]
        )

    def send(self, phase, u, src, dst, where):
        remote(src, dst, self.sent[phase].at[u], self.got[phase].at[u], where).start()

    def over(self, work, begin=0, end=Y):
        matrices = len(self.outs)
        loop(begin * matrices, end * matrices, lambda i: work(lax.div(i, matrices), lax.rem(i, matrices)))

    def start_p(self, u):
        here = self.here
        for x in range(X):
            self.send("p", u, self.stage.at[odd(u), x, 1 - here.c], self.got_p.at[lax.rem(u, 3), x], here.partner())

    def both(self, u, x, y, m):
        return self.stage[odd(u), x, self.here.c, y, m].astype(f32) + self.got_p[lax.rem(u, 3), x, y, m].astype(f32)

    def start_x1(self, u):
        here, half, slot = self.here, Y // 2, odd(u)
        wait(self.got_p.at[lax.rem(u, 3)], self.got["p"].at[u])
        far = lax.rem(here.x + FAR, X)

        def work(y, m):
            self.send_x1[y, m] = self.both(u, far, y, m).astype(bf16)

        self.over(work)
        for side in range(2):
            self.send("x1", u, self.send_x1.at[pl.ds(side * half, half)], self.got_x1.at[slot, side], here.along_x(SIDES[side]))

    def start_x2(self, u):
        here, half, slot = self.here, Y // 2, odd(u)
        wait(self.got_x1.at[slot], self.got["x1"].at[u])
        wait(self.got_x1.at[slot], self.sent["x1"].at[u])
        wait(self.got_p.at[lax.rem(u, 3)], self.sent["p"].at[u])
        right, left = here.right(), here.left()

        def first(y, m):
            self.send_x2[slot, 0, y, m] = (self.both(u, right, y, m) + self.got_x1[slot, 0, y, m].astype(f32)).astype(bf16)
            self.send_x2[slot, 1, y, m] = self.both(u, left, y, m).astype(bf16)
            self.kept_x[slot, y, m] = self.both(u, here.x, y, m)

        def second(y, m):
            self.send_x2[slot, 0, y, m] = self.both(u, right, y, m).astype(bf16)
            self.send_x2[slot, 1, y, m] = (self.both(u, left, y, m) + self.got_x1[slot, 1, y - half, m].astype(f32)).astype(bf16)
            self.kept_x[slot, y, m] = self.both(u, here.x, y, m)

        self.over(first, 0, half)
        self.over(second, half, Y)
        for side in range(2):
            self.send("x2", u, self.send_x2.at[slot, side], self.got_x2.at[slot, side], here.along_x(SIDES[side]))

    def start_y(self, u):
        here, slot = self.here, odd(u)
        wait(self.got_x2.at[slot], self.got["x2"].at[u])
        wait(self.got_x2.at[slot], self.sent["x2"].at[u])

        def total(y, m):
            return self.kept_x[slot, y, m] + self.got_x2[slot, 0, y, m].astype(f32) + self.got_x2[slot, 1, y, m].astype(f32)

        def work(y, m):
            self.send_y[y, m] = total(y, m).astype(bf16)

        def own(_, m):
            self.kept_y[m] = total(here.y, m)

        self.over(work)
        self.over(own, 0, 1)
        for k in (*SIDES, FAR):
            self.send("y", u, self.send_y.at[lax.rem(here.y + k, Y)], self.got_y.at[slot, here.y], here.along_y(k))

    def start_z(self, u):
        z, here, slot = self.z, self.here, odd(u)
        wait(self.got_y.at[slot, pl.ds(0, Y - 1)], self.got["y"].at[u])
        wait(self.got_y.at[slot, pl.ds(0, Y - 1)], self.sent["y"].at[u])

        def work(_, m):
            total = self.kept_y[m]
            for k in range(1, Y):
                total += self.got_y[slot, lax.rem(here.y + k, Y), m].astype(f32)
            self.kept_z[m] = total
            self.send_z[m] = total.astype(bf16)

        self.over(work, 0, 1)

        def send(k):
            to = lax.rem(here.z + k, z.Z)
            pl.when(to < z.active)(lambda: self.send("z", u, self.send_z.at[:, at(to * 16, 16), :], self.got_z.at[u, here.z], here.along_z(k)))

        loop(1, z.Z, send)

    def if_active(self, yes, no):
        pl.when(self.here.z < self.z.active)(yes)
        pl.when(self.here.z >= self.z.active)(no)

    def wait_pieces(self, u, n, sem):
        if n:
            wait(self.got_z.at[u, pl.ds(0, n)], sem.at[u])

    def start_az(self, u):
        z, here = self.z, self.here

        def yes():
            self.wait_pieces(u, z.active - 1, self.sent["z"])
            self.wait_pieces(u, z.Z - 1, self.got["z"])
            rows = at(here.z * 16, 16)
            total = self.kept_z[:, rows, :]
            for k in range(1, z.Z):
                total += self.got_z[u, lax.rem(here.z + k, z.Z)].astype(f32)
            self.fin[u, here.y, :, rows, :] = total.astype(bf16)
            mine = self.fin.at[u, here.y, :, rows, :]

            loop(1, z.Z, lambda k: self.send("az", u, mine, mine, here.along_z(k)))

        self.if_active(yes, lambda: self.wait_pieces(u, z.active, self.sent["z"]))

    def start_ay(self, u):
        z, here = self.z, self.here
        self.if_active(lambda: self.wait_pieces(u, z.active - 1, self.got["az"]), lambda: self.wait_pieces(u, z.active, self.got["az"]))
        share = self.fin.at[u, here.y]
        for k in (*SIDES, FAR):
            self.send("ay", u, share, share, here.along_y(k))

    def place(self, u):
        nb = self.z.NB
        return (1, u) if self.layer_first else (1 - lax.div(u + nb - 1, nb), lax.rem(u + nb - 1, nb))

    def start_f(self, u):
        z, c = self.z, self.here.c
        layer, j = self.place(u)
        wait(self.fin.at[u, pl.ds(0, Y - 1)], self.got["ay"].at[u])
        for m in range(2):
            for y in range(Y):
                out = self.outs[m].at[layer, :, at((y * z.NB + j) * LANES, LANES, LANES)]
                pltpu.make_async_copy(self.fin.at[u, y, m], out, self.out_sem.at[m, u]).start()
        self.down[u, c] = self.fin[u, :, 2]
        self.send("f", u, self.fin.at[u, :, 2], self.down.at[u, c], self.here.partner())

    def finish(self, u):
        z, c = self.z, self.here.c
        layer, j = self.place(u)
        wait(self.down.at[u, 0], self.got["f"].at[u])
        slot = odd(u)
        pl.when(u > 1)(lambda: self.turned_out(u - 2, "wait"))
        self.turned[slot] = self.down[u].reshape(z.D, LANES).T
        self.turned_out(u, "start")

    def turned_out(self, u, what):
        z, c = self.z, self.here.c
        layer, j = self.place(u)
        for half in range(2):
            row = 2 * j + half

            @pl.when(lax.div(row, z.NB) == c)
            def _(half=half, row=row):
                out = self.outs[2].at[layer, at(lax.rem(row, z.NB) * 64, 64), :]
                getattr(pltpu.make_async_copy(self.turned.at[odd(u), pl.ds(half * 64, 64), :], out, self.turned_sem.at[odd(u), half]), what)()

    def end(self):
        z = self.z

        def one(u):
            self.if_active(lambda: self.wait_pieces(u, z.Z - 1, self.sent["az"]), lambda: None)
            wait(self.fin.at[u, pl.ds(0, Y - 1)], self.sent["ay"].at[u])
            wait(self.down.at[u, 0], self.sent["f"].at[u])
            for m in range(2):
                wait(self.down.at[u, 0], self.out_sem.at[m, u])

        loop(0, self.units, one)
        for u in range(max(0, self.units - 2), self.units):
            self.turned_out(u, "wait")


def backward_kernel(z, first, *refs):
    T, TC, T3, NB, FB, D = z.T, z.TC, z.T3, z.NB, z.FB, z.D
    here = Here(z)
    refs = list(refs)

    def take(n):
        out, refs[:] = refs[:n], refs[n:]
        return out

    h_in, dh_in, w0, w1, w2 = take(5)
    if first:
        early_in = take(3)
    else:
        left_in, by_up_in, by_gate_in, act_in = take(4)
        take(3)
    dx_out, *outs = take(4)
    spill = take(1)[0]
    if first:
        left_out = take(1)[0]
    dx_buf, h_buf, a_t, dh, dh_t, wg, wu, wd, work = take(9)
    ld_sem, dh_sem, w_sem, sp_sem, s3_sem, o_sem, left_sem = take(7)
    if first:
        a = take(1)[0]
    else:
        saved, saved_sem, act_sem = take(3)
    if first:
        fetch = Fetch(z, here, (w0.at[1], w1.at[1], w2.at[1]), (wg, wu, wd), take(len(Fetch.scratch(z))), z.early, NB)
        w0, w1, w2 = early_in
    base = 0 if first else 1
    units = NB - 1 if first else NB + 1
    reduce = Reduce(z, here, units, first, outs, refs)
    met = meet(reduce.peers())
    whole = pltpu.make_async_copy(dh_in, dh, dh_sem)
    whole.start()

    def load_h(i):
        return pltpu.make_async_copy(h_in.at[at(i * T3, T3), :], h_buf.at[odd(i)], ld_sem.at[odd(i)])

    load_h(0).start()

    def loads(j):
        return [pltpu.make_async_copy(src.at[j], dst.at[j], w_sem.at[k, j]) for k, (src, dst) in enumerate(((w0, wg), (w1, wu), (w2, wd)))]

    TS, slots = z.TS, 3

    def load_saved(q):
        j, rows, slot = lax.div(q, T // TS), at(lax.rem(q, T // TS) * TS, TS), lax.rem(q, slots)
        return [pltpu.make_async_copy(v.at[j, rows, :], saved.at[slot, k], saved_sem.at[k, slot]) for k, v in enumerate((by_up_in, by_gate_in))]

    def load_act(j):
        return pltpu.make_async_copy(act_in.at[j], work.at[pl.ds(0, T), :], act_sem)

    if first:
        for j in range(z.early):
            start(loads(j))
        fetch.begin_local()
        met()
        fetch.begin_pair()
        fetch.start_a1(z.early)
    else:
        left = pltpu.make_async_copy(left_in, reduce.stage.at[0], left_sem)
        left.start()
        for j in range(NB):
            start(loads(j)[2:])
        for q in range(2):
            start(load_saved(q))
        for j in range(NB):
            start(loads(j)[:2])
    whole.wait()
    n3 = T // T3

    def prepare(i):
        rows = at(i * T3, T3, LANES)
        pl.when(i + 1 < n3)(lambda: load_h(i + 1).start())
        load_h(i).wait()
        value = normed(h_buf[odd(i)].astype(f32))[0]
        if first:
            a[rows, :] = value
        a_t[:, rows] = value.T
        dh_t[:, rows] = dh[rows, :].T

    if not first:
        met()
        left.wait()
        reduce.start_p(0)
    loop(0, n3, prepare)
    if first:
        fetch.end_pair()
        fetch.start_a2(z.early)

    def product(k, rows, cols):
        return work.at[at(k * T + rows.start, rows.size), cols]

    def spills(j):
        return [pltpu.make_async_copy(work.at[pl.ds((1 + k) * T, T), :], spill.at[k, j], sp_sem.at[k]) for k in range(2)]

    def spilled(j):
        for copy in spills(j):
            copy.wait()

    def step(name, u):
        do = getattr(reduce, "start_" + name)
        if isinstance(u, int):
            if 0 <= u < units:
                do(u)
        else:
            pl.when(jnp.logical_and(u >= 0, u < units))(lambda: do(u))

    def halfway(i, n, before, after):
        if n == 1:
            before()
            after()
        else:
            pl.when(i == 0)(before)
            pl.when(i == n // 2)(after)

    def loaded(j):
        for copy in loads(j):
            copy.wait()

    def block(j):
        u = j + base - 1
        if first:
            fetch.serve_a(j)
            pl.when(j < z.early)(lambda: loaded(j))
            pl.when(j >= z.early)(lambda: fetch.ready(j))
        else:
            load_act(j).start()
            loads(j)[2].wait()
        pl.when(j > 0)(lambda: spilled(j - 1))

        def at_0():
            if first:
                step("ay", u - 3)
                step("z", u - 2)
            else:
                step("x2", u - 1)
                step("ay", u - 4)

        def at_1():
            if first:
                step("x1", u)
            else:
                step("z", u - 3)

        def at_2():
            if first:
                fetch.serve_b(j)
                step("y", u - 1)
                step("az", u - 2)
            else:
                step("y", u - 2)
                step("x1", u)

        def at_3():
            if first:
                step("x2", u)
            else:
                step("az", u - 3)

        def piece(i):
            halfway(i, T // TS, at_0, at_1)
            q, rows = j * (T // TS) + i, at(i * TS, TS)
            pl.when(q + 2 < NB * (T // TS))(lambda: start(load_saved(q + 2)))
            for copy in load_saved(q):
                copy.wait()
            by_act = dot(dh[rows, :], wd[j], ((1,), (1,))).astype(bf16).astype(f32)
            slot = lax.rem(q, slots)
            product(1, rows, ALL)[...] = (by_act * saved[slot, 1]).astype(bf16)
            product(2, rows, ALL)[...] = (by_act * saved[slot, 0]).astype(bf16)

        def chunk(i):
            halfway(i, T // TC, at_0, at_1)
            rows = at(i * TC, TC)
            for cols in z.halves:
                gate, up = dot(a[rows, :], wg[j, :, cols]), dot(a[rows, :], wu[j, :, cols])
                by_act = dot(dh[rows, :], wd[j, cols, :], ((1,), (1,))).astype(bf16).astype(f32)
                sig = 1.0 / (1.0 + jnp.exp(-gate))
                silu = gate * sig
                product(0, rows, cols)[...] = (silu * up).astype(bf16)
                product(1, rows, cols)[...] = (by_act * up * (sig + silu * (1.0 - sig))).astype(bf16)
                product(2, rows, cols)[...] = (by_act * silu).astype(bf16)

        if first:
            loop(0, T // TC, chunk)
        else:
            loop(0, T // TS, piece)
            load_act(j).wait()
        start(spills(j))
        stage, slot, m = reduce.stage, odd(j + base), D // 2

        def rows_of(i):
            halfway(i, 2, at_2, at_3)
            rows = at(i * m, m)
            gates = dot(a_t[rows, :], work[pl.ds(T, T), :]).astype(bf16)
            ups = dot(a_t[rows, :], work[pl.ds(2 * T, T), :]).astype(bf16)
            downs = dot(dh_t[rows, :], work[pl.ds(0, T), :]).astype(bf16)
            for y in range(Y):
                lanes = slice(y * LANES, (y + 1) * LANES)
                for x in range(X // 2):
                    for c in range(CORES):
                        part = slice((x * CORES + c) * z.h, (x * CORES + c + 1) * z.h)
                        stage[slot, i * (X // 2) + x, c, y, 0] = gates[part, lanes]
                        stage[slot, i * (X // 2) + x, c, y, 1] = ups[part, lanes]
                for x in range(X):
                    stage[slot, x, i, y, 2] = downs[y * z.h : (y + 1) * z.h, x * LANES : (x + 1) * LANES]

        loop(0, 2, rows_of)
        step("p", j + base)

    loop(0, NB, block)
    if first:
        left = pltpu.make_async_copy(reduce.stage.at[(NB - 1) % 2], left_out, left_sem)
        left.start()
    spilled(NB - 1)

    def load_3(i):
        slot, rows = odd(i), at(i * T3, T3)
        out = [load_h(i)]
        for k in range(2):
            for j in range(NB):
                out.append(pltpu.make_async_copy(spill.at[k, j, rows, :], work.at[at(((slot * 2 + k) * NB + j) * T3, T3), :], s3_sem.at[slot]))
        return out

    def store_3(i):
        return pltpu.make_async_copy(dx_buf.at[odd(i)], dx_out.at[at(i * T3, T3), :], o_sem.at[odd(i)])

    start(load_3(0))
    u = NB + base - 1
    if first:
        todo = [
            [("ay", u - 3), ("z", u - 2)],
            [("az", u - 2)],
            [("y", u - 1)],
            [("ay", u - 2)],
            [("z", u - 1)],
            [("az", u - 1)],
            [("ay", u - 1)],
        ]
        rest = []
    else:
        todo = [
            [("x2", u - 1), ("ay", u - 4)],
            [("z", u - 3), ("y", u - 2), ("x1", u)],
            [],
            [("az", u - 3)],
            [("z", u - 2)],
            [("x2", u), ("y", u - 1), ("ay", u - 3)],
            [("az", u - 2)],
        ]
        rest = [("ay", u - 2), ("z", u - 1), ("y", u), ("az", u - 1), ("z", u), ("ay", u - 1), ("az", u), ("ay", u)]

    done = u - 1 if first else u - 3

    def rows_back(i):
        slot, rows = odd(i), at(i * T3, T3)
        pl.when(i + 1 < n3)(lambda: start(load_3(i + 1)))
        for when, steps in enumerate(todo):

            def now(steps=steps):
                for each in steps:
                    step(*each)

            pl.when(i == when)(now)

        @pl.when(i == n3 - 2)
        def _():
            loop(0, done, reduce.start_f)

        @pl.when(i == n3 - 1)
        def _():
            loop(0, done, reduce.finish)

        if not first:

            @pl.when(i == 0)
            def _():
                for j in range(NB):
                    for copy in loads(j)[:2]:
                        copy.wait()

        load_h(i).wait()
        wait(work.at[at(slot * 2 * NB * T3, 2 * NB * T3), :], s3_sem.at[slot])
        pl.when(i > 1)(lambda: store_3(i - 2).wait())
        back = []
        for k, w in ((0, wg), (1, wu)):
            total = None
            for j in range(NB):
                part = dot(work[at(((slot * 2 + k) * NB + j) * T3, T3), :], w[j], ((1,), (1,)))
                total = part if total is None else total + part
            back.append(total.astype(bf16))
        by_a = (back[0] + back[1]).astype(f32)
        wide = h_buf[slot].astype(f32)
        square = jnp.mean(wide * wide, -1, keepdims=True) + 1e-6
        scale = lax.rsqrt(square)
        by_scale = jnp.sum(by_a * wide, -1, keepdims=True)
        by_square = by_scale * (-0.5 * scale / square) * (2.0 / D)
        dx_buf[slot] = dh[rows, :] + (by_a * scale + by_square * wide).astype(bf16)
        store_3(i).start()

    loop(0, n3, rows_back)
    assert n3 == 8
    for each in rest:
        step(*each)
    for v in range(max(done, 0), units):
        reduce.start_f(v)
    for v in range(max(done, 0), units):
        reduce.finish(v)
    reduce.end()
    if first:
        fetch.end(())
        left.wait()
    for i in range(max(0, n3 - 2), n3):
        store_3(i).wait()


def call(body, out, n_in, scratch, number, aliases=()):
    return pl.pallas_call(
        body,
        out_shape=out,
        in_specs=[pl.BlockSpec(memory_space=HBM)] * n_in,
        out_specs=[pl.BlockSpec(memory_space=HBM)] * len(out),
        scratch_shapes=scratch,
        input_output_aliases=dict(aliases),
        compiler_params=pltpu.CompilerParams(collective_id=number, has_side_effects=True, vmem_limit_bytes=66_900_000),
    )


def forward(z, x, shards):
    S = jax.ShapeDtypeStruct
    wide, tall, tokens, hidden, piece = (z.NB, z.D, z.FB), (z.NB, z.FB, z.D), (z.T, z.D), (z.NB, z.T, z.FB), (2, z.TC, z.FB)
    scratch = [VMEM(tokens, bf16), VMEM(tokens, f32), VMEM(tokens, bf16), VMEM(piece, bf16), VMEM(piece, f32), VMEM(piece, f32)]
    early = [(z.early, *shape[1:]) for shape in (wide, wide, tall)]
    scratch += [VMEM(shape, bf16) for shape in (wide, wide, tall, *early)]
    scratch += [DMA, DMA((3,)), DMA((3,)), DMA, DMA((3, 2))] + Fetch.scratch(z) + Fetch.scratch(z)
    out = [S(tokens, bf16), S(wide, bf16), S(wide, bf16), S(tall, bf16), S(hidden, bf16), S(hidden, f32), S(hidden, f32)]
    out += [S(shape, bf16) for shape in early]
    h, *out = call(functools.partial(forward_kernel, z), out, 4, scratch, 0)(x, *shards)
    return h, out[:3], out[3:6], out[6:]


def backward(z, h, dh, w, more, first):
    S = jax.ShapeDtypeStruct
    wide, tall, tokens = (z.NB, z.D, z.FB), (z.NB, z.FB, z.D), (z.T, z.D)
    units = z.NB - 1 if first else z.NB + 1
    scratch = [VMEM((2, z.T3, z.D), bf16), VMEM((2, z.T3, z.D), bf16)]
    scratch += [VMEM(tokens[::-1], bf16), VMEM(tokens, bf16), VMEM(tokens[::-1], bf16)]
    scratch += [VMEM(wide, bf16), VMEM(wide, bf16), VMEM(tall, bf16), VMEM((max(3 * z.T, 4 * z.NB * z.T3), z.FB), bf16)]
    scratch += [DMA((2,)), DMA, DMA((3, z.NB)), DMA((2,)), DMA((2,)), DMA((2,)), DMA]
    if first:
        scratch += [VMEM(tokens, bf16)] + Fetch.scratch(z)
    else:
        scratch += [VMEM((3, 2, z.TS, z.FB), f32), DMA((2, 3)), DMA]
    scratch += Reduce.scratch(z, units)
    grads = [S((2, z.h, z.F), bf16), S((2, z.h, z.F), bf16), S((2, z.F // (X * CORES), z.D), bf16)]
    out = [S(tokens, bf16), *grads, S((2, z.NB, z.T, z.FB), bf16)]
    if first:
        out.append(S((X, CORES, *z.unit), bf16))
    args = (h, dh, *w, *more)
    aliases = {} if first else {len(args) - 3 + i: 1 + i for i in range(3)}
    dx, g, u, d, _, *left = call(functools.partial(backward_kernel, z, first), out, len(args), scratch, 1 if first else 2, aliases)(*args)
    return dx, (g, u, d), left


def solution(mesh):
    def step(x, dy, *weights):
        z = Sizes(mesh, x.shape[1], x.shape[2], weights[0].shape[2])
        h, w, (act, by_up, by_gate), early = forward(z, x[0], weights)
        dh, grads, left = backward(z, h, dy[0], weights, early, True)
        dx, grads, _ = backward(z, x[0], dh, w, (*left, by_up, by_gate, act, *grads), False)
        return dx[None], *grads

    states, cut = P(("rep", "r", "s"), None, None), P(None, "s", None)
    return jax.shard_map(
        step,
        mesh=mesh,
        in_specs=(states, states) + (cut,) * 3,
        out_specs=(states,) + (P("rep", "s", None),) * 3,
        check_vma=False,
    )
```

```python
import functools

import jax
import jax.numpy as jnp
from jax import lax
from jax.experimental import pallas as pl
from jax.experimental.pallas import tpu as pltpu
from jax.sharding import PartitionSpec as P

f32, bf16 = jnp.float32, jnp.bfloat16
MESH = pl.DeviceIdType.MESH
LANES = 128
X, CORES, Y = 4, 2, 4
HBM, VMEM, DMA = pl.ANY, pltpu.VMEM, pltpu.SemaphoreType.DMA


def dot(a, b, dims=((1,), (0,))):
    return lax.dot_general(a, b, (dims, ((), ())), preferred_element_type=f32)


def at(start, size, multiple=16):
    return pl.ds(pl.multiple_of(start, multiple) if not isinstance(start, int) else start, size)


ALL = slice(None)
LEFT, RIGHT, FAR = 3, 1, 2
SIDES = (RIGHT, LEFT)


def loop(begin, end, body):
    def one(i, carry):
        body(i)
        return carry

    lax.fori_loop(begin, end, one, 0)


def odd(i):
    return lax.rem(i, 2)


class Sizes:
    chunk, piece, rows = 1024, 512, 256

    def __init__(self, mesh, tokens, d, ff):
        self.R = mesh.shape["r"]
        self.Z = self.R // Y
        self.T, self.D, self.F = tokens, d, ff
        self.NB = ff // (X * LANES)
        self.FB = X * LANES
        self.h = d // (X * CORES)
        self.TC = min(self.chunk, tokens)
        self.T3 = min(self.rows, tokens)
        self.TS = min(self.piece, tokens)
        self.unit = (Y, 3, self.h, LANES)
        self.active = self.h // 16
        self.halves = (slice(0, self.FB // 2), slice(self.FB // 2, self.FB))
        self.early = self.NB // 2
        assert self.h % 16 == 0 and self.active <= self.Z and mesh.shape["s"] == X * CORES


class Here:
    def __init__(self, z):
        s, self.r = lax.axis_index("s"), lax.axis_index("r")
        self.x, self.c = lax.div(s, CORES), lax.rem(s, CORES)
        self.y, self.z, self.Z = lax.div(self.r, z.Z), lax.rem(self.r, z.Z), z.Z
        self.R = z.R

    def partner(self):
        return {"s": self.x * CORES + 1 - self.c}

    def along_x(self, k):
        return {"s": lax.rem(self.x + k, X) * CORES + self.c}

    def along_y(self, k):
        return {"r": lax.rem(self.y + k, Y) * self.Z + self.z}

    def right(self):
        return lax.rem(self.x + RIGHT, X)

    def left(self):
        return lax.rem(self.x + LEFT, X)

    def along_z(self, k):
        return {"r": self.y * self.Z + lax.rem(self.z + k, self.Z)}


def remote(src, dst, sent, got, where):
    return pltpu.make_async_remote_copy(src_ref=src, dst_ref=dst, send_sem=sent, recv_sem=got, device_id=where, device_id_type=MESH)


def start(copies):
    for copy in copies:
        copy.start()


def wait(ref, sem):
    pltpu.make_async_copy(ref, ref, sem).wait()


def meet(peers):
    barrier = pltpu.get_barrier_semaphore()
    for peer in peers:
        pl.semaphore_signal(barrier, inc=1, device_id=peer, device_id_type=MESH)
    return lambda: pl.semaphore_wait(barrier, len(peers))


FETCHES = (
    "a10,a11,a12,d10,a21,a20",
    "a22,b11,d20,d11,c0,b12,e0",
    "a13,d12,b21,d21,a23,d13",
    "e1,c1,a14,b13,d22,d14",
    "a24,d23,b22,La11,e2",
    "c2,d24,Ld10,Ld11,b23,b14",
    "e3",
    "c3,b24,La10",
    "e4,La21,c4,Ld21",
    "Ld20",
    "La20,Lc1,Le1",
    "Le0,Lc0",
)


class Fetch:
    PHASES = ("a1", "a2", "b1", "b2", "c", "d1", "d2", "e")

    def __init__(self, z, here, shards, w, sems, begin, end):
        self.z, self.here, self.shards, self.w, self.first, self.last = z, here, shards, w, begin, end
        self.local, self.local_d, self.pair, self.pair_sent = sems[:4]
        self.got = dict(zip(self.PHASES, sems[4::2], strict=True))
        self.sent = dict(zip(self.PHASES, sems[5::2], strict=True))
        self.parts = [[k for k in range(z.NB) if begin <= (c * z.NB + k) // 2 < end] for c in range(CORES)]

    @classmethod
    def scratch(cls, z):
        return [DMA((z.NB,)), DMA, DMA, DMA] + [DMA((z.NB,)) for _ in range(2 * len(cls.PHASES))]

    def peers(self):
        here = self.here
        return [here.partner()] + [here.along_x(k) for k in SIDES] + [here.along_y(k) for k in SIDES]

    def own(self, j):
        z, here = self.z, self.here
        for shard, w in zip(self.shards[:2], self.w[:2], strict=True):
            for l in range(X):
                slot = w.at[j, self.rows(here.x), pl.ds(l * LANES, LANES)]
                pltpu.make_async_copy(shard.at[:, at((l * z.NB + j) * LANES, LANES, LANES)], slot, self.local.at[j]).start()

    def each_core(self, do):
        for c in range(CORES):
            pl.when(self.here.c == c)(lambda c=c: do(self.parts[c], self.parts[1 - c]))

    def part(self, k):
        z, here = self.z, self.here
        place = here.c * z.NB + k
        return self.shards[2].at[pl.ds(64 * k, 64), :], self.w[2].at[lax.div(place, 2), at(here.x * LANES + odd(place) * 64, 64), :]

    def rows(self, x):
        return at(x * (CORES * self.z.h) + self.here.c * self.z.h, self.z.h)

    def lanes(self, y):
        return at(y * LANES, LANES, LANES)

    def down(self, x, begin=0, size=64):
        return at(x * LANES + self.here.c * 64 + begin, size)

    def send(self, phase, j, w, rows, lanes, where):
        slot = self.w[w].at[j, rows, lanes]
        remote(slot, slot, self.sent[phase].at[j], self.got[phase].at[j], where).start()

    def begin_local(self):
        for j in range(self.first, self.last):
            self.own(j)

        def do(mine, _):
            for k in mine:
                pltpu.make_async_copy(*self.part(k), self.local_d).start()

        self.each_core(do)

    def begin_pair(self):
        def do(mine, _):
            for k in mine:
                src, slot = self.part(k)
                remote(src, slot, self.pair_sent, self.pair, self.here.partner()).start()

        self.each_core(do)

    def wait_parts(self, n, sem):
        if n:
            wait(self.halves(0, n), sem)

    def end_pair(self):
        def do(mine, other):
            self.wait_parts(len(mine), self.local_d)
            self.wait_parts(len(other), self.pair)

        self.each_core(do)

    def start_a1(self, j, alone=False):
        here = self.here
        wait(self.pieces(j, 8), self.local.at[j])
        for k in SIDES:
            for w in range(2):
                self.send("a1", j, w, self.rows(here.x), ALL if alone else self.lanes(here.y), here.along_x(k))

    def start_d1(self, j):
        for k in SIDES:
            self.send("d1", j, 2, self.down(self.here.x), ALL, self.here.along_x(k))

    def start_a2(self, j, alone=False):
        here = self.here
        wait(self.pieces(j, 16 if alone else 4), self.got["a1"].at[j])
        lanes = ALL if alone else self.lanes(here.y)
        self.send("a2", j, 0, self.rows(here.left()), lanes, here.along_x(RIGHT))
        self.send("a2", j, 1, self.rows(here.right()), lanes, here.along_x(LEFT))

    def start_d2(self, j):
        here = self.here
        wait(self.halves(j, 2), self.got["d1"].at[j])
        self.send("d2", j, 2, self.down(here.left(), 0, 32), ALL, here.along_x(RIGHT))
        self.send("d2", j, 2, self.down(here.right(), 32, 32), ALL, here.along_x(LEFT))

    def start_b1(self, j):
        here = self.here
        wait(self.pieces(j, 2), self.got["a2"].at[j])
        for k in SIDES:
            for m in range(1, X):
                for w in range(2):
                    self.send("b1", j, w, self.rows(lax.rem(here.x + m, X)), self.lanes(here.y), here.along_y(k))

    def start_b2(self, j):
        here = self.here
        wait(self.pieces(j, 12), self.got["b1"].at[j])
        for m in range(1, X):
            rows = self.rows(lax.rem(here.x + m, X))
            self.send("b2", j, 0, rows, self.lanes(lax.rem(here.y + LEFT, Y)), here.along_y(RIGHT))
            self.send("b2", j, 1, rows, self.lanes(lax.rem(here.y + RIGHT, Y)), here.along_y(LEFT))

    def start_c(self, j, alone=False):
        if alone:
            wait(self.pieces(j, 8), self.got["a2"].at[j])
        else:
            wait(self.pieces(j, 6), self.got["b2"].at[j])
        for w in range(2):
            for x in range(X):
                self.send("c", j, w, self.rows(x), ALL, self.here.partner())

    def start_e(self, j):
        wait(self.halves(j, 1), self.got["d2"].at[j])
        for m in range(1, X):
            self.send("e", j, 2, self.down(lax.rem(self.here.x + m, X)), ALL, self.here.partner())

    def pieces(self, j, n):
        high = 6 if n % 6 == 0 else min(n, 8)
        return self.w[0].at[j, pl.ds(0, high * self.z.h), pl.ds(0, n // high * LANES)]

    def halves(self, j, n):
        return self.w[2].at[j, pl.ds(0, 64 * n), :]

    def ready(self, j):
        wait(self.w[0].at[j], self.got["c"].at[j])
        wait(self.halves(j, 3), self.got["e"].at[j])

    def serve_a(self, j):
        @self.if_mine(j + 1)
        def _():
            self.start_b2(j + 1)
            self.start_d2(j + 1)

        @self.if_mine(j + 2)
        def _():
            self.start_b1(j + 2)
            self.start_d1(j + 2)

        self.if_mine(j + 3)(lambda: self.start_a1(j + 3))

    def serve_b(self, j):
        @self.if_mine(j + 1)
        def _():
            self.start_c(j + 1)
            self.start_e(j + 1)

        self.if_mine(j + 3)(lambda: self.start_a2(j + 3))

    def if_mine(self, j):
        return pl.when(jnp.logical_and(j >= self.first, j < self.last))

    def end(self, alone):
        self.each_core(lambda mine, _: self.wait_parts(len(mine), self.pair_sent))

        def drain(j, alone=False):
            wait(self.pieces(j, 16 if alone else 4), self.sent["a1"].at[j])
            wait(self.pieces(j, 8 if alone else 2), self.sent["a2"].at[j])
            if not alone:
                wait(self.pieces(j, 12), self.sent["b1"].at[j])
                wait(self.pieces(j, 6), self.sent["b2"].at[j])
            wait(self.halves(j, 2), self.sent["d1"].at[j])
            wait(self.halves(j, 1), self.sent["d2"].at[j])
            wait(self.w[0].at[j], self.sent["c"].at[j])
            wait(self.halves(j, 3), self.sent["e"].at[j])

        for j in alone:
            drain(j, True)
        loop(self.first + len(alone), self.last, drain)


def normed(wide):
    scale = lax.rsqrt(jnp.mean(wide * wide, -1, keepdims=True) + 1e-6)
    return (wide * scale).astype(bf16), scale


def forward_kernel(z, *refs):
    refs = list(refs)

    def take(n):
        out, refs[:] = refs[:n], refs[n:]
        return out

    x_in, *shards = take(4)
    h_out, *w_out = take(4)
    kept_out, next_out = take(3), take(3)
    a, acc, xs = take(3)
    parts, w, w_next = take(3), take(3), take(3)
    act, by_up, by_gate = parts
    x_sem, out_sem, next_sem, h_sem, keep_sem = take(5)
    n_sems = len(Fetch.scratch(z))
    here = Here(z)
    fetch = Fetch(z, here, [v.at[0] for v in shards], w, take(n_sems), 0, z.NB)
    later = Fetch(z, here, [v.at[1] for v in shards], w_next, take(n_sems), 0, z.early)
    early = range(z.early)
    met = meet(fetch.peers())
    fetch.begin_local()
    load = pltpu.make_async_copy(x_in, xs, x_sem)
    load.start()
    met()
    fetch.begin_pair()

    def fetches(slot):
        for item in FETCHES[slot].split(","):
            who, phase, j = (later if item[0] == "L" else fetch), item.strip("L")[:-1], int(item[-1])
            if phase == "d1" and j == 0:
                who.end_pair()
            do = getattr(who, "start_" + phase)
            if phase in ("a1", "a2", "c"):
                do(j, alone=who is later or j == 0)
            else:
                do(j)

    fetches(0)
    load.wait()

    def prepare(i):
        rows = at(i * z.T3, z.T3)
        a[rows, :] = normed(xs[rows, :].astype(f32))[0]
        acc[rows, :] = jnp.zeros((z.T3, z.D), f32)

    loop(0, z.T // z.T3, prepare)
    fetches(1)
    n = z.T // z.TC

    def keep(j, i):
        slot = odd(i)
        return [pltpu.make_async_copy(v.at[slot], o.at[j, at(i * z.TC, z.TC), :], keep_sem.at[k, slot]) for k, (v, o) in enumerate(zip(parts, kept_out, strict=True))]

    def kept(j, i):
        for copy in keep(j, i):
            copy.wait()

    def serve(j, middle):
        for b in range(z.NB):
            pl.when(j == b)(lambda b=b: fetches(2 + 2 * b + middle))

    def block(j):
        serve(j, 0)
        fetch.ready(j)
        start([pltpu.make_async_copy(v.at[j], o.at[j], out_sem.at[k]) for k, (v, o) in enumerate(zip(w, w_out, strict=True))])

        def chunk(i):
            @pl.when(i == n // 2)
            def _():
                serve(j, 1)

                @pl.when(j == 0)
                def _():
                    later.begin_local()
                    later.begin_pair()


            pl.when(j * n + i > 1)(lambda: kept(j, i))
            rows, slot = at(i * z.TC, z.TC), odd(i)
            for cols in z.halves:
                gate, up = dot(a[rows, :], w[0][j, :, cols]), dot(a[rows, :], w[1][j, :, cols])
                sig = 1.0 / (1.0 + jnp.exp(-gate))
                silu = gate * sig
                act[slot, :, cols] = (silu * up).astype(bf16)
                by_up[slot, :, cols] = silu
                by_gate[slot, :, cols] = up * (sig + silu * (1.0 - sig))
            acc[rows, :] += dot(act[slot], w[2][j])
            start(keep(j, i))

        loop(0, n, chunk)

    loop(0, z.NB, block)

    def finish(i):
        rows = at(i * z.T3, z.T3)
        xs[rows, :] = xs[rows, :] + acc[rows, :].astype(bf16)

    loop(0, z.T // z.T3, finish)
    store = pltpu.make_async_copy(xs, h_out, h_sem)
    store.start()
    for e in early:
        later.ready(e)
    handed = [pltpu.make_async_copy(v, o, next_sem.at[k]) for k, (v, o) in enumerate(zip(w_next, next_out, strict=True))]
    start(handed)
    for i in range(2):
        kept(z.NB - 1, n - 2 + i)
    for k, v in enumerate(w):
        wait(v, out_sem.at[k])
    fetch.end((0,))
    later.end(early)
    store.wait()
    for copy in handed:
        copy.wait()


class Reduce:
    PHASES = ("p", "x1", "x2", "y", "z", "az", "ay", "f")

    def __init__(self, z, here, units, base, outs, refs):
        self.z, self.here, self.units, self.base, self.outs = z, here, units, base, outs
        (self.stage, self.got_p, self.got_x1, self.got_x2, self.got_y, self.got_z, self.send_x1, self.send_x2, self.send_y, self.send_z, *refs) = refs
        (self.kept_x, self.kept_y, self.kept_z, self.fin, self.down, self.turned, self.out_sem, self.turned_sem, self.piece_sem, *refs) = refs
        self.got = dict(zip(self.PHASES, refs[::2], strict=True))
        self.sent = dict(zip(self.PHASES, refs[1::2], strict=True))

    @classmethod
    def scratch(cls, z, units):
        unit, share = z.unit, z.unit[1:]
        data = [(2, X, CORES, *unit), (3, X, *unit), (2, 2, Y // 2, *share), (2, 2, *unit), (2, *unit), (units, z.Z, 3, 16, LANES)]
        data += [unit, (2, 2, *unit), unit, share]
        wide = [(2, *unit), share, share]
        return (
            [VMEM(shape, bf16) for shape in data]
            + [VMEM(shape, f32) for shape in wide]
            + [VMEM((units, *unit), bf16), VMEM((units, CORES, Y, z.h, LANES), bf16), VMEM((2, LANES, z.D), bf16)]
            + [DMA((2, units)), DMA((2, 2)), DMA]
            + [DMA((units + 3,)) for _ in range(2 * len(cls.PHASES))]
        )

    def peers(self):
        here = self.here
        return (
            [here.partner()] + [here.along_x(k) for k in SIDES] + [here.along_y(k) for k in range(1, Y)] + [here.along_z(k) for k in range(1, here.Z)]
        )

    def which(self, u, m):
        return (u, ALL) if m is None else (self.units + m, m)

    def send(self, phase, i, src, dst, where):
        remote(src, dst, self.sent[phase].at[i], self.got[phase].at[i], where).start()

    def over(self, m, work, begin=0, end=Y):
        def share(y):
            for k in range(len(self.outs)) if m is None else (m,):
                work(y, k)

        loop(begin, end, share)

    def start_p(self, u, m=None):
        here, (i, mm) = self.here, self.which(u, m)
        for x in range(X):
            self.send("p", i, self.stage.at[odd(u), x, 1 - here.c, :, mm], self.got_p.at[lax.rem(u, 3), x, :, mm], here.partner())

    def both(self, u, x, y, m):
        return self.stage[odd(u), x, self.here.c, y, m].astype(f32) + self.got_p[lax.rem(u, 3), x, y, m].astype(f32)

    def start_x1(self, u, m=None):
        here, half, slot, (i, mm) = self.here, Y // 2, odd(u), self.which(u, m)
        wait(self.got_p.at[lax.rem(u, 3), :, :, mm], self.got["p"].at[i])
        far = lax.rem(here.x + FAR, X)

        def work(y, k):
            self.send_x1[y, k] = self.both(u, far, y, k).astype(bf16)

        self.over(m, work)
        for side in range(2):
            self.send("x1", i, self.send_x1.at[pl.ds(side * half, half), mm], self.got_x1.at[slot, side, :, mm], here.along_x(SIDES[side]))

    def start_x2(self, u, m=None):
        here, half, slot, (i, mm) = self.here, Y // 2, odd(u), self.which(u, m)
        wait(self.got_x1.at[slot, :, :, mm], self.got["x1"].at[i])
        wait(self.got_x1.at[slot, :, :, mm], self.sent["x1"].at[i])
        wait(self.got_p.at[lax.rem(u, 3), :, :, mm], self.sent["p"].at[i])
        right, left = here.right(), here.left()

        def first(y, k):
            self.send_x2[slot, 0, y, k] = (self.both(u, right, y, k) + self.got_x1[slot, 0, y, k].astype(f32)).astype(bf16)
            self.send_x2[slot, 1, y, k] = self.both(u, left, y, k).astype(bf16)
            self.kept_x[slot, y, k] = self.both(u, here.x, y, k)

        def second(y, k):
            self.send_x2[slot, 0, y, k] = self.both(u, right, y, k).astype(bf16)
            self.send_x2[slot, 1, y, k] = (self.both(u, left, y, k) + self.got_x1[slot, 1, y - half, k].astype(f32)).astype(bf16)
            self.kept_x[slot, y, k] = self.both(u, here.x, y, k)

        self.over(m, first, 0, half)
        self.over(m, second, half, Y)
        for side in range(2):
            self.send("x2", i, self.send_x2.at[slot, side, :, mm], self.got_x2.at[slot, side, :, mm], here.along_x(SIDES[side]))

    def start_y(self, u, m=None):
        here, slot, (i, mm) = self.here, odd(u), self.which(u, m)
        wait(self.got_x2.at[slot, :, :, mm], self.got["x2"].at[i])
        wait(self.got_x2.at[slot, :, :, mm], self.sent["x2"].at[i])

        def total(y, k):
            return self.kept_x[slot, y, k] + self.got_x2[slot, 0, y, k].astype(f32) + self.got_x2[slot, 1, y, k].astype(f32)

        def work(y, k):
            self.send_y[y, k] = total(y, k).astype(bf16)

        def own(_, k):
            self.kept_y[k] = total(here.y, k)

        self.over(m, work)
        self.over(m, own, 0, 1)
        for k in (*SIDES, FAR):
            self.send("y", i, self.send_y.at[lax.rem(here.y + k, Y), mm], self.got_y.at[slot, here.y, mm], here.along_y(k))

    def start_z(self, u, m=None):
        z, here, slot, (i, mm) = self.z, self.here, odd(u), self.which(u, m)
        wait(self.got_y.at[slot, pl.ds(0, Y - 1), mm], self.got["y"].at[i])
        wait(self.got_y.at[slot, pl.ds(0, Y - 1), mm], self.sent["y"].at[i])

        def work(_, k):
            total = self.kept_y[k]
            for place in range(1, Y):
                total += self.got_y[slot, lax.rem(here.y + place, Y), k].astype(f32)
            self.kept_z[k] = total
            self.send_z[k] = total.astype(bf16)

        self.over(m, work, 0, 1)

        def send(k):
            to = lax.rem(here.z + k, z.Z)
            pl.when(to < z.active)(lambda: self.send("z", i, self.send_z.at[mm, at(to * 16, 16), :], self.got_z.at[u, here.z, mm], here.along_z(k)))

        loop(1, z.Z, send)

    def if_active(self, yes, no):
        pl.when(self.here.z < self.z.active)(yes)
        pl.when(self.here.z >= self.z.active)(no)

    def wait_pieces(self, i, mm, n, sem):
        if n:
            wait(self.got_z.at[0, pl.ds(0, n), mm], sem.at[i])

    def mine(self, mm):
        return self.here.y, mm, at(self.here.z * 16, 16)

    def add_pieces(self, u, m):
        z, here, (i, mm) = self.z, self.here, self.which(u, m)
        self.wait_pieces(i, mm, z.active - 1, self.sent["z"])
        self.wait_pieces(i, mm, z.Z - 1, self.got["z"])
        y, mm, rows = self.mine(mm)
        total = self.kept_z[mm, rows, :]
        for k in range(1, z.Z):
            total += self.got_z[u, lax.rem(here.z + k, z.Z), mm].astype(f32)
        self.fin[u, y, mm, rows, :] = total.astype(bf16)

    def send_pieces(self, u, m=None):
        i, mm = self.which(u, m)
        y, mm, rows = self.mine(mm)
        piece = self.fin.at[u, y, mm, rows, :]
        loop(1, self.z.Z, lambda k: self.send("az", i, piece, piece, self.here.along_z(k)))

    def start_az(self, u, m=None):
        i, mm = self.which(u, m)

        def yes():
            self.add_pieces(u, m)
            self.send_pieces(u, m)

        self.if_active(yes, lambda: self.wait_pieces(i, mm, self.z.active, self.sent["z"]))

    def hand_on(self, u, out):
        def yes():
            self.add_pieces(u, None)
            y, mm, rows = self.mine(ALL)
            copy = pltpu.make_async_copy(self.fin.at[u, y, mm, rows, :], out, self.piece_sem)
            copy.start()
            copy.wait()

        self.if_active(yes, lambda: self.wait_pieces(u, ALL, self.z.active, self.sent["z"]))

    def take_over(self, u, piece):
        def yes():
            y, mm, rows = self.mine(ALL)
            copy = pltpu.make_async_copy(piece, self.fin.at[u, y, mm, rows, :], self.piece_sem)
            copy.start()
            copy.wait()
            self.send_pieces(u)

        pl.when(self.here.z < self.z.active)(yes)

    def start_ay(self, u, m=None):
        z, here, (i, mm) = self.z, self.here, self.which(u, m)
        self.if_active(lambda: self.wait_pieces(i, mm, z.active - 1, self.got["az"]), lambda: self.wait_pieces(i, mm, z.active, self.got["az"]))
        share = self.fin.at[u, here.y, mm]
        for k in (*SIDES, FAR):
            self.send("ay", i, share, share, here.along_y(k))

    def place(self, u):
        nb = self.z.NB
        return (1, u) if self.base == 0 else (1 - lax.div(u + nb - self.base, nb), lax.rem(u + nb - self.base, nb))

    def start_f(self, u, m=None):
        z, c, (i, mm) = self.z, self.here.c, self.which(u, m)
        layer, j = self.place(u)
        wait(self.fin.at[u, pl.ds(0, Y - 1), mm], self.got["ay"].at[i])
        for k in range(2) if m is None else (m,):
            if k == 2:
                break
            for y in range(Y):
                out = self.outs[k].at[layer, :, at((y * z.NB + j) * LANES, LANES, LANES)]
                pltpu.make_async_copy(self.fin.at[u, y, k], out, self.out_sem.at[k, u]).start()
        if m in (None, 2):
            self.down[u, c] = self.fin[u, :, 2]
            self.send("f", u, self.fin.at[u, :, 2], self.down.at[u, c], self.here.partner())

    def finish(self, u):
        z, c = self.z, self.here.c
        layer, j = self.place(u)
        wait(self.down.at[u, 0], self.got["f"].at[u])
        slot = odd(u)
        pl.when(u > 1)(lambda: self.turned_out(u - 2, "wait"))
        self.turned[slot] = self.down[u].reshape(z.D, LANES).T
        self.turned_out(u, "start")

    def turned_out(self, u, what):
        z, c = self.z, self.here.c
        layer, j = self.place(u)
        for half in range(2):
            row = 2 * j + half

            @pl.when(lax.div(row, z.NB) == c)
            def _(half=half, row=row):
                out = self.outs[2].at[layer, at(lax.rem(row, z.NB) * 64, 64), :]
                getattr(pltpu.make_async_copy(self.turned.at[odd(u), pl.ds(half * 64, 64), :], out, self.turned_sem.at[odd(u), half]), what)()

    def end(self, units, in_parts):
        z = self.z

        def sent_back(i, mm):
            self.if_active(lambda: self.wait_pieces(i, mm, z.Z - 1, self.sent["az"]), lambda: None)
            wait(self.fin.at[0, pl.ds(0, Y - 1), mm], self.sent["ay"].at[i])

        def one(u):
            wait(self.down.at[0, 0], self.sent["f"].at[u])
            for m in range(2):
                wait(self.down.at[0, 0], self.out_sem.at[m, u])

        loop(0, units, one)
        loop(0, units - in_parts, lambda u: sent_back(u, ALL))
        for m in range(len(self.outs) if in_parts else 0):
            sent_back(self.units + m, m)
        for u in range(max(0, units - 2), units):
            self.turned_out(u, "wait")


def backward_kernel(z, first, *refs):
    T, TC, T3, NB, FB, D = z.T, z.TC, z.T3, z.NB, z.FB, z.D
    here = Here(z)
    refs = list(refs)

    def take(n):
        out, refs[:] = refs[:n], refs[n:]
        return out

    h_in, dh_in, w0, w1, w2 = take(5)
    if first:
        early_in = take(3)
    else:
        left_in, piece_in, by_up_in, by_gate_in, act_in = take(5)
        take(3)
    dx_out, *outs = take(4)
    spill = take(1)[0]
    if first:
        left_out, piece_out = take(2)
    dx_buf, h_buf, a_t, dh, dh_t, wg, wu, wd, work = take(9)
    ld_sem, dh_sem, w_sem, sp_sem, s3_sem, o_sem, left_sem = take(7)
    if first:
        a = take(1)[0]
    else:
        saved, saved_sem, act_sem = take(3)
    if first:
        fetch = Fetch(z, here, (w0.at[1], w1.at[1], w2.at[1]), (wg, wu, wd), take(len(Fetch.scratch(z))), z.early, NB)
        w0, w1, w2 = early_in
    base = 0 if first else 2
    units = NB - 1 if first else NB + base
    reduce = Reduce(z, here, units, base, outs, refs)
    met = meet(reduce.peers())
    whole = pltpu.make_async_copy(dh_in, dh, dh_sem)
    whole.start()

    def load_h(i):
        return pltpu.make_async_copy(h_in.at[at(i * T3, T3), :], h_buf.at[odd(i)], ld_sem.at[odd(i)])

    load_h(0).start()

    def loads(j):
        return [pltpu.make_async_copy(src.at[j], dst.at[j], w_sem.at[k, j]) for k, (src, dst) in enumerate(((w0, wg), (w1, wu), (w2, wd)))]

    TS, slots = z.TS, 3

    def load_saved(q):
        j, rows, slot = lax.div(q, T // TS), at(lax.rem(q, T // TS) * TS, TS), lax.rem(q, slots)
        return [pltpu.make_async_copy(v.at[j, rows, :], saved.at[slot, k], saved_sem.at[k, slot]) for k, v in enumerate((by_up_in, by_gate_in))]

    def load_act(j):
        return pltpu.make_async_copy(act_in.at[j], work.at[pl.ds(0, T), :], act_sem)

    if first:
        for j in range(z.early):
            start(loads(j))
        fetch.begin_local()
        met()
        fetch.begin_pair()
        fetch.start_a1(z.early)
    else:
        left = pltpu.make_async_copy(left_in, reduce.stage.at[1], left_sem)
        left.start()
        for j in range(NB):
            start(loads(j)[2:])
        for q in range(2):
            start(load_saved(q))
        for j in range(NB):
            start(loads(j)[:2])
    whole.wait()
    n3 = T // T3

    def prepare(i):
        rows = at(i * T3, T3, LANES)
        pl.when(i + 1 < n3)(lambda: load_h(i + 1).start())
        load_h(i).wait()
        value = normed(h_buf[odd(i)].astype(f32))[0]
        if first:
            a[rows, :] = value
        a_t[:, rows] = value.T
        dh_t[:, rows] = dh[rows, :].T

    if not first:
        met()
        left.wait()
        reduce.start_p(1)
        reduce.take_over(0, piece_in)
    loop(0, n3, prepare)
    if first:
        fetch.end_pair()
        fetch.start_a2(z.early)

    def product(k, rows, cols):
        return work.at[at(k * T + rows.start, rows.size), cols]

    def spills(j):
        return [pltpu.make_async_copy(work.at[pl.ds((1 + k) * T, T), :], spill.at[k, j], sp_sem.at[k]) for k in range(2)]

    def spilled(j):
        for copy in spills(j):
            copy.wait()

    def step(name, u, m=None):
        do = getattr(reduce, "start_" + name)
        back = name in ("ay", "az")
        begin = 0 if first or name == "ay" else 1
        end = units - 1 if first and back else units
        if isinstance(u, int):
            if begin <= u < end:
                do(u, m)
        else:
            pl.when(jnp.logical_and(u >= begin, u < end))(lambda: do(u))

    def halfway(i, n, before, after):
        if n == 1:
            before()
            after()
        else:
            pl.when(i == 0)(before)
            pl.when(i == n // 2)(after)

    def loaded(j):
        for copy in loads(j):
            copy.wait()

    def block(j):
        u = j + base - 1
        if first:
            fetch.serve_a(j)
            pl.when(j < z.early)(lambda: loaded(j))
            pl.when(j >= z.early)(lambda: fetch.ready(j))
        else:
            load_act(j).start()
            loads(j)[2].wait()
        pl.when(j > 0)(lambda: spilled(j - 1))

        def at_0():
            step("x2", u - 1)

        def at_1():
            step("z", u - 2)
            step("ay", u - 3)

        def at_2():
            if first:
                fetch.serve_b(j)
            step("x1", u)

        def at_3():
            step("y", u - 1)
            step("az", u - 2)

        def piece(i):
            halfway(i, T // TS, at_0, at_1)
            q, rows = j * (T // TS) + i, at(i * TS, TS)
            pl.when(q + 2 < NB * (T // TS))(lambda: start(load_saved(q + 2)))
            for copy in load_saved(q):
                copy.wait()
            by_act = dot(dh[rows, :], wd[j], ((1,), (1,))).astype(bf16).astype(f32)
            slot = lax.rem(q, slots)
            product(1, rows, ALL)[...] = (by_act * saved[slot, 1]).astype(bf16)
            product(2, rows, ALL)[...] = (by_act * saved[slot, 0]).astype(bf16)

        def chunk(i):
            halfway(i, T // TC, at_0, at_1)
            rows = at(i * TC, TC)
            for cols in z.halves:
                gate, up = dot(a[rows, :], wg[j, :, cols]), dot(a[rows, :], wu[j, :, cols])
                by_act = dot(dh[rows, :], wd[j, cols, :], ((1,), (1,))).astype(bf16).astype(f32)
                sig = 1.0 / (1.0 + jnp.exp(-gate))
                silu = gate * sig
                product(0, rows, cols)[...] = (silu * up).astype(bf16)
                product(1, rows, cols)[...] = (by_act * up * (sig + silu * (1.0 - sig))).astype(bf16)
                product(2, rows, cols)[...] = (by_act * silu).astype(bf16)

        if first:
            loop(0, T // TC, chunk)
        else:
            loop(0, T // TS, piece)
            load_act(j).wait()
        start(spills(j))
        stage, slot, m = reduce.stage, odd(j + base), D // 2

        def rows_of(i):
            halfway(i, 2, at_2, at_3)
            rows = at(i * m, m)
            gates = dot(a_t[rows, :], work[pl.ds(T, T), :]).astype(bf16)
            ups = dot(a_t[rows, :], work[pl.ds(2 * T, T), :]).astype(bf16)
            downs = dot(dh_t[rows, :], work[pl.ds(0, T), :]).astype(bf16)
            for y in range(Y):
                lanes = slice(y * LANES, (y + 1) * LANES)
                for x in range(X // 2):
                    for c in range(CORES):
                        part = slice((x * CORES + c) * z.h, (x * CORES + c + 1) * z.h)
                        stage[slot, i * (X // 2) + x, c, y, 0] = gates[part, lanes]
                        stage[slot, i * (X // 2) + x, c, y, 1] = ups[part, lanes]
                for x in range(X):
                    stage[slot, x, i, y, 2] = downs[y * z.h : (y + 1) * z.h, x * LANES : (x + 1) * LANES]

        loop(0, 2, rows_of)
        if first:
            step("p", j)
        else:
            pl.when(j + 1 < NB)(lambda: reduce.start_p(j + base))

            @pl.when(j + 1 == NB)
            def _():
                for m in range(3):
                    reduce.start_p(NB + base - 1, m)

    loop(0, NB, block)
    if first:
        left = pltpu.make_async_copy(reduce.stage.at[(NB - 1) % 2], left_out, left_sem)
        left.start()
    spilled(NB - 1)

    def load_3(i):
        slot, rows = odd(i), at(i * T3, T3)
        out = [load_h(i)]
        for k in range(2):
            for j in range(NB):
                out.append(pltpu.make_async_copy(spill.at[k, j, rows, :], work.at[at(((slot * 2 + k) * NB + j) * T3, T3), :], s3_sem.at[slot]))
        return out

    def store_3(i):
        return pltpu.make_async_copy(dx_buf.at[odd(i)], dx_out.at[at(i * T3, T3), :], o_sem.at[odd(i)])

    start(load_3(0))
    u = NB + base - 1
    if first:
        todo = ("x2:1", "z:2,ay:3", "", "az:2,y:1", "", "ay:2,z:1", "", "")
    else:
        todo = (
            "x2:1,ay:3",
            "x1.0,x1.1,z:2",
            "x1.2",
            "x2.0,az:2,y:1,x2.1",
            "x2.2,ay:2",
            "z:1,y.0,y.1",
            "y.2,az:1,z.0,z.1",
            "z.2,ay:1,az.0",
            "az.1,az.2,ay.0,ay.1,ay.2",
        )

    def steps(text):
        for item in filter(None, text.split(",")):
            name, _, behind = item.partition(":")
            if behind:
                step(name, u - int(behind))
            else:
                name, _, m = item.partition(".")
                step(name, u, int(m))

    done = units - 2 if first else units - 4

    def rows_back(i):
        slot, rows = odd(i), at(i * T3, T3)
        pl.when(i + 1 < n3)(lambda: start(load_3(i + 1)))
        for when, text in enumerate(todo[:n3]):
            pl.when(i == when)(lambda text=text: steps(text))

        @pl.when(i == n3 - 2)
        def _():
            loop(0, done, reduce.start_f)

        @pl.when(i == n3 - 1)
        def _():
            loop(0, done, reduce.finish)

        if not first:

            @pl.when(i == 0)
            def _():
                for j in range(NB):
                    for copy in loads(j)[:2]:
                        copy.wait()

        load_h(i).wait()
        wait(work.at[at(slot * 2 * NB * T3, 2 * NB * T3), :], s3_sem.at[slot])
        pl.when(i > 1)(lambda: store_3(i - 2).wait())
        back = []
        for k, w in ((0, wg), (1, wu)):
            total = None
            for j in range(NB):
                part = dot(work[at(((slot * 2 + k) * NB + j) * T3, T3), :], w[j], ((1,), (1,)))
                total = part if total is None else total + part
            back.append(total.astype(bf16))
        by_a = (back[0] + back[1]).astype(f32)
        wide = h_buf[slot].astype(f32)
        square = jnp.mean(wide * wide, -1, keepdims=True) + 1e-6
        scale = lax.rsqrt(square)
        by_scale = jnp.sum(by_a * wide, -1, keepdims=True)
        by_square = by_scale * (-0.5 * scale / square) * (2.0 / D)
        dx_buf[slot] = dh[rows, :] + (by_a * scale + by_square * wide).astype(bf16)
        store_3(i).start()

    loop(0, n3, rows_back)
    assert n3 == 8
    for text in todo[n3:]:
        steps(text)
    if first:
        reduce.hand_on(units - 1, piece_out)
    back = units - 1 if first else units
    for v in range(done, back):
        if first or v + 1 < back:
            reduce.start_f(v)
        else:
            for m in range(3):
                reduce.start_f(v, m)
    for v in range(done, back):
        reduce.finish(v)
    reduce.end(back, 0 if first else 1)
    if first:
        fetch.end(())
        left.wait()
    for i in range(max(0, n3 - 2), n3):
        store_3(i).wait()


def call(body, out, n_in, scratch, number, aliases=()):
    return pl.pallas_call(
        body,
        out_shape=out,
        in_specs=[pl.BlockSpec(memory_space=HBM)] * n_in,
        out_specs=[pl.BlockSpec(memory_space=HBM)] * len(out),
        scratch_shapes=scratch,
        input_output_aliases=dict(aliases),
        compiler_params=pltpu.CompilerParams(collective_id=number, has_side_effects=True, vmem_limit_bytes=66_900_000),
    )


def forward(z, x, shards):
    S = jax.ShapeDtypeStruct
    wide, tall, tokens, hidden, piece = (z.NB, z.D, z.FB), (z.NB, z.FB, z.D), (z.T, z.D), (z.NB, z.T, z.FB), (2, z.TC, z.FB)
    scratch = [VMEM(tokens, bf16), VMEM(tokens, f32), VMEM(tokens, bf16), VMEM(piece, bf16), VMEM(piece, f32), VMEM(piece, f32)]
    early = [(z.early, *shape[1:]) for shape in (wide, wide, tall)]
    scratch += [VMEM(shape, bf16) for shape in (wide, wide, tall, *early)]
    scratch += [DMA, DMA((3,)), DMA((3,)), DMA, DMA((3, 2))] + Fetch.scratch(z) + Fetch.scratch(z)
    out = [S(tokens, bf16), S(wide, bf16), S(wide, bf16), S(tall, bf16), S(hidden, bf16), S(hidden, f32), S(hidden, f32)]
    out += [S(shape, bf16) for shape in early]
    h, *out = call(functools.partial(forward_kernel, z), out, 4, scratch, 0)(x, *shards)
    return h, out[:3], out[3:6], out[6:]


def backward(z, h, dh, w, more, first):
    S = jax.ShapeDtypeStruct
    wide, tall, tokens = (z.NB, z.D, z.FB), (z.NB, z.FB, z.D), (z.T, z.D)
    units = z.NB - 1 if first else z.NB + 2
    scratch = [VMEM((2, z.T3, z.D), bf16), VMEM((2, z.T3, z.D), bf16)]
    scratch += [VMEM(tokens[::-1], bf16), VMEM(tokens, bf16), VMEM(tokens[::-1], bf16)]
    scratch += [VMEM(wide, bf16), VMEM(wide, bf16), VMEM(tall, bf16), VMEM((max(3 * z.T, 4 * z.NB * z.T3), z.FB), bf16)]
    scratch += [DMA((2,)), DMA, DMA((3, z.NB)), DMA((2,)), DMA((2,)), DMA((2,)), DMA]
    if first:
        scratch += [VMEM(tokens, bf16)] + Fetch.scratch(z)
    else:
        scratch += [VMEM((3, 2, z.TS, z.FB), f32), DMA((2, 3)), DMA]
    scratch += Reduce.scratch(z, units)
    grads = [S((2, z.h, z.F), bf16), S((2, z.h, z.F), bf16), S((2, z.F // (X * CORES), z.D), bf16)]
    out = [S(tokens, bf16), *grads, S((2, z.NB, z.T, z.FB), bf16)]
    if first:
        out += [S((X, CORES, *z.unit), bf16), S((3, 16, LANES), bf16)]
    args = (h, dh, *w, *more)
    aliases = {} if first else {len(args) - 3 + i: 1 + i for i in range(3)}
    dx, g, u, d, _, *left = call(functools.partial(backward_kernel, z, first), out, len(args), scratch, 1 if first else 2, aliases)(*args)
    return dx, (g, u, d), left


def solution(mesh):
    def step(x, dy, *weights):
        z = Sizes(mesh, x.shape[1], x.shape[2], weights[0].shape[2])
        h, w, (act, by_up, by_gate), early = forward(z, x[0], weights)
        dh, grads, left = backward(z, h, dy[0], weights, early, True)
        dx, grads, _ = backward(z, x[0], dh, w, (*left, by_up, by_gate, act, *grads), False)
        return dx[None], *grads

    states, cut = P(("rep", "r", "s"), None, None), P(None, "s", None)
    return jax.shard_map(
        step,
        mesh=mesh,
        in_specs=(states, states) + (cut,) * 3,
        out_specs=(states,) + (P("rep", "s", None),) * 3,
        check_vma=False,
    )
```

```python
import functools

import jax
import jax.numpy as jnp
from jax import lax
from jax.experimental import pallas as pl
from jax.experimental.pallas import tpu as pltpu
from jax.sharding import PartitionSpec as P

f32, bf16 = jnp.float32, jnp.bfloat16
MESH = pl.DeviceIdType.MESH
LANES = 128
X, CORES, Y = 4, 2, 4
HBM, VMEM, DMA = pl.ANY, pltpu.VMEM, pltpu.SemaphoreType.DMA


def dot(a, b, dims=((1,), (0,))):
    return lax.dot_general(a, b, (dims, ((), ())), preferred_element_type=f32)


def at(start, size, multiple=16):
    return pl.ds(pl.multiple_of(start, multiple) if not isinstance(start, int) else start, size)


ALL = slice(None)
LEFT, RIGHT, FAR = 3, 1, 2
SIDES = (RIGHT, LEFT)


def loop(begin, end, body):
    def one(i, carry):
        body(i)
        return carry

    lax.fori_loop(begin, end, one, 0)


def odd(i):
    return lax.rem(i, 2)


class Sizes:
    chunk, piece, rows, slots = 1024, 512, 256, 4

    def __init__(self, mesh, tokens, d, ff):
        self.R = mesh.shape["r"]
        self.Z = self.R // Y
        self.T, self.D, self.F = tokens, d, ff
        self.NB = ff // (X * LANES)
        self.FB = X * LANES
        self.h = d // (X * CORES)
        self.TC = min(self.chunk, tokens)
        self.T3 = min(self.rows, tokens)
        self.TS = min(self.piece, tokens)
        self.unit = (Y, 3, self.h, LANES)
        self.active = self.h // 16
        self.halves = (slice(0, self.FB // 2), slice(self.FB // 2, self.FB))
        self.early = self.NB // 2
        assert self.h % 16 == 0 and self.active <= self.Z and mesh.shape["s"] == X * CORES


class Here:
    def __init__(self, z):
        s, self.r = lax.axis_index("s"), lax.axis_index("r")
        self.x, self.c = lax.div(s, CORES), lax.rem(s, CORES)
        self.y, self.z, self.Z = lax.div(self.r, z.Z), lax.rem(self.r, z.Z), z.Z
        self.R = z.R

    def partner(self):
        return {"s": self.x * CORES + 1 - self.c}

    def along_x(self, k):
        return {"s": lax.rem(self.x + k, X) * CORES + self.c}

    def along_y(self, k):
        return {"r": lax.rem(self.y + k, Y) * self.Z + self.z}

    def right(self):
        return lax.rem(self.x + RIGHT, X)

    def left(self):
        return lax.rem(self.x + LEFT, X)

    def along_z(self, k):
        return {"r": self.y * self.Z + lax.rem(self.z + k, self.Z)}


def remote(src, dst, sent, got, where):
    return pltpu.make_async_remote_copy(src_ref=src, dst_ref=dst, send_sem=sent, recv_sem=got, device_id=where, device_id_type=MESH)


def start(copies):
    for copy in copies:
        copy.start()


def wait(ref, sem):
    pltpu.make_async_copy(ref, ref, sem).wait()


def meet(peers):
    barrier = pltpu.get_barrier_semaphore()
    for peer in peers:
        pl.semaphore_signal(barrier, inc=1, device_id=peer, device_id_type=MESH)
    return lambda: pl.semaphore_wait(barrier, len(peers))


FETCHES = (
    "a10,a11,a20,d10,b10,d11,a21",
    "d20,a12,a14,b20,a13,e0,b11,d21,c0,a22,d12",
    "e1,a23,d13,a24,b21,b12",
    "d22,c1,d14,b13",
    "d23,La11,e2,La10,b22",
    "b23,b14,La21,d24,c2,Ld10,Ld11",
    "e4,c3,Lb11",
    "e3,La20,Ld21,b24",
    "Lb10",
    "Ld20,c4,Lb21",
    "Lb20,Le0,Le1,Lc1",
    "Lc0",
)


class Fetch:
    PHASES = ("a1", "a2", "b1", "b2", "c", "d1", "d2", "e")

    def __init__(self, z, here, shards, w, sems, begin, end):
        self.z, self.here, self.shards, self.w, self.first, self.last = z, here, shards, w, begin, end
        self.local, self.local_d, self.pair, self.pair_sent = sems[:4]
        self.got = dict(zip(self.PHASES, sems[4::2], strict=True))
        self.sent = dict(zip(self.PHASES, sems[5::2], strict=True))
        self.parts = [[k for k in range(z.NB) if begin <= (c * z.NB + k) // 2 < end] for c in range(CORES)]

    @classmethod
    def scratch(cls, z):
        return [DMA((z.NB,)), DMA, DMA, DMA] + [DMA((z.NB,)) for _ in range(2 * len(cls.PHASES))]

    def peers(self):
        here = self.here
        return [here.partner()] + [here.along_x(k) for k in SIDES] + [here.along_y(k) for k in SIDES]

    def own(self, j):
        z, here = self.z, self.here
        for shard, w in zip(self.shards[:2], self.w[:2], strict=True):
            for l in range(X):
                slot = w.at[j, self.rows(here.x), pl.ds(l * LANES, LANES)]
                pltpu.make_async_copy(shard.at[:, at((l * z.NB + j) * LANES, LANES, LANES)], slot, self.local.at[j]).start()

    def each_core(self, do):
        for c in range(CORES):
            pl.when(self.here.c == c)(lambda c=c: do(self.parts[c], self.parts[1 - c]))

    def part(self, k):
        z, here = self.z, self.here
        place = here.c * z.NB + k
        return self.shards[2].at[pl.ds(64 * k, 64), :], self.w[2].at[lax.div(place, 2), at(here.x * LANES + odd(place) * 64, 64), :]

    def rows(self, x):
        return at(x * (CORES * self.z.h) + self.here.c * self.z.h, self.z.h)

    def lanes(self, y):
        return at(y * LANES, LANES, LANES)

    def down(self, x, begin=0, size=64):
        return at(x * LANES + self.here.c * 64 + begin, size)

    def send(self, phase, j, w, rows, lanes, where):
        slot = self.w[w].at[j, rows, lanes]
        remote(slot, slot, self.sent[phase].at[j], self.got[phase].at[j], where).start()

    def begin_local(self):
        for j in range(self.first, self.last):
            self.own(j)

        def do(mine, _):
            for k in mine:
                pltpu.make_async_copy(*self.part(k), self.local_d).start()

        self.each_core(do)

    def begin_pair(self):
        def do(mine, _):
            for k in mine:
                src, slot = self.part(k)
                remote(src, slot, self.pair_sent, self.pair, self.here.partner()).start()

        self.each_core(do)

    def wait_parts(self, n, sem):
        if n:
            wait(self.halves(0, n), sem)

    def end_pair(self):
        def do(mine, other):
            self.wait_parts(len(mine), self.local_d)
            self.wait_parts(len(other), self.pair)

        self.each_core(do)

    def start_a1(self, j):
        here = self.here
        wait(self.pieces(j, 8), self.local.at[j])
        for k in SIDES:
            for w in range(2):
                self.send("a1", j, w, self.rows(here.x), self.lanes(here.y), here.along_x(k))

    def start_d1(self, j):
        for k in SIDES:
            self.send("d1", j, 2, self.down(self.here.x), ALL, self.here.along_x(k))

    def start_a2(self, j):
        here = self.here
        wait(self.pieces(j, 4), self.got["a1"].at[j])
        lanes = self.lanes(here.y)
        self.send("a2", j, 0, self.rows(here.left()), lanes, here.along_x(RIGHT))
        self.send("a2", j, 1, self.rows(here.right()), lanes, here.along_x(LEFT))

    def start_d2(self, j):
        here = self.here
        wait(self.halves(j, 2), self.got["d1"].at[j])
        self.send("d2", j, 2, self.down(here.left(), 0, 32), ALL, here.along_x(RIGHT))
        self.send("d2", j, 2, self.down(here.right(), 32, 32), ALL, here.along_x(LEFT))

    def start_b1(self, j):
        here = self.here
        wait(self.pieces(j, 2), self.got["a2"].at[j])
        for k in SIDES:
            for m in range(1, X):
                for w in range(2):
                    self.send("b1", j, w, self.rows(lax.rem(here.x + m, X)), self.lanes(here.y), here.along_y(k))

    def start_b2(self, j):
        here = self.here
        wait(self.pieces(j, 12), self.got["b1"].at[j])
        for m in range(1, X):
            rows = self.rows(lax.rem(here.x + m, X))
            self.send("b2", j, 0, rows, self.lanes(lax.rem(here.y + LEFT, Y)), here.along_y(RIGHT))
            self.send("b2", j, 1, rows, self.lanes(lax.rem(here.y + RIGHT, Y)), here.along_y(LEFT))

    def start_c(self, j):
        wait(self.pieces(j, 6), self.got["b2"].at[j])
        for w in range(2):
            for x in range(X):
                self.send("c", j, w, self.rows(x), ALL, self.here.partner())

    def start_e(self, j):
        wait(self.halves(j, 1), self.got["d2"].at[j])
        for m in range(1, X):
            self.send("e", j, 2, self.down(lax.rem(self.here.x + m, X)), ALL, self.here.partner())

    def pieces(self, j, n):
        high = 6 if n % 6 == 0 else min(n, 8)
        return self.w[0].at[j, pl.ds(0, high * self.z.h), pl.ds(0, n // high * LANES)]

    def halves(self, j, n):
        return self.w[2].at[j, pl.ds(0, 64 * n), :]

    def ready(self, j):
        wait(self.w[0].at[j], self.got["c"].at[j])
        wait(self.halves(j, 3), self.got["e"].at[j])

    def serve_a(self, j):
        @self.if_mine(j + 1)
        def _():
            self.start_b2(j + 1)
            self.start_d2(j + 1)

        @self.if_mine(j + 2)
        def _():
            self.start_b1(j + 2)
            self.start_d1(j + 2)

        self.if_mine(j + 3)(lambda: self.start_a1(j + 3))

    def serve_b(self, j):
        @self.if_mine(j + 1)
        def _():
            self.start_c(j + 1)
            self.start_e(j + 1)

        self.if_mine(j + 3)(lambda: self.start_a2(j + 3))

    def if_mine(self, j):
        return pl.when(jnp.logical_and(j >= self.first, j < self.last))

    def end(self):
        self.each_core(lambda mine, _: self.wait_parts(len(mine), self.pair_sent))

        def drain(j):
            for phase, n in (("a1", 4), ("a2", 2), ("b1", 12), ("b2", 6)):
                wait(self.pieces(j, n), self.sent[phase].at[j])
            for phase, n in (("d1", 2), ("d2", 1), ("e", 3)):
                wait(self.halves(j, n), self.sent[phase].at[j])
            wait(self.w[0].at[j], self.sent["c"].at[j])

        loop(self.first, self.last, drain)


def normed(wide):
    scale = lax.rsqrt(jnp.mean(wide * wide, -1, keepdims=True) + 1e-6)
    return (wide * scale).astype(bf16), scale


def forward_kernel(z, *refs):
    refs = list(refs)

    def take(n):
        out, refs[:] = refs[:n], refs[n:]
        return out

    x_in, dy_in, *shards = take(5)
    h_out, *w_out = take(4)
    kept_out, next_out, turned_out = take(3), take(3), take(2)
    a, acc, xs, dy_buf = take(4)
    turned = take(2)
    parts, w, w_next = take(3), take(3), take(3)
    act, by_up, by_gate = parts
    x_sem, out_sem, next_sem, h_sem, keep_sem, dy_sem, turned_sem = take(7)
    n_sems = len(Fetch.scratch(z))
    here = Here(z)
    fetch = Fetch(z, here, [v.at[0] for v in shards], w, take(n_sems), 0, z.NB)
    later = Fetch(z, here, [v.at[1] for v in shards], w_next, take(n_sems), 0, z.early)
    early = range(z.early)
    met = meet(fetch.peers())
    fetch.begin_local()
    load = pltpu.make_async_copy(x_in, xs, x_sem)
    load.start()
    met()
    fetch.begin_pair()

    def fetches(slot):
        for item in FETCHES[slot].split(","):
            who, phase, j = (later if item[0] == "L" else fetch), item.strip("L")[:-1], int(item[-1])
            if phase == "d1" and j == 0:
                who.end_pair()
            getattr(who, "start_" + phase)(j)

    fetches(0)
    load.wait()

    def load_dy(i):
        return pltpu.make_async_copy(dy_in.at[at(i * z.T3, z.T3), :], dy_buf.at[odd(i)], dy_sem.at[odd(i)])

    load_dy(0).start()

    def prepare(i):
        rows = at(i * z.T3, z.T3, LANES)
        pl.when(i + 1 < z.T // z.T3)(lambda: load_dy(i + 1).start())
        value = normed(xs[rows, :].astype(f32))[0]
        a[rows, :] = value
        acc[rows, :] = jnp.zeros((z.T3, z.D), f32)
        load_dy(i).wait()
        for v, part in zip(turned, (value, dy_buf[odd(i)]), strict=True):
            v[:, rows] = part.T

    loop(0, z.T // z.T3, prepare)
    turn = [pltpu.make_async_copy(v, o, turned_sem.at[k]) for k, (v, o) in enumerate(zip(turned, turned_out, strict=True))]
    start(turn)
    fetches(1)
    n = z.T // z.TC

    def keep(j, i):
        slot = odd(i)
        return [pltpu.make_async_copy(v.at[slot], o.at[j, at(i * z.TC, z.TC), :], keep_sem.at[k, slot]) for k, (v, o) in enumerate(zip(parts, kept_out, strict=True))]

    def kept(j, i):
        for copy in keep(j, i):
            copy.wait()

    def serve(j, middle):
        for b in range(z.NB):
            pl.when(j == b)(lambda b=b: fetches(2 + 2 * b + middle))

    def block(j):
        serve(j, 0)
        fetch.ready(j)
        start([pltpu.make_async_copy(v.at[j], o.at[j], out_sem.at[k]) for k, (v, o) in enumerate(zip(w, w_out, strict=True))])

        def chunk(i):
            @pl.when(i == n // 2)
            def _():
                serve(j, 1)

                @pl.when(j == 0)
                def _():
                    later.begin_local()
                    later.begin_pair()


            pl.when(j * n + i > 1)(lambda: kept(j, i))
            rows, slot = at(i * z.TC, z.TC), odd(i)
            for cols in z.halves:
                gate, up = dot(a[rows, :], w[0][j, :, cols]), dot(a[rows, :], w[1][j, :, cols])
                sig = 1.0 / (1.0 + jnp.exp(-gate))
                silu = gate * sig
                act[slot, :, cols] = (silu * up).astype(bf16)
                by_up[slot, :, cols] = silu
                by_gate[slot, :, cols] = up * (sig + silu * (1.0 - sig))
            acc[rows, :] += dot(act[slot], w[2][j])
            start(keep(j, i))

        loop(0, n, chunk)

    loop(0, z.NB, block)

    def finish(i):
        rows = at(i * z.T3, z.T3)
        xs[rows, :] = xs[rows, :] + acc[rows, :].astype(bf16)

    loop(0, z.T // z.T3, finish)
    store = pltpu.make_async_copy(xs, h_out, h_sem)
    store.start()
    for e in early:
        later.ready(e)
    handed = [pltpu.make_async_copy(v, o, next_sem.at[k]) for k, (v, o) in enumerate(zip(w_next, next_out, strict=True))]
    start(handed)
    for i in range(2):
        kept(z.NB - 1, n - 2 + i)
    for k, v in enumerate(w):
        wait(v, out_sem.at[k])
    fetch.end()
    later.end()
    store.wait()
    for copy in (*handed, *turn):
        copy.wait()


class Reduce:
    PHASES = ("p", "x1", "x2", "y", "z", "az", "ay", "f")

    def __init__(self, z, here, units, base, outs, refs):
        self.z, self.here, self.units, self.base, self.outs = z, here, units, base, outs
        (self.stage, self.got_p, self.got_x1, self.got_x2, self.got_y, self.got_z, self.send_x1, self.send_x2, self.send_y, self.send_z, *refs) = refs
        (self.kept_x, self.kept_y, self.kept_z, self.fin, self.down, self.turned, self.out_sem, self.turned_sem, self.piece_sem, *refs) = refs
        self.got = dict(zip(self.PHASES, refs[::2], strict=True))
        self.sent = dict(zip(self.PHASES, refs[1::2], strict=True))

    @classmethod
    def scratch(cls, z, units):
        unit, share = z.unit, z.unit[1:]
        data = [(2, X, CORES, *unit), (3, X, *unit), (2, 2, Y // 2, *share), (2, 2, *unit), (2, *unit), (units, z.Z, 3, 16, LANES)]
        data += [unit, (2, 2, *unit), unit, share]
        wide = [(2, *unit), share, share]
        return (
            [VMEM(shape, bf16) for shape in data]
            + [VMEM(shape, f32) for shape in wide]
            + [VMEM((units, *unit), bf16), VMEM((units, CORES, Y, z.h, LANES), bf16), VMEM((2, LANES, z.D), bf16)]
            + [DMA((2, units)), DMA((2, 2)), DMA]
            + [DMA((units + 3,)) for _ in range(2 * len(cls.PHASES))]
        )

    def peers(self):
        here = self.here
        return (
            [here.partner()] + [here.along_x(k) for k in SIDES] + [here.along_y(k) for k in range(1, Y)] + [here.along_z(k) for k in range(1, here.Z)]
        )

    def which(self, u, m):
        return (u, ALL) if m is None else (self.units + m, m)

    def send(self, phase, i, src, dst, where):
        remote(src, dst, self.sent[phase].at[i], self.got[phase].at[i], where).start()

    def over(self, m, work, begin=0, end=Y):
        def share(y):
            for k in range(len(self.outs)) if m is None else (m,):
                work(y, k)

        loop(begin, end, share)

    def start_p(self, u, m=None, places=range(X)):
        here, (i, mm) = self.here, self.which(u, None if isinstance(m, slice) else m)
        mm = m if isinstance(m, slice) else mm
        for x in places:
            self.send("p", i, self.stage.at[odd(u), x, 1 - here.c, :, mm], self.got_p.at[lax.rem(u, 3), x, :, mm], here.partner())

    def start_early_p(self, u):
        self.start_p(u, slice(0, 2), range(2))

    def start_late_p(self, u):
        self.start_p(u, slice(0, 2), range(2, X))
        self.start_p(u, slice(2, 3))

    def both(self, u, x, y, m):
        return self.stage[odd(u), x, self.here.c, y, m].astype(f32) + self.got_p[lax.rem(u, 3), x, y, m].astype(f32)

    def start_x1(self, u, m=None):
        here, half, slot, (i, mm) = self.here, Y // 2, odd(u), self.which(u, m)
        wait(self.got_p.at[lax.rem(u, 3), :, :, mm], self.got["p"].at[i])
        far = lax.rem(here.x + FAR, X)

        def work(y, k):
            self.send_x1[y, k] = self.both(u, far, y, k).astype(bf16)

        self.over(m, work)
        for side in range(2):
            self.send("x1", i, self.send_x1.at[pl.ds(side * half, half), mm], self.got_x1.at[slot, side, :, mm], here.along_x(SIDES[side]))

    def start_x2(self, u, m=None):
        here, half, slot, (i, mm) = self.here, Y // 2, odd(u), self.which(u, m)
        wait(self.got_x1.at[slot, :, :, mm], self.got["x1"].at[i])
        wait(self.got_x1.at[slot, :, :, mm], self.sent["x1"].at[i])
        wait(self.got_p.at[lax.rem(u, 3), :, :, mm], self.sent["p"].at[i])
        right, left = here.right(), here.left()

        def first(y, k):
            self.send_x2[slot, 0, y, k] = (self.both(u, right, y, k) + self.got_x1[slot, 0, y, k].astype(f32)).astype(bf16)
            self.send_x2[slot, 1, y, k] = self.both(u, left, y, k).astype(bf16)
            self.kept_x[slot, y, k] = self.both(u, here.x, y, k)

        def second(y, k):
            self.send_x2[slot, 0, y, k] = self.both(u, right, y, k).astype(bf16)
            self.send_x2[slot, 1, y, k] = (self.both(u, left, y, k) + self.got_x1[slot, 1, y - half, k].astype(f32)).astype(bf16)
            self.kept_x[slot, y, k] = self.both(u, here.x, y, k)

        self.over(m, first, 0, half)
        self.over(m, second, half, Y)
        for side in range(2):
            self.send("x2", i, self.send_x2.at[slot, side, :, mm], self.got_x2.at[slot, side, :, mm], here.along_x(SIDES[side]))

    def start_y(self, u, m=None):
        here, slot, (i, mm) = self.here, odd(u), self.which(u, m)
        wait(self.got_x2.at[slot, :, :, mm], self.got["x2"].at[i])
        wait(self.got_x2.at[slot, :, :, mm], self.sent["x2"].at[i])

        def total(y, k):
            return self.kept_x[slot, y, k] + self.got_x2[slot, 0, y, k].astype(f32) + self.got_x2[slot, 1, y, k].astype(f32)

        def work(y, k):
            self.send_y[y, k] = total(y, k).astype(bf16)

        def own(_, k):
            self.kept_y[k] = total(here.y, k)

        self.over(m, work)
        self.over(m, own, 0, 1)
        for k in (*SIDES, FAR):
            self.send("y", i, self.send_y.at[lax.rem(here.y + k, Y), mm], self.got_y.at[slot, here.y, mm], here.along_y(k))

    def start_z(self, u, m=None):
        z, here, slot, (i, mm) = self.z, self.here, odd(u), self.which(u, m)
        wait(self.got_y.at[slot, pl.ds(0, Y - 1), mm], self.got["y"].at[i])
        wait(self.got_y.at[slot, pl.ds(0, Y - 1), mm], self.sent["y"].at[i])

        def work(_, k):
            total = self.kept_y[k]
            for place in range(1, Y):
                total += self.got_y[slot, lax.rem(here.y + place, Y), k].astype(f32)
            self.kept_z[k] = total
            self.send_z[k] = total.astype(bf16)

        self.over(m, work, 0, 1)

        def send(k):
            to = lax.rem(here.z + k, z.Z)
            pl.when(to < z.active)(lambda: self.send("z", i, self.send_z.at[mm, at(to * 16, 16), :], self.got_z.at[u, here.z, mm], here.along_z(k)))

        loop(1, z.Z, send)

    def if_active(self, yes, no):
        pl.when(self.here.z < self.z.active)(yes)
        pl.when(self.here.z >= self.z.active)(no)

    def wait_pieces(self, i, mm, n, sem):
        if n:
            wait(self.got_z.at[0, pl.ds(0, n), mm], sem.at[i])

    def mine(self, mm):
        return self.here.y, mm, at(self.here.z * 16, 16)

    def add_pieces(self, u, m):
        z, here, (i, mm) = self.z, self.here, self.which(u, m)
        self.wait_pieces(i, mm, z.active - 1, self.sent["z"])
        self.wait_pieces(i, mm, z.Z - 1, self.got["z"])
        y, mm, rows = self.mine(mm)
        total = self.kept_z[mm, rows, :]
        for k in range(1, z.Z):
            total += self.got_z[u, lax.rem(here.z + k, z.Z), mm].astype(f32)
        self.fin[u, y, mm, rows, :] = total.astype(bf16)

    def send_pieces(self, u, m=None):
        i, mm = self.which(u, m)
        y, mm, rows = self.mine(mm)
        piece = self.fin.at[u, y, mm, rows, :]
        loop(1, self.z.Z, lambda k: self.send("az", i, piece, piece, self.here.along_z(k)))

    def start_az(self, u, m=None):
        i, mm = self.which(u, m)

        def yes():
            self.add_pieces(u, m)
            self.send_pieces(u, m)

        self.if_active(yes, lambda: self.wait_pieces(i, mm, self.z.active, self.sent["z"]))

    def hand_on(self, u, out):
        def yes():
            self.add_pieces(u, None)
            y, mm, rows = self.mine(ALL)
            copy = pltpu.make_async_copy(self.fin.at[u, y, mm, rows, :], out, self.piece_sem)
            copy.start()
            copy.wait()

        self.if_active(yes, lambda: self.wait_pieces(u, ALL, self.z.active, self.sent["z"]))

    def take_over(self, u, piece):
        def yes():
            y, mm, rows = self.mine(ALL)
            copy = pltpu.make_async_copy(piece, self.fin.at[u, y, mm, rows, :], self.piece_sem)
            copy.start()
            copy.wait()
            self.send_pieces(u)

        pl.when(self.here.z < self.z.active)(yes)

    def start_ay(self, u, m=None):
        z, here, (i, mm) = self.z, self.here, self.which(u, m)
        self.if_active(lambda: self.wait_pieces(i, mm, z.active - 1, self.got["az"]), lambda: self.wait_pieces(i, mm, z.active, self.got["az"]))
        share = self.fin.at[u, here.y, mm]
        for k in (*SIDES, FAR):
            self.send("ay", i, share, share, here.along_y(k))

    def place(self, u):
        nb = self.z.NB
        return (1, u) if self.base == 0 else (1 - lax.div(u + nb - self.base, nb), lax.rem(u + nb - self.base, nb))

    def start_f(self, u, m=None):
        z, c, (i, mm) = self.z, self.here.c, self.which(u, m)
        layer, j = self.place(u)
        wait(self.fin.at[u, pl.ds(0, Y - 1), mm], self.got["ay"].at[i])
        for k in range(2) if m is None else (m,):
            if k == 2:
                break
            for y in range(Y):
                out = self.outs[k].at[layer, :, at((y * z.NB + j) * LANES, LANES, LANES)]
                pltpu.make_async_copy(self.fin.at[u, y, k], out, self.out_sem.at[k, u]).start()
        if m in (None, 2):
            self.down[u, c] = self.fin[u, :, 2]
            self.send("f", u, self.fin.at[u, :, 2], self.down.at[u, c], self.here.partner())

    def finish(self, u):
        z, c = self.z, self.here.c
        layer, j = self.place(u)
        wait(self.down.at[u, 0], self.got["f"].at[u])
        slot = odd(u)
        pl.when(u > 1)(lambda: self.turned_out(u - 2, "wait"))
        self.turned[slot] = self.down[u].reshape(z.D, LANES).T
        self.turned_out(u, "start")

    def turned_out(self, u, what):
        z, c = self.z, self.here.c
        layer, j = self.place(u)
        for half in range(2):
            row = 2 * j + half

            @pl.when(lax.div(row, z.NB) == c)
            def _(half=half, row=row):
                out = self.outs[2].at[layer, at(lax.rem(row, z.NB) * 64, 64), :]
                getattr(pltpu.make_async_copy(self.turned.at[odd(u), pl.ds(half * 64, 64), :], out, self.turned_sem.at[odd(u), half]), what)()

    def end(self, units, in_parts):
        z = self.z

        def sent_back(i, mm):
            self.if_active(lambda: self.wait_pieces(i, mm, z.Z - 1, self.sent["az"]), lambda: None)
            wait(self.fin.at[0, pl.ds(0, Y - 1), mm], self.sent["ay"].at[i])

        def one(u):
            wait(self.down.at[0, 0], self.sent["f"].at[u])
            for m in range(2):
                wait(self.down.at[0, 0], self.out_sem.at[m, u])

        loop(0, units, one)
        loop(0, units - in_parts, lambda u: sent_back(u, ALL))
        for m in range(len(self.outs) if in_parts else 0):
            sent_back(self.units + m, m)
        for u in range(max(0, units - 2), units):
            self.turned_out(u, "wait")


def backward_kernel(z, first, *refs):
    T, TC, T3, NB, FB, D = z.T, z.TC, z.T3, z.NB, z.FB, z.D
    here = Here(z)
    refs = list(refs)

    def take(n):
        out, refs[:] = refs[:n], refs[n:]
        return out

    h_in, dh_in, dh_t_in, w0, w1, w2 = take(6)
    if first:
        early_in = take(3)
    else:
        left_in, piece_in, by_up_in, by_gate_in, act_in, a_t_in = take(6)
        take(3)
    dx_out, *outs = take(4)
    spill = take(1)[0]
    if first:
        left_out, piece_out, dx_t_out = take(3)
    dx_buf, h_buf, a_t, dh, dh_t, wg, wu, wd, work = take(9)
    ld_sem, dh_sem, w_sem, sp_sem, s3_sem, o_sem, left_sem, turned_sem = take(8)
    if first:
        a, dx_t_buf, dx_t_sem = take(3)
    else:
        saved, saved_sem, act_sem = take(3)
    if first:
        fetch = Fetch(z, here, (w0.at[1], w1.at[1], w2.at[1]), (wg, wu, wd), take(len(Fetch.scratch(z))), z.early, NB)
        w0, w1, w2 = early_in
    base = 0 if first else 2
    units = NB - 1 if first else NB + base
    reduce = Reduce(z, here, units, base, outs, refs)
    met = meet(reduce.peers())
    whole = pltpu.make_async_copy(dh_in, dh, dh_sem)
    whole.start()

    def load_h(i):
        return pltpu.make_async_copy(h_in.at[at(i * T3, T3), :], h_buf.at[odd(i)], ld_sem.at[odd(i)])

    turn = [pltpu.make_async_copy(dh_t_in, dh_t, turned_sem.at[0])]
    if first:
        load_h(0).start()
        start(turn)
    else:
        turn.append(pltpu.make_async_copy(a_t_in, a_t, turned_sem.at[1]))

    def loads(j):
        return [pltpu.make_async_copy(src.at[j], dst.at[j], w_sem.at[k, j]) for k, (src, dst) in enumerate(((w0, wg), (w1, wu), (w2, wd)))]

    TS, slots = z.TS, z.slots

    def load_saved(q):
        j, rows, slot = lax.div(q, T // TS), at(lax.rem(q, T // TS) * TS, TS), lax.rem(q, slots)
        return [pltpu.make_async_copy(v.at[j, rows, :], saved.at[slot, k], saved_sem.at[k, slot]) for k, v in enumerate((by_up_in, by_gate_in))]

    def load_act(j):
        return pltpu.make_async_copy(act_in.at[j], work.at[pl.ds(0, T), :], act_sem)

    if first:
        for j in range(z.early):
            start(loads(j))
        fetch.begin_local()
        met()
        fetch.begin_pair()
        fetch.start_a1(z.early)
    else:
        left = pltpu.make_async_copy(left_in, reduce.stage.at[1], left_sem)
        left.start()
        start(loads(0)[2:])
        for q in range(slots - 1):
            start(load_saved(q))
        start(turn)
        for j in range(1, NB):
            start(loads(j)[2:])
        for j in range(NB):
            start(loads(j)[:2])
    whole.wait()
    n3 = T // T3

    def prepare(i):
        rows = at(i * T3, T3, LANES)
        pl.when(i + 1 < n3)(lambda: load_h(i + 1).start())
        load_h(i).wait()
        value = normed(h_buf[odd(i)].astype(f32))[0]
        a[rows, :] = value
        a_t[:, rows] = value.T

    if not first:
        met()
        left.wait()
        reduce.start_p(1)
        reduce.take_over(0, piece_in)
    def turned():
        for copy in turn:
            copy.wait()

    if first:
        loop(0, n3, prepare)
        turned()
        fetch.end_pair()
        fetch.start_a2(z.early)

    def product(k, rows, cols):
        return work.at[at(k * T + rows.start, rows.size), cols]

    def spills(j):
        return [pltpu.make_async_copy(work.at[pl.ds((1 + k) * T, T), :], spill.at[k, j], sp_sem.at[k]) for k in range(2)]

    def spilled(j):
        for copy in spills(j):
            copy.wait()

    def step(name, u, m=None):
        do = getattr(reduce, "start_" + name)
        back = name in ("ay", "az")
        begin = 0 if first or name == "ay" else 1
        end = units - 1 if first and back else units
        if isinstance(u, int):
            if begin <= u < end:
                do(u, m)
        else:
            pl.when(jnp.logical_and(u >= begin, u < end))(lambda: do(u))

    def halfway(i, n, before, after):
        if n == 1:
            before()
            after()
        else:
            pl.when(i == 0)(before)
            pl.when(i == n // 2)(after)

    def loaded(j):
        for copy in loads(j):
            copy.wait()

    def block(j):
        u = j + base - 1
        if first:
            fetch.serve_a(j)
            pl.when(j < z.early)(lambda: loaded(j))
            pl.when(j >= z.early)(lambda: fetch.ready(j))
        else:
            load_act(j).start()
            loads(j)[2].wait()
        pl.when(j > 0)(lambda: spilled(j - 1))

        def at_0():
            step("x2", u - 1)

        def at_1():
            step("z", u - 2)
            step("ay", u - 3)

        def at_2():
            if first:
                fetch.serve_b(j)
            else:
                pl.when(j == 0)(turned)
            step("x1", u)

        def at_3():
            if first:
                step("early_p", j)
            else:
                pl.when(j + 1 < NB)(lambda: reduce.start_early_p(j + base))
            step("y", u - 1)
            step("az", u - 2)

        def piece(i):
            halfway(i, T // TS, at_0, at_1)
            q, rows = j * (T // TS) + i, at(i * TS, TS)
            pl.when(q + slots - 1 < NB * (T // TS))(lambda: start(load_saved(q + slots - 1)))
            for copy in load_saved(q):
                copy.wait()
            by_act = dot(dh[rows, :], wd[j], ((1,), (1,))).astype(bf16).astype(f32)
            slot = lax.rem(q, slots)
            product(1, rows, ALL)[...] = (by_act * saved[slot, 1]).astype(bf16)
            product(2, rows, ALL)[...] = (by_act * saved[slot, 0]).astype(bf16)

        def chunk(i):
            halfway(i, T // TC, at_0, at_1)
            rows = at(i * TC, TC)
            for cols in z.halves:
                gate, up = dot(a[rows, :], wg[j, :, cols]), dot(a[rows, :], wu[j, :, cols])
                by_act = dot(dh[rows, :], wd[j, cols, :], ((1,), (1,))).astype(bf16).astype(f32)
                sig = 1.0 / (1.0 + jnp.exp(-gate))
                silu = gate * sig
                product(0, rows, cols)[...] = (silu * up).astype(bf16)
                product(1, rows, cols)[...] = (by_act * up * (sig + silu * (1.0 - sig))).astype(bf16)
                product(2, rows, cols)[...] = (by_act * silu).astype(bf16)

        if first:
            loop(0, T // TC, chunk)
        else:
            loop(0, T // TS, piece)
            load_act(j).wait()
        start(spills(j))
        stage, slot, m = reduce.stage, odd(j + base), D // 2

        def rows_of(i):
            halfway(i, 2, at_2, at_3)
            rows = at(i * m, m)
            gates = dot(a_t[rows, :], work[pl.ds(T, T), :]).astype(bf16)
            ups = dot(a_t[rows, :], work[pl.ds(2 * T, T), :]).astype(bf16)
            downs = dot(dh_t[rows, :], work[pl.ds(0, T), :]).astype(bf16)
            for y in range(Y):
                lanes = slice(y * LANES, (y + 1) * LANES)
                for x in range(X // 2):
                    for c in range(CORES):
                        part = slice((x * CORES + c) * z.h, (x * CORES + c + 1) * z.h)
                        stage[slot, i * (X // 2) + x, c, y, 0] = gates[part, lanes]
                        stage[slot, i * (X // 2) + x, c, y, 1] = ups[part, lanes]
                for x in range(X):
                    stage[slot, x, i, y, 2] = downs[y * z.h : (y + 1) * z.h, x * LANES : (x + 1) * LANES]

        loop(0, 2, rows_of)
        if first:
            step("late_p", j)
        else:
            pl.when(j + 1 < NB)(lambda: reduce.start_late_p(j + base))

            @pl.when(j + 1 == NB)
            def _():
                for m in range(3):
                    reduce.start_p(NB + base - 1, m)

    loop(0, NB, block)
    if first:
        left = pltpu.make_async_copy(reduce.stage.at[(NB - 1) % 2], left_out, left_sem)
        left.start()
    spilled(NB - 1)

    def load_3(i):
        slot, rows = odd(i), at(i * T3, T3)
        out = [load_h(i)]
        for k in range(2):
            for j in range(NB):
                out.append(pltpu.make_async_copy(spill.at[k, j, rows, :], work.at[at(((slot * 2 + k) * NB + j) * T3, T3), :], s3_sem.at[slot]))
        return out

    def store_3(i):
        return pltpu.make_async_copy(dx_buf.at[odd(i)], dx_out.at[at(i * T3, T3), :], o_sem.at[odd(i)])

    def store_turned(i):
        return pltpu.make_async_copy(dx_t_buf.at[odd(i)], dx_t_out.at[:, at(i * T3, T3, LANES)], dx_t_sem.at[odd(i)])

    start(load_3(0))
    u = NB + base - 1
    if first:
        todo = ("x2:1", "z:2,ay:3", "", "az:2,y:1", "", "ay:2,z:1", "", "")
    else:
        todo = (
            "x2:1,ay:3",
            "x1.0,x1.1,z:2",
            "x1.2",
            "x2.0,az:2,y:1,x2.1",
            "x2.2,ay:2",
            "z:1,y.0,y.1",
            "y.2,az:1,z.0,z.1",
            "z.2,ay:1,az.0",
            "az.1,az.2,ay.0,ay.1,ay.2",
        )

    def steps(text):
        for item in filter(None, text.split(",")):
            name, _, behind = item.partition(":")
            if behind:
                step(name, u - int(behind))
            else:
                name, _, m = item.partition(".")
                step(name, u, int(m))

    done = units - 2 if first else units - 4

    def rows_back(i):
        slot, rows = odd(i), at(i * T3, T3)
        pl.when(i + 1 < n3)(lambda: start(load_3(i + 1)))
        for when, text in enumerate(todo[:n3]):
            pl.when(i == when)(lambda text=text: steps(text))

        @pl.when(i == n3 - 2)
        def _():
            loop(0, done, reduce.start_f)

        @pl.when(i == n3 - 1)
        def _():
            loop(0, done, reduce.finish)

        if not first:

            @pl.when(i == 0)
            def _():
                for j in range(NB):
                    for copy in loads(j)[:2]:
                        copy.wait()

        load_h(i).wait()
        wait(work.at[at(slot * 2 * NB * T3, 2 * NB * T3), :], s3_sem.at[slot])
        pl.when(i > 1)(lambda: store_3(i - 2).wait())
        back = []
        for k, w in ((0, wg), (1, wu)):
            total = None
            for j in range(NB):
                part = dot(work[at(((slot * 2 + k) * NB + j) * T3, T3), :], w[j], ((1,), (1,)))
                total = part if total is None else total + part
            back.append(total.astype(bf16))
        by_a = (back[0] + back[1]).astype(f32)
        wide = h_buf[slot].astype(f32)
        square = jnp.mean(wide * wide, -1, keepdims=True) + 1e-6
        scale = lax.rsqrt(square)
        by_scale = jnp.sum(by_a * wide, -1, keepdims=True)
        by_square = by_scale * (-0.5 * scale / square) * (2.0 / D)
        dx_buf[slot] = dh[rows, :] + (by_a * scale + by_square * wide).astype(bf16)
        store_3(i).start()
        if first:
            pl.when(i > 1)(lambda: store_turned(i - 2).wait())
            dx_t_buf[slot] = dx_buf[slot].T
            store_turned(i).start()

    loop(0, n3, rows_back)
    assert n3 == 8
    for text in todo[n3:]:
        steps(text)
    if first:
        reduce.hand_on(units - 1, piece_out)
    back = units - 1 if first else units
    for v in range(done, back):
        if first or v + 1 < back:
            reduce.start_f(v)
        else:
            for m in range(3):
                reduce.start_f(v, m)
    for v in range(done, back):
        reduce.finish(v)
    reduce.end(back, 0 if first else 1)
    if first:
        fetch.end()
        left.wait()
    for i in range(max(0, n3 - 2), n3):
        store_3(i).wait()
        if first:
            store_turned(i).wait()


def call(body, out, n_in, scratch, number, aliases=()):
    return pl.pallas_call(
        body,
        out_shape=out,
        in_specs=[pl.BlockSpec(memory_space=HBM)] * n_in,
        out_specs=[pl.BlockSpec(memory_space=HBM)] * len(out),
        scratch_shapes=scratch,
        input_output_aliases=dict(aliases),
        compiler_params=pltpu.CompilerParams(collective_id=number, has_side_effects=True, vmem_limit_bytes=66_900_000),
    )


def forward(z, x, dy, shards):
    S = jax.ShapeDtypeStruct
    wide, tall, tokens, hidden, piece = (z.NB, z.D, z.FB), (z.NB, z.FB, z.D), (z.T, z.D), (z.NB, z.T, z.FB), (2, z.TC, z.FB)
    scratch = [VMEM(tokens, bf16), VMEM(tokens, f32), VMEM(tokens, bf16), VMEM((2, z.T3, z.D), bf16), VMEM(tokens[::-1], bf16), VMEM(tokens[::-1], bf16)]
    scratch += [VMEM(piece, bf16), VMEM(piece, f32), VMEM(piece, f32)]
    early = [(z.early, *shape[1:]) for shape in (wide, wide, tall)]
    scratch += [VMEM(shape, bf16) for shape in (wide, wide, tall, *early)]
    scratch += [DMA, DMA((3,)), DMA((3,)), DMA, DMA((3, 2)), DMA((2,)), DMA((2,))] + Fetch.scratch(z) + Fetch.scratch(z)
    out = [S(tokens, bf16), S(wide, bf16), S(wide, bf16), S(tall, bf16), S(hidden, bf16), S(hidden, f32), S(hidden, f32)]
    out += [S(shape, bf16) for shape in (*early, tokens[::-1], tokens[::-1])]
    h, *out = call(functools.partial(forward_kernel, z), out, 5, scratch, 0)(x, dy, *shards)
    return h, out[:3], out[3:6], out[6:9], out[9:]


def backward(z, h, dh, dh_t, w, more, first):
    S = jax.ShapeDtypeStruct
    wide, tall, tokens = (z.NB, z.D, z.FB), (z.NB, z.FB, z.D), (z.T, z.D)
    units = z.NB - 1 if first else z.NB + 2
    scratch = [VMEM((2, z.T3, z.D), bf16), VMEM((2, z.T3, z.D), bf16)]
    scratch += [VMEM(tokens[::-1], bf16), VMEM(tokens, bf16), VMEM(tokens[::-1], bf16)]
    scratch += [VMEM(wide, bf16), VMEM(wide, bf16), VMEM(tall, bf16), VMEM((max(3 * z.T, 4 * z.NB * z.T3), z.FB), bf16)]
    scratch += [DMA((2,)), DMA, DMA((3, z.NB)), DMA((2,)), DMA((2,)), DMA((2,)), DMA, DMA((2,))]
    if first:
        scratch += [VMEM(tokens, bf16), VMEM((2, z.D, z.T3), bf16), DMA((2,))] + Fetch.scratch(z)
    else:
        scratch += [VMEM((z.slots, 2, z.TS, z.FB), f32), DMA((2, z.slots)), DMA]
    scratch += Reduce.scratch(z, units)
    grads = [S((2, z.h, z.F), bf16), S((2, z.h, z.F), bf16), S((2, z.F // (X * CORES), z.D), bf16)]
    out = [S(tokens, bf16), *grads, S((2, z.NB, z.T, z.FB), bf16)]
    if first:
        out += [S((X, CORES, *z.unit), bf16), S((3, 16, LANES), bf16), S(tokens[::-1], bf16)]
    args = (h, dh, dh_t, *w, *more)
    aliases = {} if first else {len(args) - 3 + i: 1 + i for i in range(3)}
    dx, g, u, d, _, *left = call(functools.partial(backward_kernel, z, first), out, len(args), scratch, 1 if first else 2, aliases)(*args)
    return dx, (g, u, d), left


def solution(mesh):
    def step(x, dy, *weights):
        z = Sizes(mesh, x.shape[1], x.shape[2], weights[0].shape[2])
        h, w, (act, by_up, by_gate), early, (a_t, dy_t) = forward(z, x[0], dy[0], weights)
        dh, grads, (left, piece, dh_t) = backward(z, h, dy[0], dy_t, weights, early, True)
        dx, grads, _ = backward(z, x[0], dh, dh_t, w, (left, piece, by_up, by_gate, act, a_t, *grads), False)
        return dx[None], *grads

    states, cut = P(("rep", "r", "s"), None, None), P(None, "s", None)
    return jax.shard_map(
        step,
        mesh=mesh,
        in_specs=(states, states) + (cut,) * 3,
        out_specs=(states,) + (P("rep", "s", None),) * 3,
        check_vma=False,
    )
```

```python
import functools

import jax
import jax.numpy as jnp
from jax import lax
from jax.experimental import pallas as pl
from jax.experimental.pallas import tpu as pltpu
from jax.sharding import PartitionSpec as P

f32, bf16 = jnp.float32, jnp.bfloat16
MESH = pl.DeviceIdType.MESH
LANES = 128
X, CORES, Y = 4, 2, 4
HBM, VMEM, DMA = pl.ANY, pltpu.VMEM, pltpu.SemaphoreType.DMA


def dot(a, b, dims=((1,), (0,))):
    return lax.dot_general(a, b, (dims, ((), ())), preferred_element_type=f32)


def at(start, size, multiple=16):
    return pl.ds(pl.multiple_of(start, multiple) if not isinstance(start, int) else start, size)


ALL = slice(None)
LEFT, RIGHT, FAR = 3, 1, 2
SIDES = (RIGHT, LEFT)


def loop(begin, end, body):
    def one(i, carry):
        body(i)
        return carry

    lax.fori_loop(begin, end, one, 0)


def odd(i):
    return lax.rem(i, 2)


class Sizes:
    chunk, piece, rows, slots = 1024, 512, 256, 4

    def __init__(self, mesh, tokens, d, ff):
        self.R = mesh.shape["r"]
        self.Z = self.R // Y
        self.T, self.D, self.F = tokens, d, ff
        self.NB = ff // (X * LANES)
        self.FB = X * LANES
        self.h = d // (X * CORES)
        self.TC = min(self.chunk, tokens)
        self.T3 = min(self.rows, tokens)
        self.TS = min(self.piece, tokens)
        self.unit = (Y, 3, self.h, LANES)
        self.active = self.h // 16
        self.halves = (slice(0, self.FB // 2), slice(self.FB // 2, self.FB))
        self.early = self.NB // 2
        assert self.h % 16 == 0 and self.active <= self.Z and mesh.shape["s"] == X * CORES


class Here:
    def __init__(self, z):
        s, self.r = lax.axis_index("s"), lax.axis_index("r")
        self.x, self.c = lax.div(s, CORES), lax.rem(s, CORES)
        self.y, self.z, self.Z = lax.div(self.r, z.Z), lax.rem(self.r, z.Z), z.Z
        self.R = z.R

    def partner(self):
        return {"s": self.x * CORES + 1 - self.c}

    def along_x(self, k):
        return {"s": lax.rem(self.x + k, X) * CORES + self.c}

    def along_y(self, k):
        return {"r": lax.rem(self.y + k, Y) * self.Z + self.z}

    def right(self):
        return lax.rem(self.x + RIGHT, X)

    def left(self):
        return lax.rem(self.x + LEFT, X)

    def along_z(self, k):
        return {"r": self.y * self.Z + lax.rem(self.z + k, self.Z)}


def remote(src, dst, sent, got, where):
    return pltpu.make_async_remote_copy(src_ref=src, dst_ref=dst, send_sem=sent, recv_sem=got, device_id=where, device_id_type=MESH)


def start(copies):
    for copy in copies:
        copy.start()


def wait(ref, sem):
    pltpu.make_async_copy(ref, ref, sem).wait()


def meet(peers):
    barrier = pltpu.get_barrier_semaphore()
    for peer in peers:
        pl.semaphore_signal(barrier, inc=1, device_id=peer, device_id_type=MESH)
    return lambda: pl.semaphore_wait(barrier, len(peers))


FETCHES = (
    "a10,a11,a20,d10,b10,d11,a21",
    "d20,a12,a14,b20,a13,e0,b11,d21,c0,a22,d12",
    "e1,a23,d13,a24,b21,b12",
    "d22,c1,d14,b13",
    "d23,La11,e2,La10,b22",
    "b23,b14,La21,d24,c2,Ld10,Ld11",
    "e4,c3,Lb11",
    "e3,La20,Ld21,b24",
    "Lb10",
    "Ld20,c4,Lb21",
    "Lb20,Le0,Le1,Lc1",
    "Lc0",
)


class Fetch:
    PHASES = ("a1", "a2", "b1", "b2", "c", "d1", "d2", "e")

    def __init__(self, z, here, shards, w, sems, begin, end):
        self.z, self.here, self.shards, self.w, self.first, self.last = z, here, shards, w, begin, end
        self.local, self.local_d, self.pair, self.pair_sent = sems[:4]
        self.got = dict(zip(self.PHASES, sems[4::2]))
        self.sent = dict(zip(self.PHASES, sems[5::2]))
        self.parts = [[k for k in range(z.NB) if begin <= (c * z.NB + k) // 2 < end] for c in range(CORES)]

    @classmethod
    def scratch(cls, z):
        return [DMA((z.NB,)), DMA, DMA, DMA] + [DMA((z.NB,)) for _ in range(2 * len(cls.PHASES))]

    def peers(self):
        here = self.here
        return [here.partner()] + [here.along_x(k) for k in SIDES] + [here.along_y(k) for k in SIDES]

    def own(self, j):
        z, here = self.z, self.here
        for shard, w in zip(self.shards[:2], self.w[:2]):
            for l in range(X):
                slot = w.at[j, self.rows(here.x), pl.ds(l * LANES, LANES)]
                pltpu.make_async_copy(shard.at[:, at((l * z.NB + j) * LANES, LANES, LANES)], slot, self.local.at[j]).start()

    def each_core(self, do):
        for c in range(CORES):
            pl.when(self.here.c == c)(lambda c=c: do(self.parts[c], self.parts[1 - c]))

    def part(self, k):
        z, here = self.z, self.here
        place = here.c * z.NB + k
        return self.shards[2].at[pl.ds(64 * k, 64), :], self.w[2].at[lax.div(place, 2), at(here.x * LANES + odd(place) * 64, 64), :]

    def rows(self, x):
        return at(x * (CORES * self.z.h) + self.here.c * self.z.h, self.z.h)

    def lanes(self, y):
        return at(y * LANES, LANES, LANES)

    def down(self, x, begin=0, size=64):
        return at(x * LANES + self.here.c * 64 + begin, size)

    def send(self, phase, j, w, rows, lanes, where):
        slot = self.w[w].at[j, rows, lanes]
        remote(slot, slot, self.sent[phase].at[j], self.got[phase].at[j], where).start()

    def begin_local(self):
        for j in range(self.first, self.last):
            self.own(j)

        def do(mine, _):
            for k in mine:
                pltpu.make_async_copy(*self.part(k), self.local_d).start()

        self.each_core(do)

    def begin_pair(self):
        def do(mine, _):
            for k in mine:
                src, slot = self.part(k)
                remote(src, slot, self.pair_sent, self.pair, self.here.partner()).start()

        self.each_core(do)

    def wait_parts(self, n, sem):
        if n:
            wait(self.halves(0, n), sem)

    def end_pair(self):
        def do(mine, other):
            self.wait_parts(len(mine), self.local_d)
            self.wait_parts(len(other), self.pair)

        self.each_core(do)

    def start_a1(self, j):
        here = self.here
        wait(self.pieces(j, 8), self.local.at[j])
        for k in SIDES:
            for w in range(2):
                self.send("a1", j, w, self.rows(here.x), self.lanes(here.y), here.along_x(k))

    def start_d1(self, j):
        for k in SIDES:
            self.send("d1", j, 2, self.down(self.here.x), ALL, self.here.along_x(k))

    def start_a2(self, j):
        here = self.here
        wait(self.pieces(j, 4), self.got["a1"].at[j])
        lanes = self.lanes(here.y)
        self.send("a2", j, 0, self.rows(here.left()), lanes, here.along_x(RIGHT))
        self.send("a2", j, 1, self.rows(here.right()), lanes, here.along_x(LEFT))

    def start_d2(self, j):
        here = self.here
        wait(self.halves(j, 2), self.got["d1"].at[j])
        self.send("d2", j, 2, self.down(here.left(), 0, 32), ALL, here.along_x(RIGHT))
        self.send("d2", j, 2, self.down(here.right(), 32, 32), ALL, here.along_x(LEFT))

    def start_b1(self, j):
        here = self.here
        wait(self.pieces(j, 2), self.got["a2"].at[j])
        for k in SIDES:
            for m in range(1, X):
                for w in range(2):
                    self.send("b1", j, w, self.rows(lax.rem(here.x + m, X)), self.lanes(here.y), here.along_y(k))

    def start_b2(self, j):
        here = self.here
        wait(self.pieces(j, 12), self.got["b1"].at[j])
        for m in range(1, X):
            rows = self.rows(lax.rem(here.x + m, X))
            self.send("b2", j, 0, rows, self.lanes(lax.rem(here.y + LEFT, Y)), here.along_y(RIGHT))
            self.send("b2", j, 1, rows, self.lanes(lax.rem(here.y + RIGHT, Y)), here.along_y(LEFT))

    def start_c(self, j):
        wait(self.pieces(j, 6), self.got["b2"].at[j])
        for w in range(2):
            for x in range(X):
                self.send("c", j, w, self.rows(x), ALL, self.here.partner())

    def start_e(self, j):
        wait(self.halves(j, 1), self.got["d2"].at[j])
        for m in range(1, X):
            self.send("e", j, 2, self.down(lax.rem(self.here.x + m, X)), ALL, self.here.partner())

    def pieces(self, j, n):
        high = 6 if n % 6 == 0 else min(n, 8)
        return self.w[0].at[j, pl.ds(0, high * self.z.h), pl.ds(0, n // high * LANES)]

    def halves(self, j, n):
        return self.w[2].at[j, pl.ds(0, 64 * n), :]

    def ready(self, j):
        wait(self.w[0].at[j], self.got["c"].at[j])
        wait(self.halves(j, 3), self.got["e"].at[j])

    def serve_a(self, j):
        @self.if_mine(j + 1)
        def _():
            self.start_b2(j + 1)
            self.start_d2(j + 1)

        @self.if_mine(j + 2)
        def _():
            self.start_b1(j + 2)
            self.start_d1(j + 2)

        self.if_mine(j + 3)(lambda: self.start_a1(j + 3))

    def serve_b(self, j):
        @self.if_mine(j + 1)
        def _():
            self.start_c(j + 1)
            self.start_e(j + 1)

        self.if_mine(j + 3)(lambda: self.start_a2(j + 3))

    def if_mine(self, j):
        return pl.when(jnp.logical_and(j >= self.first, j < self.last))

    def end(self):
        self.each_core(lambda mine, _: self.wait_parts(len(mine), self.pair_sent))

        def drain(j):
            for phase, n in (("a1", 4), ("a2", 2), ("b1", 12), ("b2", 6)):
                wait(self.pieces(j, n), self.sent[phase].at[j])
            for phase, n in (("d1", 2), ("d2", 1), ("e", 3)):
                wait(self.halves(j, n), self.sent[phase].at[j])
            wait(self.w[0].at[j], self.sent["c"].at[j])

        loop(self.first, self.last, drain)


def normed(wide):
    scale = lax.rsqrt(jnp.mean(wide * wide, -1, keepdims=True) + 1e-6)
    return (wide * scale).astype(bf16), scale


def forward_kernel(z, *refs):
    refs = list(refs)

    def take(n):
        out, refs[:] = refs[:n], refs[n:]
        return out

    x_in, dy_in, *shards = take(5)
    h_out, *w_out = take(4)
    kept_out, next_out, turned_out = take(3), take(3), take(2)
    a, acc, xs, dy_buf = take(4)
    turned = take(2)
    parts, w, w_next = take(3), take(3), take(3)
    act, by_up, by_gate = parts
    x_sem, out_sem, next_sem, h_sem, keep_sem, dy_sem, turned_sem = take(7)
    n_sems = len(Fetch.scratch(z))
    here = Here(z)
    fetch = Fetch(z, here, [v.at[0] for v in shards], w, take(n_sems), 0, z.NB)
    later = Fetch(z, here, [v.at[1] for v in shards], w_next, take(n_sems), 0, z.early)
    early = range(z.early)
    met = meet(fetch.peers())
    fetch.begin_local()
    load = pltpu.make_async_copy(x_in, xs, x_sem)
    load.start()
    met()
    fetch.begin_pair()

    def fetches(slot):
        for item in FETCHES[slot].split(","):
            who, phase, j = (later if item[0] == "L" else fetch), item.strip("L")[:-1], int(item[-1])
            if phase == "d1" and j == 0:
                who.end_pair()
            getattr(who, "start_" + phase)(j)

    fetches(0)
    load.wait()

    def load_dy(i):
        return pltpu.make_async_copy(dy_in.at[at(i * z.T3, z.T3), :], dy_buf.at[odd(i)], dy_sem.at[odd(i)])

    load_dy(0).start()
    n3 = z.T // z.T3

    def prepare(i):
        rows = at(i * z.T3, z.T3)
        a[rows, :] = normed(xs[rows, :].astype(f32))[0]
        acc[rows, :] = jnp.zeros((z.T3, z.D), f32)

    loop(0, n3, prepare)
    fetches(1)

    def turn(i):
        rows = at(i * z.T3, z.T3, LANES)
        pl.when(i + 1 < n3)(lambda: load_dy(i + 1).start())
        load_dy(i).wait()
        for v, part in zip(turned, (a[rows, :], dy_buf[odd(i)])):
            v[:, rows] = part.T

    loop(0, n3, turn)
    sent = [pltpu.make_async_copy(v, o, turned_sem.at[k]) for k, (v, o) in enumerate(zip(turned, turned_out))]
    start(sent)
    n = z.T // z.TC

    def keep(j, i):
        slot = odd(i)
        return [pltpu.make_async_copy(v.at[slot], o.at[j, at(i * z.TC, z.TC), :], keep_sem.at[k, slot]) for k, (v, o) in enumerate(zip(parts, kept_out))]

    def kept(j, i):
        for copy in keep(j, i):
            copy.wait()

    def serve(j, middle):
        for b in range(z.NB):
            pl.when(j == b)(lambda b=b: fetches(2 + 2 * b + middle))

    def block(j):
        serve(j, 0)
        fetch.ready(j)
        start([pltpu.make_async_copy(v.at[j], o.at[j], out_sem.at[k]) for k, (v, o) in enumerate(zip(w, w_out))])

        def chunk(i):
            @pl.when(i == n // 2)
            def _():
                serve(j, 1)

                @pl.when(j == 0)
                def _():
                    later.begin_local()
                    later.begin_pair()


            pl.when(j * n + i > 1)(lambda: kept(j, i))
            rows, slot = at(i * z.TC, z.TC), odd(i)
            for cols in z.halves:
                gate, up = dot(a[rows, :], w[0][j, :, cols]), dot(a[rows, :], w[1][j, :, cols])
                sig = 1.0 / (1.0 + jnp.exp(-gate))
                silu = gate * sig
                act[slot, :, cols] = (silu * up).astype(bf16)
                by_up[slot, :, cols] = silu
                by_gate[slot, :, cols] = up * (sig + silu * (1.0 - sig))
            acc[rows, :] += dot(act[slot], w[2][j])
            start(keep(j, i))

        loop(0, n, chunk)

    loop(0, z.NB, block)

    def finish(i):
        rows = at(i * z.T3, z.T3)
        xs[rows, :] = xs[rows, :] + acc[rows, :].astype(bf16)

    loop(0, z.T // z.T3, finish)
    store = pltpu.make_async_copy(xs, h_out, h_sem)
    store.start()
    for e in early:
        later.ready(e)
    handed = [pltpu.make_async_copy(v, o, next_sem.at[k]) for k, (v, o) in enumerate(zip(w_next, next_out))]
    start(handed)
    for i in range(2):
        kept(z.NB - 1, n - 2 + i)
    for k, v in enumerate(w):
        wait(v, out_sem.at[k])
    fetch.end()
    later.end()
    store.wait()
    for copy in (*handed, *sent):
        copy.wait()


class Reduce:
    PHASES = ("p", "x1", "x2", "y", "z", "az", "ay", "f")

    def __init__(self, z, here, units, base, outs, refs):
        self.z, self.here, self.units, self.base, self.outs = z, here, units, base, outs
        (self.stage, self.got_p, self.got_x1, self.got_x2, self.got_y, self.got_z, self.send_x1, self.send_x2, self.send_y, self.send_z, *refs) = refs
        (self.kept_x, self.kept_y, self.kept_z, self.fin, self.down, self.turned, self.out_sem, self.turned_sem, self.piece_sem, *refs) = refs
        self.got = dict(zip(self.PHASES, refs[::2]))
        self.sent = dict(zip(self.PHASES, refs[1::2]))

    @classmethod
    def scratch(cls, z, units):
        unit, share = z.unit, z.unit[1:]
        data = [(2, X, CORES, *unit), (3, X, *unit), (2, 2, Y // 2, *share), (2, 2, *unit), (2, *unit), (units, z.Z, 3, 16, LANES)]
        data += [unit, (2, 2, *unit), unit, share]
        wide = [(2, *unit), share, share]
        return (
            [VMEM(shape, bf16) for shape in data]
            + [VMEM(shape, f32) for shape in wide]
            + [VMEM((units, *unit), bf16), VMEM((units, CORES, Y, z.h, LANES), bf16), VMEM((2, LANES, z.D), bf16)]
            + [DMA((2, units)), DMA((2, 2)), DMA]
            + [DMA((units + 3,)) for _ in range(2 * len(cls.PHASES))]
        )

    def peers(self):
        here = self.here
        return (
            [here.partner()] + [here.along_x(k) for k in SIDES] + [here.along_y(k) for k in range(1, Y)] + [here.along_z(k) for k in range(1, here.Z)]
        )

    def which(self, u, m):
        return (u, ALL) if m is None else (self.units + m, m)

    def send(self, phase, i, src, dst, where):
        remote(src, dst, self.sent[phase].at[i], self.got[phase].at[i], where).start()

    def over(self, m, work, begin=0, end=Y):
        def share(y):
            for k in range(len(self.outs)) if m is None else (m,):
                work(y, k)

        loop(begin, end, share)

    def start_p(self, u, m=None, places=range(X)):
        here, (i, mm) = self.here, self.which(u, None if isinstance(m, slice) else m)
        mm = m if isinstance(m, slice) else mm
        for x in places:
            self.send("p", i, self.stage.at[odd(u), x, 1 - here.c, :, mm], self.got_p.at[lax.rem(u, 3), x, :, mm], here.partner())

    def start_early_p(self, u):
        self.start_p(u, slice(0, 2), range(2))

    def start_late_p(self, u):
        self.start_p(u, slice(0, 2), range(2, X))
        self.start_p(u, slice(2, 3))

    def both(self, u, x, y, m):
        return self.stage[odd(u), x, self.here.c, y, m].astype(f32) + self.got_p[lax.rem(u, 3), x, y, m].astype(f32)

    def start_x1(self, u, m=None):
        here, half, slot, (i, mm) = self.here, Y // 2, odd(u), self.which(u, m)
        wait(self.got_p.at[lax.rem(u, 3), :, :, mm], self.got["p"].at[i])
        far = lax.rem(here.x + FAR, X)

        def work(y, k):
            self.send_x1[y, k] = self.both(u, far, y, k).astype(bf16)

        self.over(m, work)
        for side in range(2):
            self.send("x1", i, self.send_x1.at[pl.ds(side * half, half), mm], self.got_x1.at[slot, side, :, mm], here.along_x(SIDES[side]))

    def start_x2(self, u, m=None):
        here, half, slot, (i, mm) = self.here, Y // 2, odd(u), self.which(u, m)
        wait(self.got_x1.at[slot, :, :, mm], self.got["x1"].at[i])
        wait(self.got_x1.at[slot, :, :, mm], self.sent["x1"].at[i])
        wait(self.got_p.at[lax.rem(u, 3), :, :, mm], self.sent["p"].at[i])
        right, left = here.right(), here.left()

        def first(y, k):
            self.send_x2[slot, 0, y, k] = (self.both(u, right, y, k) + self.got_x1[slot, 0, y, k].astype(f32)).astype(bf16)
            self.send_x2[slot, 1, y, k] = self.both(u, left, y, k).astype(bf16)
            self.kept_x[slot, y, k] = self.both(u, here.x, y, k)

        def second(y, k):
            self.send_x2[slot, 0, y, k] = self.both(u, right, y, k).astype(bf16)
            self.send_x2[slot, 1, y, k] = (self.both(u, left, y, k) + self.got_x1[slot, 1, y - half, k].astype(f32)).astype(bf16)
            self.kept_x[slot, y, k] = self.both(u, here.x, y, k)

        self.over(m, first, 0, half)
        self.over(m, second, half, Y)
        for side in range(2):
            self.send("x2", i, self.send_x2.at[slot, side, :, mm], self.got_x2.at[slot, side, :, mm], here.along_x(SIDES[side]))

    def start_y(self, u, m=None):
        here, slot, (i, mm) = self.here, odd(u), self.which(u, m)
        wait(self.got_x2.at[slot, :, :, mm], self.got["x2"].at[i])
        wait(self.got_x2.at[slot, :, :, mm], self.sent["x2"].at[i])

        def total(y, k):
            return self.kept_x[slot, y, k] + self.got_x2[slot, 0, y, k].astype(f32) + self.got_x2[slot, 1, y, k].astype(f32)

        def work(y, k):
            self.send_y[y, k] = total(y, k).astype(bf16)

        def own(_, k):
            self.kept_y[k] = total(here.y, k)

        self.over(m, work)
        self.over(m, own, 0, 1)
        for k in (*SIDES, FAR):
            self.send("y", i, self.send_y.at[lax.rem(here.y + k, Y), mm], self.got_y.at[slot, here.y, mm], here.along_y(k))

    def start_z(self, u, m=None):
        z, here, slot, (i, mm) = self.z, self.here, odd(u), self.which(u, m)
        wait(self.got_y.at[slot, pl.ds(0, Y - 1), mm], self.got["y"].at[i])
        wait(self.got_y.at[slot, pl.ds(0, Y - 1), mm], self.sent["y"].at[i])

        def work(_, k):
            total = self.kept_y[k]
            for place in range(1, Y):
                total += self.got_y[slot, lax.rem(here.y + place, Y), k].astype(f32)
            self.kept_z[k] = total
            self.send_z[k] = total.astype(bf16)

        self.over(m, work, 0, 1)

        def send(k):
            to = lax.rem(here.z + k, z.Z)
            pl.when(to < z.active)(lambda: self.send("z", i, self.send_z.at[mm, at(to * 16, 16), :], self.got_z.at[u, here.z, mm], here.along_z(k)))

        loop(1, z.Z, send)

    def if_active(self, yes, no):
        pl.when(self.here.z < self.z.active)(yes)
        pl.when(self.here.z >= self.z.active)(no)

    def wait_pieces(self, i, mm, n, sem):
        if n:
            wait(self.got_z.at[0, pl.ds(0, n), mm], sem.at[i])

    def mine(self, mm):
        return self.here.y, mm, at(self.here.z * 16, 16)

    def add_pieces(self, u, m):
        z, here, (i, mm) = self.z, self.here, self.which(u, m)
        self.wait_pieces(i, mm, z.active - 1, self.sent["z"])
        self.wait_pieces(i, mm, z.Z - 1, self.got["z"])
        y, mm, rows = self.mine(mm)
        total = self.kept_z[mm, rows, :]
        for k in range(1, z.Z):
            total += self.got_z[u, lax.rem(here.z + k, z.Z), mm].astype(f32)
        self.fin[u, y, mm, rows, :] = total.astype(bf16)

    def send_pieces(self, u, m=None):
        i, mm = self.which(u, m)
        y, mm, rows = self.mine(mm)
        piece = self.fin.at[u, y, mm, rows, :]
        loop(1, self.z.Z, lambda k: self.send("az", i, piece, piece, self.here.along_z(k)))

    def start_az(self, u, m=None):
        i, mm = self.which(u, m)

        def yes():
            self.add_pieces(u, m)
            self.send_pieces(u, m)

        self.if_active(yes, lambda: self.wait_pieces(i, mm, self.z.active, self.sent["z"]))

    def hand_on(self, u, out):
        def yes():
            self.add_pieces(u, None)
            y, mm, rows = self.mine(ALL)
            copy = pltpu.make_async_copy(self.fin.at[u, y, mm, rows, :], out, self.piece_sem)
            copy.start()
            copy.wait()

        self.if_active(yes, lambda: self.wait_pieces(u, ALL, self.z.active, self.sent["z"]))

    def take_over(self, u, piece):
        def yes():
            y, mm, rows = self.mine(ALL)
            copy = pltpu.make_async_copy(piece, self.fin.at[u, y, mm, rows, :], self.piece_sem)
            copy.start()
            copy.wait()
            self.send_pieces(u)

        pl.when(self.here.z < self.z.active)(yes)

    def start_ay(self, u, m=None):
        z, here, (i, mm) = self.z, self.here, self.which(u, m)
        self.if_active(lambda: self.wait_pieces(i, mm, z.active - 1, self.got["az"]), lambda: self.wait_pieces(i, mm, z.active, self.got["az"]))
        share = self.fin.at[u, here.y, mm]
        for k in (*SIDES, FAR):
            self.send("ay", i, share, share, here.along_y(k))

    def place(self, u):
        nb = self.z.NB
        return (1, u) if self.base == 0 else (1 - lax.div(u + nb - self.base, nb), lax.rem(u + nb - self.base, nb))

    def start_f(self, u, m=None):
        z, c, (i, mm) = self.z, self.here.c, self.which(u, m)
        layer, j = self.place(u)
        wait(self.fin.at[u, pl.ds(0, Y - 1), mm], self.got["ay"].at[i])
        for k in range(2) if m is None else (m,):
            if k == 2:
                break
            for y in range(Y):
                out = self.outs[k].at[layer, :, at((y * z.NB + j) * LANES, LANES, LANES)]
                pltpu.make_async_copy(self.fin.at[u, y, k], out, self.out_sem.at[k, u]).start()
        if m in (None, 2):
            self.down[u, c] = self.fin[u, :, 2]
            self.send("f", u, self.fin.at[u, :, 2], self.down.at[u, c], self.here.partner())

    def finish(self, u):
        z, c = self.z, self.here.c
        layer, j = self.place(u)
        wait(self.down.at[u, 0], self.got["f"].at[u])
        slot = odd(u)
        pl.when(u > 1)(lambda: self.turned_out(u - 2, "wait"))
        self.turned[slot] = self.down[u].reshape(z.D, LANES).T
        self.turned_out(u, "start")

    def turned_out(self, u, what):
        z, c = self.z, self.here.c
        layer, j = self.place(u)
        for half in range(2):
            row = 2 * j + half

            @pl.when(lax.div(row, z.NB) == c)
            def _(half=half, row=row):
                out = self.outs[2].at[layer, at(lax.rem(row, z.NB) * 64, 64), :]
                getattr(pltpu.make_async_copy(self.turned.at[odd(u), pl.ds(half * 64, 64), :], out, self.turned_sem.at[odd(u), half]), what)()

    def end(self, units, in_parts):
        z = self.z

        def sent_back(i, mm):
            self.if_active(lambda: self.wait_pieces(i, mm, z.Z - 1, self.sent["az"]), lambda: None)
            wait(self.fin.at[0, pl.ds(0, Y - 1), mm], self.sent["ay"].at[i])

        def one(u):
            wait(self.down.at[0, 0], self.sent["f"].at[u])
            for m in range(2):
                wait(self.down.at[0, 0], self.out_sem.at[m, u])

        loop(0, units, one)
        loop(0, units - in_parts, lambda u: sent_back(u, ALL))
        for m in range(len(self.outs) if in_parts else 0):
            sent_back(self.units + m, m)
        for u in range(max(0, units - 2), units):
            self.turned_out(u, "wait")


def backward_kernel(z, first, *refs):
    T, TC, T3, NB, FB, D = z.T, z.TC, z.T3, z.NB, z.FB, z.D
    here = Here(z)
    refs = list(refs)

    def take(n):
        out, refs[:] = refs[:n], refs[n:]
        return out

    h_in, dh_in, dh_t_in, w0, w1, w2 = take(6)
    if first:
        early_in = take(3)
    else:
        left_in, piece_in, by_up_in, by_gate_in, act_in, a_t_in = take(6)
        take(3)
    dx_out, *outs = take(4)
    spill = take(1)[0]
    if first:
        left_out, piece_out, dx_t_out = take(3)
    dx_buf, h_buf, a_t, dh, dh_t, wg, wu, wd, work = take(9)
    ld_sem, dh_sem, w_sem, sp_sem, s3_sem, o_sem, left_sem, turned_sem = take(8)
    if first:
        a, dx_t_buf, dx_t_sem = take(3)
    else:
        saved, saved_sem, act_sem = take(3)
    if first:
        fetch = Fetch(z, here, (w0.at[1], w1.at[1], w2.at[1]), (wg, wu, wd), take(len(Fetch.scratch(z))), z.early, NB)
        w0, w1, w2 = early_in
    base = 0 if first else 2
    units = NB - 1 if first else NB + base
    reduce = Reduce(z, here, units, base, outs, refs)
    met = meet(reduce.peers())
    whole = pltpu.make_async_copy(dh_in, dh, dh_sem)
    whole.start()

    def load_h(i):
        return pltpu.make_async_copy(h_in.at[at(i * T3, T3), :], h_buf.at[odd(i)], ld_sem.at[odd(i)])

    turn = [pltpu.make_async_copy(dh_t_in, dh_t, turned_sem.at[0])]
    if first:
        load_h(0).start()
    else:
        turn.append(pltpu.make_async_copy(a_t_in, a_t, turned_sem.at[1]))

    def loads(j):
        return [pltpu.make_async_copy(src.at[j], dst.at[j], w_sem.at[k, j]) for k, (src, dst) in enumerate(((w0, wg), (w1, wu), (w2, wd)))]

    TS, slots = z.TS, z.slots

    def load_saved(q):
        j, rows, slot = lax.div(q, T // TS), at(lax.rem(q, T // TS) * TS, TS), lax.rem(q, slots)
        return [pltpu.make_async_copy(v.at[j, rows, :], saved.at[slot, k], saved_sem.at[k, slot]) for k, v in enumerate((by_up_in, by_gate_in))]

    def load_act(j):
        return pltpu.make_async_copy(act_in.at[j], work.at[pl.ds(0, T), :], act_sem)

    if first:
        start(loads(0))
        fetch.begin_local()
        met()
        fetch.begin_pair()
        fetch.start_a1(z.early)
    else:
        left = pltpu.make_async_copy(left_in, reduce.stage.at[1], left_sem)
        left.start()
        start(loads(0)[2:])
        for q in range(slots - 1):
            start(load_saved(q))
        load_act(0).start()
        start(turn)
        for j in range(1, NB):
            start(loads(j)[2:])
    n3 = T // T3

    def prepare(i):
        rows = at(i * T3, T3, LANES)
        pl.when(i + 1 < n3)(lambda: load_h(i + 1).start())
        load_h(i).wait()
        value = normed(h_buf[odd(i)].astype(f32))[0]
        a[rows, :] = value
        a_t[:, rows] = value.T

    if not first:
        met()
        left.wait()
        reduce.start_p(1)
        reduce.take_over(0, piece_in)
    def turned():
        for copy in turn:
            copy.wait()

    if first:
        loop(0, n3, prepare)
        for j in range(1, z.early):
            start(loads(j))
        start(turn)
        fetch.end_pair()
        fetch.start_a2(z.early)

    def product(k, rows, cols):
        return work.at[at(k * T + rows.start, rows.size), cols]

    def spills(j):
        return [pltpu.make_async_copy(work.at[pl.ds((1 + k) * T, T), :], spill.at[k, j], sp_sem.at[k]) for k in range(2)]

    def spilled(j):
        for copy in spills(j):
            copy.wait()

    def step(name, u, m=None):
        do = getattr(reduce, "start_" + name)
        back = name in ("ay", "az")
        begin = 0 if first or name == "ay" else 1
        end = units - 1 if first and back else units
        if isinstance(u, int):
            if begin <= u < end:
                do(u, m)
        else:
            pl.when(jnp.logical_and(u >= begin, u < end))(lambda: do(u))

    def halfway(i, n, before, after):
        if n == 1:
            before()
            after()
        else:
            pl.when(i == 0)(before)
            pl.when(i == n // 2)(after)

    whole.wait()

    def loaded(j):
        for copy in loads(j):
            copy.wait()

    def block(j):
        u = j + base - 1
        if first:
            fetch.serve_a(j)
            pl.when(j < z.early)(lambda: loaded(j))
            pl.when(j >= z.early)(lambda: fetch.ready(j))
        else:
            pl.when(j > 0)(lambda: load_act(j).start())
            loads(j)[2].wait()
        pl.when(j > 0)(lambda: spilled(j - 1))

        def at_0():
            step("x2", u - 1)

        def at_1():
            step("z", u - 2)
            step("ay", u - 3)

        def at_2():
            if first:
                fetch.serve_b(j)
            pl.when(j == 0)(turned)
            step("x1", u)

        def at_3():
            if first:
                step("early_p", j)
            else:
                pl.when(j + 1 < NB)(lambda: reduce.start_early_p(j + base))
            step("y", u - 1)
            step("az", u - 2)

        def piece(i):
            halfway(i, T // TS, at_0, at_1)
            q, rows = j * (T // TS) + i, at(i * TS, TS)
            pl.when(q + slots - 1 < NB * (T // TS))(lambda: start(load_saved(q + slots - 1)))
            for copy in load_saved(q):
                copy.wait()
            by_act = dot(dh[rows, :], wd[j], ((1,), (1,))).astype(bf16).astype(f32)
            slot = lax.rem(q, slots)
            product(1, rows, ALL)[...] = (by_act * saved[slot, 1]).astype(bf16)
            product(2, rows, ALL)[...] = (by_act * saved[slot, 0]).astype(bf16)

        def chunk(i):
            halfway(i, T // TC, at_0, at_1)
            rows = at(i * TC, TC)
            for cols in z.halves:
                gate, up = dot(a[rows, :], wg[j, :, cols]), dot(a[rows, :], wu[j, :, cols])
                by_act = dot(dh[rows, :], wd[j, cols, :], ((1,), (1,))).astype(bf16).astype(f32)
                sig = 1.0 / (1.0 + jnp.exp(-gate))
                silu = gate * sig
                product(0, rows, cols)[...] = (silu * up).astype(bf16)
                product(1, rows, cols)[...] = (by_act * up * (sig + silu * (1.0 - sig))).astype(bf16)
                product(2, rows, cols)[...] = (by_act * silu).astype(bf16)

        if first:
            loop(0, T // TC, chunk)
        else:
            loop(0, T // TS, piece)
            load_act(j).wait()
            start(loads(j)[:2])
        start(spills(j))
        stage, slot, m = reduce.stage, odd(j + base), D // 2

        def rows_of(i):
            halfway(i, 2, at_2, at_3)
            rows = at(i * m, m)
            gates = dot(a_t[rows, :], work[pl.ds(T, T), :]).astype(bf16)
            ups = dot(a_t[rows, :], work[pl.ds(2 * T, T), :]).astype(bf16)
            downs = dot(dh_t[rows, :], work[pl.ds(0, T), :]).astype(bf16)
            for y in range(Y):
                lanes = slice(y * LANES, (y + 1) * LANES)
                for x in range(X // 2):
                    for c in range(CORES):
                        part = slice((x * CORES + c) * z.h, (x * CORES + c + 1) * z.h)
                        stage[slot, i * (X // 2) + x, c, y, 0] = gates[part, lanes]
                        stage[slot, i * (X // 2) + x, c, y, 1] = ups[part, lanes]
                for x in range(X):
                    stage[slot, x, i, y, 2] = downs[y * z.h : (y + 1) * z.h, x * LANES : (x + 1) * LANES]

        loop(0, 2, rows_of)
        if first:
            step("late_p", j)
        else:
            pl.when(j + 1 < NB)(lambda: reduce.start_late_p(j + base))

            @pl.when(j + 1 == NB)
            def _():
                for m in range(3):
                    reduce.start_p(NB + base - 1, m)

    loop(0, NB, block)
    if first:
        left = pltpu.make_async_copy(reduce.stage.at[(NB - 1) % 2], left_out, left_sem)
        left.start()
    spilled(NB - 1)

    def load_3(i):
        slot, rows = odd(i), at(i * T3, T3)
        out = [load_h(i)]
        for k in range(2):
            for j in range(NB):
                out.append(pltpu.make_async_copy(spill.at[k, j, rows, :], work.at[at(((slot * 2 + k) * NB + j) * T3, T3), :], s3_sem.at[slot]))
        return out

    def store_3(i):
        return pltpu.make_async_copy(dx_buf.at[odd(i)], dx_out.at[at(i * T3, T3), :], o_sem.at[odd(i)])

    def store_turned(i):
        return pltpu.make_async_copy(dx_t_buf.at[odd(i)], dx_t_out.at[:, at(i * T3, T3, LANES)], dx_t_sem.at[odd(i)])

    start(load_3(0))
    u = NB + base - 1
    if first:
        todo = ("x2:1", "z:2,ay:3", "", "az:2,y:1", "", "ay:2,z:1", "", "")
    else:
        todo = (
            "x2:1,ay:3",
            "x1.0,x1.1,z:2",
            "x1.2",
            "x2.0,az:2,y:1,x2.1",
            "x2.2,ay:2",
            "z:1,y.0,y.1",
            "y.2,az:1,z.0,z.1",
            "z.2,ay:1,az.0",
            "az.1,az.2,ay.0,ay.1,ay.2",
        )

    def steps(text):
        for item in filter(None, text.split(",")):
            name, _, behind = item.partition(":")
            if behind:
                step(name, u - int(behind))
            else:
                name, _, m = item.partition(".")
                step(name, u, int(m))

    done = units - 2 if first else units - 4

    def rows_back(i):
        slot, rows = odd(i), at(i * T3, T3)
        pl.when(i + 1 < n3)(lambda: start(load_3(i + 1)))
        for when, text in enumerate(todo[:n3]):
            pl.when(i == when)(lambda text=text: steps(text))

        @pl.when(i == n3 - 2)
        def _():
            loop(0, done, reduce.start_f)

        @pl.when(i == n3 - 1)
        def _():
            loop(0, done, reduce.finish)

        if not first:

            @pl.when(i == 0)
            def _():
                for j in range(NB):
                    for copy in loads(j)[:2]:
                        copy.wait()

        load_h(i).wait()
        wait(work.at[at(slot * 2 * NB * T3, 2 * NB * T3), :], s3_sem.at[slot])
        pl.when(i > 1)(lambda: store_3(i - 2).wait())
        if first:
            pl.when(i > 2)(lambda: store_turned(i - 3).wait())
            dx_t_buf[1 - slot] = dx_buf[1 - slot].T
        back = []
        for k, w in ((0, wg), (1, wu)):
            total = None
            for j in range(NB):
                part = dot(work[at(((slot * 2 + k) * NB + j) * T3, T3), :], w[j], ((1,), (1,)))
                total = part if total is None else total + part
            back.append(total.astype(bf16))
        by_a = (back[0] + back[1]).astype(f32)
        wide = h_buf[slot].astype(f32)
        square = jnp.mean(wide * wide, -1, keepdims=True) + 1e-6
        scale = lax.rsqrt(square)
        by_scale = jnp.sum(by_a * wide, -1, keepdims=True)
        by_square = by_scale * (-0.5 * scale / square) * (2.0 / D)
        dx_buf[slot] = dh[rows, :] + (by_a * scale + by_square * wide).astype(bf16)
        store_3(i).start()
        if first:
            pl.when(i > 0)(lambda: store_turned(i - 1).start())

    loop(0, n3, rows_back)
    if first:
        store_turned(n3 - 3).wait()
        dx_t_buf[odd(n3 - 1)] = dx_buf[odd(n3 - 1)].T
        store_turned(n3 - 1).start()
    assert n3 == 8
    for text in todo[n3:]:
        steps(text)
    if first:
        reduce.hand_on(units - 1, piece_out)
    back = units - 1 if first else units
    for v in range(done, back):
        if first or v + 1 < back:
            reduce.start_f(v)
        else:
            for m in range(3):
                reduce.start_f(v, m)
    for v in range(done, back):
        reduce.finish(v)
    reduce.end(back, 0 if first else 1)
    if first:
        fetch.end()
        left.wait()
    for i in range(max(0, n3 - 2), n3):
        store_3(i).wait()
        if first:
            store_turned(i).wait()


def call(body, out, n_in, scratch, number, aliases=()):
    return pl.pallas_call(
        body,
        out_shape=out,
        in_specs=[pl.BlockSpec(memory_space=HBM)] * n_in,
        out_specs=[pl.BlockSpec(memory_space=HBM)] * len(out),
        scratch_shapes=scratch,
        input_output_aliases=dict(aliases),
        compiler_params=pltpu.CompilerParams(collective_id=number, has_side_effects=True, vmem_limit_bytes=66_900_000),
    )


def forward(z, x, dy, shards):
    S = jax.ShapeDtypeStruct
    wide, tall, tokens, hidden, piece = (z.NB, z.D, z.FB), (z.NB, z.FB, z.D), (z.T, z.D), (z.NB, z.T, z.FB), (2, z.TC, z.FB)
    scratch = [VMEM(tokens, bf16), VMEM(tokens, f32), VMEM(tokens, bf16), VMEM((2, z.T3, z.D), bf16), VMEM(tokens[::-1], bf16), VMEM(tokens[::-1], bf16)]
    scratch += [VMEM(piece, bf16), VMEM(piece, f32), VMEM(piece, f32)]
    early = [(z.early, *shape[1:]) for shape in (wide, wide, tall)]
    scratch += [VMEM(shape, bf16) for shape in (wide, wide, tall, *early)]
    scratch += [DMA, DMA((3,)), DMA((3,)), DMA, DMA((3, 2)), DMA((2,)), DMA((2,))] + Fetch.scratch(z) + Fetch.scratch(z)
    out = [S(tokens, bf16), S(wide, bf16), S(wide, bf16), S(tall, bf16), S(hidden, bf16), S(hidden, f32), S(hidden, f32)]
    out += [S(shape, bf16) for shape in (*early, tokens[::-1], tokens[::-1])]
    h, *out = call(functools.partial(forward_kernel, z), out, 5, scratch, 0)(x, dy, *shards)
    return h, out[:3], out[3:6], out[6:9], out[9:]


def backward(z, h, dh, dh_t, w, more, first):
    S = jax.ShapeDtypeStruct
    wide, tall, tokens = (z.NB, z.D, z.FB), (z.NB, z.FB, z.D), (z.T, z.D)
    units = z.NB - 1 if first else z.NB + 2
    scratch = [VMEM((2, z.T3, z.D), bf16), VMEM((2, z.T3, z.D), bf16)]
    scratch += [VMEM(tokens[::-1], bf16), VMEM(tokens, bf16), VMEM(tokens[::-1], bf16)]
    scratch += [VMEM(wide, bf16), VMEM(wide, bf16), VMEM(tall, bf16), VMEM((max(3 * z.T, 4 * z.NB * z.T3), z.FB), bf16)]
    scratch += [DMA((2,)), DMA, DMA((3, z.NB)), DMA((2,)), DMA((2,)), DMA((2,)), DMA, DMA((2,))]
    if first:
        scratch += [VMEM(tokens, bf16), VMEM((2, z.D, z.T3), bf16), DMA((2,))] + Fetch.scratch(z)
    else:
        scratch += [VMEM((z.slots, 2, z.TS, z.FB), f32), DMA((2, z.slots)), DMA]
    scratch += Reduce.scratch(z, units)
    grads = [S((2, z.h, z.F), bf16), S((2, z.h, z.F), bf16), S((2, z.F // (X * CORES), z.D), bf16)]
    out = [S(tokens, bf16), *grads, S((2, z.NB, z.T, z.FB), bf16)]
    if first:
        out += [S((X, CORES, *z.unit), bf16), S((3, 16, LANES), bf16), S(tokens[::-1], bf16)]
    args = (h, dh, dh_t, *w, *more)
    aliases = {} if first else {len(args) - 3 + i: 1 + i for i in range(3)}
    dx, g, u, d, _, *left = call(functools.partial(backward_kernel, z, first), out, len(args), scratch, 1 if first else 2, aliases)(*args)
    return dx, (g, u, d), left


def solution(mesh):
    def step(x, dy, *weights):
        z = Sizes(mesh, x.shape[1], x.shape[2], weights[0].shape[2])
        h, w, (act, by_up, by_gate), early, (a_t, dy_t) = forward(z, x[0], dy[0], weights)
        dh, grads, (left, piece, dh_t) = backward(z, h, dy[0], dy_t, weights, early, True)
        dx, grads, _ = backward(z, x[0], dh, dh_t, w, (left, piece, by_up, by_gate, act, a_t, *grads), False)
        return dx[None], *grads

    states, cut = P(("rep", "r", "s"), None, None), P(None, "s", None)
    return jax.shard_map(
        step,
        mesh=mesh,
        in_specs=(states, states) + (cut,) * 3,
        out_specs=(states,) + (P("rep", "s", None),) * 3,
        check_vma=False,
    )
```

```python
import functools

import jax
import jax.numpy as jnp
from jax import lax
from jax.experimental import pallas as pl
from jax.experimental.pallas import tpu as pltpu
from jax.sharding import PartitionSpec as P

f32, bf16 = jnp.float32, jnp.bfloat16
MESH = pl.DeviceIdType.MESH
LANES = 128
X, CORES, Y = 4, 2, 4
HBM, VMEM, DMA = pl.ANY, pltpu.VMEM, pltpu.SemaphoreType.DMA


def dot(a, b, dims=((1,), (0,))):
    return lax.dot_general(a, b, (dims, ((), ())), preferred_element_type=f32)


def at(start, size, multiple=16):
    return pl.ds(pl.multiple_of(start, multiple) if not isinstance(start, int) else start, size)


ALL = slice(None)
LEFT, RIGHT, FAR = 3, 1, 2
SIDES = (RIGHT, LEFT)


def loop(begin, end, body):
    def one(i, carry):
        body(i)
        return carry

    lax.fori_loop(begin, end, one, 0)


def odd(i):
    return lax.rem(i, 2)


class Sizes:
    chunk, piece, rows, slots = 1024, 512, 256, 4

    def __init__(self, mesh, tokens, d, ff):
        self.R = mesh.shape["r"]
        self.Z = self.R // Y
        self.T, self.D, self.F = tokens, d, ff
        self.NB = ff // (X * LANES)
        self.FB = X * LANES
        self.h = d // (X * CORES)
        self.TC = min(self.chunk, tokens)
        self.T3 = min(self.rows, tokens)
        self.TS = min(self.piece, tokens)
        self.unit = (Y, 3, self.h, LANES)
        self.active = self.h // 16
        self.halves = (slice(0, self.FB // 2), slice(self.FB // 2, self.FB))
        self.early = self.NB // 2
        assert self.h % 16 == 0 and self.active <= self.Z and mesh.shape["s"] == X * CORES


class Here:
    def __init__(self, z):
        s, self.r = lax.axis_index("s"), lax.axis_index("r")
        self.x, self.c = lax.div(s, CORES), lax.rem(s, CORES)
        self.y, self.z, self.Z = lax.div(self.r, z.Z), lax.rem(self.r, z.Z), z.Z
        self.R = z.R

    def partner(self):
        return {"s": self.x * CORES + 1 - self.c}

    def along_x(self, k):
        return {"s": lax.rem(self.x + k, X) * CORES + self.c}

    def along_y(self, k):
        return {"r": lax.rem(self.y + k, Y) * self.Z + self.z}

    def right(self):
        return lax.rem(self.x + RIGHT, X)

    def left(self):
        return lax.rem(self.x + LEFT, X)

    def along_z(self, k):
        return {"r": self.y * self.Z + lax.rem(self.z + k, self.Z)}


def remote(src, dst, sent, got, where):
    return pltpu.make_async_remote_copy(src_ref=src, dst_ref=dst, send_sem=sent, recv_sem=got, device_id=where, device_id_type=MESH)


def start(copies):
    for copy in copies:
        copy.start()


def wait(ref, sem):
    pltpu.make_async_copy(ref, ref, sem).wait()


def meet(peers):
    barrier = pltpu.get_barrier_semaphore()
    for peer in peers:
        pl.semaphore_signal(barrier, inc=1, device_id=peer, device_id_type=MESH)
    return lambda: pl.semaphore_wait(barrier, len(peers))


FETCHES = (
    "a10,a11,a20,d10,b10,d11,a21",
    "d20,a12,a14,b20,a13,e0,b11,d21,c0,a22,d12",
    "e1,a23,d13,a24,b21,b12",
    "d22,c1,d14,b13",
    "d23,La11,e2,La10,b22",
    "b23,b14,La21,d24,c2,Ld10,Ld11",
    "e4,c3,Lb11",
    "e3,La20,Ld21,b24",
    "Lb10",
    "Ld20,c4,Lb21",
    "Lb20,Le0,Le1,Lc1",
    "Lc0",
)


class Fetch:
    PHASES = ("a1", "a2", "b1", "b2", "c", "d1", "d2", "e")

    def __init__(self, z, here, shards, w, sems, begin, end):
        self.z, self.here, self.shards, self.w, self.first, self.last = z, here, shards, w, begin, end
        self.local, self.local_d, self.pair, self.pair_sent = sems[:4]
        self.got = dict(zip(self.PHASES, sems[4::2]))
        self.sent = dict(zip(self.PHASES, sems[5::2]))
        self.parts = [[k for k in range(z.NB) if begin <= (c * z.NB + k) // 2 < end] for c in range(CORES)]

    @classmethod
    def scratch(cls, z):
        return [DMA((z.NB,)), DMA, DMA, DMA] + [DMA((z.NB,)) for _ in range(2 * len(cls.PHASES))]

    def peers(self):
        here = self.here
        return [here.partner()] + [here.along_x(k) for k in SIDES] + [here.along_y(k) for k in SIDES]

    def own(self, j):
        z, here = self.z, self.here
        for shard, w in zip(self.shards[:2], self.w[:2]):
            for l in range(X):
                slot = w.at[j, self.rows(here.x), pl.ds(l * LANES, LANES)]
                pltpu.make_async_copy(shard.at[:, at((l * z.NB + j) * LANES, LANES, LANES)], slot, self.local.at[j]).start()

    def each_core(self, do):
        for c in range(CORES):
            pl.when(self.here.c == c)(lambda c=c: do(self.parts[c], self.parts[1 - c]))

    def part(self, k):
        z, here = self.z, self.here
        place = here.c * z.NB + k
        return self.shards[2].at[pl.ds(64 * k, 64), :], self.w[2].at[lax.div(place, 2), at(here.x * LANES + odd(place) * 64, 64), :]

    def rows(self, x):
        return at(x * (CORES * self.z.h) + self.here.c * self.z.h, self.z.h)

    def lanes(self, y):
        return at(y * LANES, LANES, LANES)

    def down(self, x, begin=0, size=64):
        return at(x * LANES + self.here.c * 64 + begin, size)

    def send(self, phase, j, w, rows, lanes, where):
        slot = self.w[w].at[j, rows, lanes]
        remote(slot, slot, self.sent[phase].at[j], self.got[phase].at[j], where).start()

    def begin_local(self):
        for j in range(self.first, self.last):
            self.own(j)

        def do(mine, _):
            for k in mine:
                pltpu.make_async_copy(*self.part(k), self.local_d).start()

        self.each_core(do)

    def begin_pair(self):
        def do(mine, _):
            for k in mine:
                src, slot = self.part(k)
                remote(src, slot, self.pair_sent, self.pair, self.here.partner()).start()

        self.each_core(do)

    def wait_parts(self, n, sem):
        if n:
            wait(self.halves(0, n), sem)

    def end_pair(self):
        def do(mine, other):
            self.wait_parts(len(mine), self.local_d)
            self.wait_parts(len(other), self.pair)

        self.each_core(do)

    def start_a1(self, j):
        here = self.here
        wait(self.pieces(j, 8), self.local.at[j])
        for k in SIDES:
            for w in range(2):
                self.send("a1", j, w, self.rows(here.x), self.lanes(here.y), here.along_x(k))

    def start_d1(self, j):
        for k in SIDES:
            self.send("d1", j, 2, self.down(self.here.x), ALL, self.here.along_x(k))

    def start_a2(self, j):
        here = self.here
        wait(self.pieces(j, 4), self.got["a1"].at[j])
        lanes = self.lanes(here.y)
        self.send("a2", j, 0, self.rows(here.left()), lanes, here.along_x(RIGHT))
        self.send("a2", j, 1, self.rows(here.right()), lanes, here.along_x(LEFT))

    def start_d2(self, j):
        here = self.here
        wait(self.halves(j, 2), self.got["d1"].at[j])
        self.send("d2", j, 2, self.down(here.left(), 0, 32), ALL, here.along_x(RIGHT))
        self.send("d2", j, 2, self.down(here.right(), 32, 32), ALL, here.along_x(LEFT))

    def start_b1(self, j):
        here = self.here
        wait(self.pieces(j, 2), self.got["a2"].at[j])
        for k in SIDES:
            for m in range(1, X):
                for w in range(2):
                    self.send("b1", j, w, self.rows(lax.rem(here.x + m, X)), self.lanes(here.y), here.along_y(k))

    def start_b2(self, j):
        here = self.here
        wait(self.pieces(j, 12), self.got["b1"].at[j])
        for m in range(1, X):
            rows = self.rows(lax.rem(here.x + m, X))
            self.send("b2", j, 0, rows, self.lanes(lax.rem(here.y + LEFT, Y)), here.along_y(RIGHT))
            self.send("b2", j, 1, rows, self.lanes(lax.rem(here.y + RIGHT, Y)), here.along_y(LEFT))

    def start_c(self, j):
        wait(self.pieces(j, 6), self.got["b2"].at[j])
        for w in range(2):
            for x in range(X):
                self.send("c", j, w, self.rows(x), ALL, self.here.partner())

    def start_e(self, j):
        wait(self.halves(j, 1), self.got["d2"].at[j])
        for m in range(1, X):
            self.send("e", j, 2, self.down(lax.rem(self.here.x + m, X)), ALL, self.here.partner())

    def pieces(self, j, n):
        high = 6 if n % 6 == 0 else min(n, 8)
        return self.w[0].at[j, pl.ds(0, high * self.z.h), pl.ds(0, n // high * LANES)]

    def halves(self, j, n):
        return self.w[2].at[j, pl.ds(0, 64 * n), :]

    def ready(self, j):
        wait(self.w[0].at[j], self.got["c"].at[j])
        wait(self.halves(j, 3), self.got["e"].at[j])

    def serve_a(self, j):
        @self.if_mine(j + 1)
        def _():
            self.start_b2(j + 1)
            self.start_d2(j + 1)

        @self.if_mine(j + 2)
        def _():
            self.start_b1(j + 2)
            self.start_d1(j + 2)

        self.if_mine(j + 3)(lambda: self.start_a1(j + 3))

    def serve_b(self, j):
        @self.if_mine(j + 1)
        def _():
            self.start_c(j + 1)
            self.start_e(j + 1)

        self.if_mine(j + 3)(lambda: self.start_a2(j + 3))

    def if_mine(self, j):
        return pl.when(jnp.logical_and(j >= self.first, j < self.last))

    def end(self):
        self.each_core(lambda mine, _: self.wait_parts(len(mine), self.pair_sent))

        def drain(j):
            for phase, n in (("a1", 4), ("a2", 2), ("b1", 12), ("b2", 6)):
                wait(self.pieces(j, n), self.sent[phase].at[j])
            for phase, n in (("d1", 2), ("d2", 1), ("e", 3)):
                wait(self.halves(j, n), self.sent[phase].at[j])
            wait(self.w[0].at[j], self.sent["c"].at[j])

        loop(self.first, self.last, drain)


def sigmoid(v):
    return 1.0 / (1.0 + jnp.exp(-v))


def normed(wide):
    scale = lax.rsqrt(jnp.mean(wide * wide, -1, keepdims=True) + 1e-6)
    return (wide * scale).astype(bf16), scale


def forward_kernel(z, *refs):
    refs = list(refs)

    def take(n):
        out, refs[:] = refs[:n], refs[n:]
        return out

    x_in, dy_in, *shards = take(5)
    h_out, *w_out = take(4)
    kept_out, next_out, turned_out = take(3), take(3), take(2)
    a, acc, xs, dy_buf = take(4)
    turned = take(2)
    parts, w, w_next = take(3), take(3), take(3)
    act, by_up, by_gate = parts
    x_sem, out_sem, next_sem, h_sem, keep_sem, dy_sem, turned_sem = take(7)
    n_sems = len(Fetch.scratch(z))
    here = Here(z)
    fetch = Fetch(z, here, [v.at[0] for v in shards], w, take(n_sems), 0, z.NB)
    later = Fetch(z, here, [v.at[1] for v in shards], w_next, take(n_sems), 0, z.early)
    early = range(z.early)
    met = meet(fetch.peers())
    fetch.begin_local()
    load = pltpu.make_async_copy(x_in, xs, x_sem)
    load.start()
    met()
    fetch.begin_pair()

    def fetches(slot):
        for item in FETCHES[slot].split(","):
            who, phase, j = (later if item[0] == "L" else fetch), item.strip("L")[:-1], int(item[-1])
            if phase == "d1" and j == 0:
                who.end_pair()
            getattr(who, "start_" + phase)(j)

    fetches(0)
    load.wait()

    def load_dy(i):
        return pltpu.make_async_copy(dy_in.at[at(i * z.T3, z.T3), :], dy_buf.at[odd(i)], dy_sem.at[odd(i)])

    load_dy(0).start()
    n3 = z.T // z.T3

    def prepare(i):
        rows = at(i * z.T3, z.T3)
        a[rows, :] = normed(xs[rows, :].astype(f32))[0]
        acc[rows, :] = jnp.zeros((z.T3, z.D), f32)

    loop(0, n3, prepare)
    fetches(1)

    def turn(i):
        rows = at(i * z.T3, z.T3, LANES)
        pl.when(i + 1 < n3)(lambda: load_dy(i + 1).start())
        load_dy(i).wait()
        for v, part in zip(turned, (a[rows, :], dy_buf[odd(i)])):
            v[:, rows] = part.T

    loop(0, n3, turn)
    sent = [pltpu.make_async_copy(v, o, turned_sem.at[k]) for k, (v, o) in enumerate(zip(turned, turned_out))]
    start(sent)
    n = z.T // z.TC

    def keep(j, i):
        slot = odd(i)
        return [pltpu.make_async_copy(v.at[slot], o.at[j, at(i * z.TC, z.TC), :], keep_sem.at[k, slot]) for k, (v, o) in enumerate(zip(parts, kept_out))]

    def kept(j, i):
        for copy in keep(j, i):
            copy.wait()

    def serve(j, middle):
        for b in range(z.NB):
            pl.when(j == b)(lambda b=b: fetches(2 + 2 * b + middle))

    def block(j):
        serve(j, 0)
        fetch.ready(j)
        start([pltpu.make_async_copy(v.at[j], o.at[j], out_sem.at[k]) for k, (v, o) in enumerate(zip(w, w_out))])

        def chunk(i):
            @pl.when(i == n // 2)
            def _():
                serve(j, 1)

                @pl.when(j == 0)
                def _():
                    later.begin_local()
                    later.begin_pair()


            pl.when(j * n + i > 1)(lambda: kept(j, i))
            rows, slot = at(i * z.TC, z.TC), odd(i)
            for cols in z.halves:
                gate, up = dot(a[rows, :], w[0][j, :, cols]), dot(a[rows, :], w[1][j, :, cols])
                sig = sigmoid(gate)
                silu = gate * sig
                act[slot, :, cols] = (silu * up).astype(bf16)
                by_up[slot, :, cols] = silu
                by_gate[slot, :, cols] = up * (sig + silu * (1.0 - sig))
            acc[rows, :] += dot(act[slot], w[2][j])
            start(keep(j, i))

        loop(0, n, chunk)

    loop(0, z.NB, block)

    def finish(i):
        rows = at(i * z.T3, z.T3)
        xs[rows, :] = xs[rows, :] + acc[rows, :].astype(bf16)

    loop(0, z.T // z.T3, finish)
    store = pltpu.make_async_copy(xs, h_out, h_sem)
    store.start()
    for e in early:
        later.ready(e)
    handed = [pltpu.make_async_copy(v, o, next_sem.at[k]) for k, (v, o) in enumerate(zip(w_next, next_out))]
    start(handed)
    for i in range(2):
        kept(z.NB - 1, n - 2 + i)
    for k, v in enumerate(w):
        wait(v, out_sem.at[k])
    fetch.end()
    later.end()
    store.wait()
    for copy in (*handed, *sent):
        copy.wait()


class Reduce:
    PHASES = ("p", "x1", "x2", "y", "z", "az", "ay", "f")

    def __init__(self, z, here, units, base, outs, refs):
        self.z, self.here, self.units, self.base, self.outs = z, here, units, base, outs
        (self.stage, self.got_p, self.got_x1, self.got_x2, self.got_y, self.got_z, self.send_x1, self.send_x2, self.send_y, self.send_z, *refs) = refs
        (self.kept_x, self.kept_y, self.kept_z, self.fin, self.down, self.turned, self.out_sem, self.turned_sem, self.piece_sem, *refs) = refs
        self.got = dict(zip(self.PHASES, refs[::2]))
        self.sent = dict(zip(self.PHASES, refs[1::2]))

    @classmethod
    def scratch(cls, z, units):
        unit, share = z.unit, z.unit[1:]
        data = [(2, X, CORES, *unit), (3, X, *unit), (2, 2, Y // 2, *share), (2, 2, *unit), (2, *unit), (units, z.Z, 3, 16, LANES)]
        data += [unit, (2, 2, *unit), unit, share]
        wide = [(2, *unit), share, share]
        return (
            [VMEM(shape, bf16) for shape in data]
            + [VMEM(shape, f32) for shape in wide]
            + [VMEM((units, *unit), bf16), VMEM((units, CORES, Y, z.h, LANES), bf16), VMEM((2, LANES, z.D), bf16)]
            + [DMA((2, units)), DMA((2, 2)), DMA]
            + [DMA((units + 3,)) for _ in range(2 * len(cls.PHASES))]
        )

    def peers(self):
        here = self.here
        return (
            [here.partner()] + [here.along_x(k) for k in SIDES] + [here.along_y(k) for k in range(1, Y)] + [here.along_z(k) for k in range(1, here.Z)]
        )

    def which(self, u, m):
        return (u, ALL) if m is None else (self.units + m, m)

    def send(self, phase, i, src, dst, where):
        remote(src, dst, self.sent[phase].at[i], self.got[phase].at[i], where).start()

    def over(self, m, work, begin=0, end=Y):
        def share(y):
            for k in range(len(self.outs)) if m is None else (m,):
                work(y, k)

        loop(begin, end, share)

    def start_p(self, u, m=None, places=range(X)):
        here, (i, mm) = self.here, self.which(u, None if isinstance(m, slice) else m)
        mm = m if isinstance(m, slice) else mm
        for x in places:
            self.send("p", i, self.stage.at[odd(u), x, 1 - here.c, :, mm], self.got_p.at[lax.rem(u, 3), x, :, mm], here.partner())

    def start_early_p(self, u):
        self.start_p(u, slice(0, 2), range(2))

    def start_late_p(self, u):
        self.start_p(u, slice(0, 2), range(2, X))
        self.start_p(u, slice(2, 3))

    def both(self, u, x, y, m):
        return self.stage[odd(u), x, self.here.c, y, m].astype(f32) + self.got_p[lax.rem(u, 3), x, y, m].astype(f32)

    def start_x1(self, u, m=None):
        here, half, slot, (i, mm) = self.here, Y // 2, odd(u), self.which(u, m)
        wait(self.got_p.at[lax.rem(u, 3), :, :, mm], self.got["p"].at[i])
        far = lax.rem(here.x + FAR, X)

        def work(y, k):
            self.send_x1[y, k] = self.both(u, far, y, k).astype(bf16)

        self.over(m, work)
        for side in range(2):
            self.send("x1", i, self.send_x1.at[pl.ds(side * half, half), mm], self.got_x1.at[slot, side, :, mm], here.along_x(SIDES[side]))

    def start_x2(self, u, m=None):
        here, half, slot, (i, mm) = self.here, Y // 2, odd(u), self.which(u, m)
        wait(self.got_x1.at[slot, :, :, mm], self.got["x1"].at[i])
        wait(self.got_x1.at[slot, :, :, mm], self.sent["x1"].at[i])
        wait(self.got_p.at[lax.rem(u, 3), :, :, mm], self.sent["p"].at[i])
        right, left = here.right(), here.left()

        def first(y, k):
            self.send_x2[slot, 0, y, k] = (self.both(u, right, y, k) + self.got_x1[slot, 0, y, k].astype(f32)).astype(bf16)
            self.send_x2[slot, 1, y, k] = self.both(u, left, y, k).astype(bf16)
            self.kept_x[slot, y, k] = self.both(u, here.x, y, k)

        def second(y, k):
            self.send_x2[slot, 0, y, k] = self.both(u, right, y, k).astype(bf16)
            self.send_x2[slot, 1, y, k] = (self.both(u, left, y, k) + self.got_x1[slot, 1, y - half, k].astype(f32)).astype(bf16)
            self.kept_x[slot, y, k] = self.both(u, here.x, y, k)

        self.over(m, first, 0, half)
        self.over(m, second, half, Y)
        for side in range(2):
            self.send("x2", i, self.send_x2.at[slot, side, :, mm], self.got_x2.at[slot, side, :, mm], here.along_x(SIDES[side]))

    def start_y(self, u, m=None):
        here, slot, (i, mm) = self.here, odd(u), self.which(u, m)
        wait(self.got_x2.at[slot, :, :, mm], self.got["x2"].at[i])
        wait(self.got_x2.at[slot, :, :, mm], self.sent["x2"].at[i])

        def total(y, k):
            return self.kept_x[slot, y, k] + self.got_x2[slot, 0, y, k].astype(f32) + self.got_x2[slot, 1, y, k].astype(f32)

        def work(y, k):
            self.send_y[y, k] = total(y, k).astype(bf16)

        def own(_, k):
            self.kept_y[k] = total(here.y, k)

        self.over(m, work)
        self.over(m, own, 0, 1)
        for k in (*SIDES, FAR):
            self.send("y", i, self.send_y.at[lax.rem(here.y + k, Y), mm], self.got_y.at[slot, here.y, mm], here.along_y(k))

    def start_z(self, u, m=None):
        z, here, slot, (i, mm) = self.z, self.here, odd(u), self.which(u, m)
        wait(self.got_y.at[slot, pl.ds(0, Y - 1), mm], self.got["y"].at[i])
        wait(self.got_y.at[slot, pl.ds(0, Y - 1), mm], self.sent["y"].at[i])

        def work(_, k):
            total = self.kept_y[k]
            for place in range(1, Y):
                total += self.got_y[slot, lax.rem(here.y + place, Y), k].astype(f32)
            self.kept_z[k] = total
            self.send_z[k] = total.astype(bf16)

        self.over(m, work, 0, 1)

        def send(k):
            to = lax.rem(here.z + k, z.Z)
            pl.when(to < z.active)(lambda: self.send("z", i, self.send_z.at[mm, at(to * 16, 16), :], self.got_z.at[u, here.z, mm], here.along_z(k)))

        loop(1, z.Z, send)

    def if_active(self, yes, no):
        pl.when(self.here.z < self.z.active)(yes)
        pl.when(self.here.z >= self.z.active)(no)

    def wait_pieces(self, i, mm, n, sem):
        if n:
            wait(self.got_z.at[0, pl.ds(0, n), mm], sem.at[i])

    def mine(self, mm):
        return self.here.y, mm, at(self.here.z * 16, 16)

    def add_pieces(self, u, m):
        z, here, (i, mm) = self.z, self.here, self.which(u, m)
        self.wait_pieces(i, mm, z.active - 1, self.sent["z"])
        self.wait_pieces(i, mm, z.Z - 1, self.got["z"])
        y, mm, rows = self.mine(mm)
        total = self.kept_z[mm, rows, :]
        for k in range(1, z.Z):
            total += self.got_z[u, lax.rem(here.z + k, z.Z), mm].astype(f32)
        self.fin[u, y, mm, rows, :] = total.astype(bf16)

    def send_pieces(self, u, m=None):
        i, mm = self.which(u, m)
        y, mm, rows = self.mine(mm)
        piece = self.fin.at[u, y, mm, rows, :]
        loop(1, self.z.Z, lambda k: self.send("az", i, piece, piece, self.here.along_z(k)))

    def start_az(self, u, m=None):
        i, mm = self.which(u, m)

        def yes():
            self.add_pieces(u, m)
            self.send_pieces(u, m)

        self.if_active(yes, lambda: self.wait_pieces(i, mm, self.z.active, self.sent["z"]))

    def hand_on(self, u, out):
        def yes():
            self.add_pieces(u, None)
            y, mm, rows = self.mine(ALL)
            copy = pltpu.make_async_copy(self.fin.at[u, y, mm, rows, :], out, self.piece_sem)
            copy.start()
            copy.wait()

        self.if_active(yes, lambda: self.wait_pieces(u, ALL, self.z.active, self.sent["z"]))

    def take_over(self, u, piece):
        def yes():
            y, mm, rows = self.mine(ALL)
            copy = pltpu.make_async_copy(piece, self.fin.at[u, y, mm, rows, :], self.piece_sem)
            copy.start()
            copy.wait()
            self.send_pieces(u)

        pl.when(self.here.z < self.z.active)(yes)

    def start_ay(self, u, m=None):
        z, here, (i, mm) = self.z, self.here, self.which(u, m)
        self.if_active(lambda: self.wait_pieces(i, mm, z.active - 1, self.got["az"]), lambda: self.wait_pieces(i, mm, z.active, self.got["az"]))
        share = self.fin.at[u, here.y, mm]
        for k in (*SIDES, FAR):
            self.send("ay", i, share, share, here.along_y(k))

    def place(self, u):
        nb = self.z.NB
        return (1, u) if self.base == 0 else (1 - lax.div(u + nb - self.base, nb), lax.rem(u + nb - self.base, nb))

    def start_f(self, u, m=None):
        z, c, (i, mm) = self.z, self.here.c, self.which(u, m)
        layer, j = self.place(u)
        wait(self.fin.at[u, pl.ds(0, Y - 1), mm], self.got["ay"].at[i])
        for k in range(2) if m is None else (m,):
            if k == 2:
                break
            for y in range(Y):
                out = self.outs[k].at[layer, :, at((y * z.NB + j) * LANES, LANES, LANES)]
                pltpu.make_async_copy(self.fin.at[u, y, k], out, self.out_sem.at[k, u]).start()
        if m in (None, 2):
            self.down[u, c] = self.fin[u, :, 2]
            self.send("f", u, self.fin.at[u, :, 2], self.down.at[u, c], self.here.partner())

    def finish(self, u):
        z, c = self.z, self.here.c
        layer, j = self.place(u)
        wait(self.down.at[u, 0], self.got["f"].at[u])
        slot = odd(u)
        pl.when(u > 1)(lambda: self.turned_out(u - 2, "wait"))
        self.turned[slot] = self.down[u].reshape(z.D, LANES).T
        self.turned_out(u, "start")

    def turned_out(self, u, what):
        z, c = self.z, self.here.c
        layer, j = self.place(u)
        for half in range(2):
            row = 2 * j + half

            @pl.when(lax.div(row, z.NB) == c)
            def _(half=half, row=row):
                out = self.outs[2].at[layer, at(lax.rem(row, z.NB) * 64, 64), :]
                getattr(pltpu.make_async_copy(self.turned.at[odd(u), pl.ds(half * 64, 64), :], out, self.turned_sem.at[odd(u), half]), what)()

    def end(self, units, in_parts):
        z = self.z

        def sent_back(i, mm):
            self.if_active(lambda: self.wait_pieces(i, mm, z.Z - 1, self.sent["az"]), lambda: None)
            wait(self.fin.at[0, pl.ds(0, Y - 1), mm], self.sent["ay"].at[i])

        def one(u):
            wait(self.down.at[0, 0], self.sent["f"].at[u])
            for m in range(2):
                wait(self.down.at[0, 0], self.out_sem.at[m, u])

        loop(0, units, one)
        loop(0, units - in_parts, lambda u: sent_back(u, ALL))
        for m in range(len(self.outs) if in_parts else 0):
            sent_back(self.units + m, m)
        for u in range(max(0, units - 2), units):
            self.turned_out(u, "wait")


def backward_kernel(z, first, *refs):
    T, TC, T3, NB, FB, D = z.T, z.TC, z.T3, z.NB, z.FB, z.D
    here = Here(z)
    refs = list(refs)

    def take(n):
        out, refs[:] = refs[:n], refs[n:]
        return out

    h_in, dh_in, dh_t_in, w0, w1, w2 = take(6)
    if first:
        early_in = take(3)
    else:
        left_in, piece_in, by_up_in, by_gate_in, act_in, a_t_in = take(6)
        take(3)
    dx_out, *outs = take(4)
    spill = take(1)[0]
    if first:
        left_out, piece_out, dx_t_out = take(3)
    dx_buf, h_buf, a_t, dh, dh_t, wg, wu, wd, work = take(9)
    ld_sem, dh_sem, w_sem, sp_sem, s3_sem, o_sem, left_sem, turned_sem = take(8)
    if first:
        a, dx_t_buf, dx_t_sem = take(3)
    else:
        saved, saved_sem, act_sem = take(3)
    if first:
        fetch = Fetch(z, here, (w0.at[1], w1.at[1], w2.at[1]), (wg, wu, wd), take(len(Fetch.scratch(z))), z.early, NB)
        w0, w1, w2 = early_in
    base = 0 if first else 2
    units = NB - 1 if first else NB + base
    reduce = Reduce(z, here, units, base, outs, refs)
    met = meet(reduce.peers())
    whole = pltpu.make_async_copy(dh_in, dh, dh_sem)
    whole.start()

    def load_h(i):
        return pltpu.make_async_copy(h_in.at[at(i * T3, T3), :], h_buf.at[odd(i)], ld_sem.at[odd(i)])

    turn = [pltpu.make_async_copy(dh_t_in, dh_t, turned_sem.at[0])]
    if first:
        load_h(0).start()
    else:
        turn.append(pltpu.make_async_copy(a_t_in, a_t, turned_sem.at[1]))

    def loads(j):
        return [pltpu.make_async_copy(src.at[j], dst.at[j], w_sem.at[k, j]) for k, (src, dst) in enumerate(((w0, wg), (w1, wu), (w2, wd)))]

    TS, slots = z.TS, z.slots

    def load_saved(q):
        j, rows, slot = lax.div(q, T // TS), at(lax.rem(q, T // TS) * TS, TS), lax.rem(q, slots)
        return [pltpu.make_async_copy(v.at[j, rows, :], saved.at[slot, k], saved_sem.at[k, slot]) for k, v in enumerate((by_up_in, by_gate_in))]

    def load_act(j):
        return pltpu.make_async_copy(act_in.at[j], work.at[pl.ds(0, T), :], act_sem)

    if first:
        start(loads(0))
        fetch.begin_local()
        met()
        fetch.begin_pair()
        fetch.start_a1(z.early)
    else:
        left = pltpu.make_async_copy(left_in, reduce.stage.at[1], left_sem)
        left.start()
        start(loads(0)[2:])
        for q in range(slots - 1):
            start(load_saved(q))
        load_act(0).start()
        start(turn)
        for j in range(1, NB):
            start(loads(j)[2:])
    n3 = T // T3

    def prepare(i):
        rows = at(i * T3, T3, LANES)
        pl.when(i + 1 < n3)(lambda: load_h(i + 1).start())
        load_h(i).wait()
        value = normed(h_buf[odd(i)].astype(f32))[0]
        a[rows, :] = value
        a_t[:, rows] = value.T

    if not first:
        met()
        left.wait()
        reduce.start_p(1)
        reduce.take_over(0, piece_in)
    def turned():
        for copy in turn:
            copy.wait()

    if first:
        loop(0, n3, prepare)
        for j in range(1, z.early):
            start(loads(j))
        start(turn)
        fetch.end_pair()
        fetch.start_a2(z.early)

    def product(k, rows, cols):
        return work.at[at(k * T + rows.start, rows.size), cols]

    def spills(j):
        return [pltpu.make_async_copy(work.at[pl.ds((1 + k) * T, T), :], spill.at[k, j], sp_sem.at[k]) for k in range(2)]

    def spilled(j):
        for copy in spills(j):
            copy.wait()

    def step(name, u, m=None):
        do = getattr(reduce, "start_" + name)
        back = name in ("ay", "az")
        begin = 0 if first or name == "ay" else 1
        end = units - 1 if first and back else units
        if isinstance(u, int):
            if begin <= u < end:
                do(u, m)
        else:
            pl.when(jnp.logical_and(u >= begin, u < end))(lambda: do(u))

    def halfway(i, n, before, after):
        if n == 1:
            before()
            after()
        else:
            pl.when(i == 0)(before)
            pl.when(i == n // 2)(after)

    whole.wait()

    def loaded(j):
        for copy in loads(j):
            copy.wait()

    def block(j):
        u = j + base - 1
        if first:
            fetch.serve_a(j)
            pl.when(j < z.early)(lambda: loaded(j))
            pl.when(j >= z.early)(lambda: fetch.ready(j))
        else:
            pl.when(j > 0)(lambda: load_act(j).start())
            loads(j)[2].wait()
        pl.when(j > 0)(lambda: spilled(j - 1))

        def at_0():
            step("x2", u - 1)

        def at_1():
            step("z", u - 2)
            step("ay", u - 3)

        def at_2():
            if first:
                fetch.serve_b(j)
            pl.when(j == 0)(turned)
            step("x1", u)

        def at_3():
            if first:
                step("early_p", j)
            else:
                pl.when(j + 1 < NB)(lambda: reduce.start_early_p(j + base))
            step("y", u - 1)
            step("az", u - 2)

        def piece(i):
            halfway(i, T // TS, at_0, at_1)
            q, rows = j * (T // TS) + i, at(i * TS, TS)
            pl.when(q + slots - 1 < NB * (T // TS))(lambda: start(load_saved(q + slots - 1)))
            for copy in load_saved(q):
                copy.wait()
            by_act = dot(dh[rows, :], wd[j], ((1,), (1,))).astype(bf16).astype(f32)
            slot = lax.rem(q, slots)
            product(1, rows, ALL)[...] = (by_act * saved[slot, 1]).astype(bf16)
            product(2, rows, ALL)[...] = (by_act * saved[slot, 0]).astype(bf16)

        def chunk(i):
            halfway(i, T // TC, at_0, at_1)
            rows = at(i * TC, TC)
            for cols in z.halves:
                gate, up = dot(a[rows, :], wg[j, :, cols]), dot(a[rows, :], wu[j, :, cols])
                by_act = dot(dh[rows, :], wd[j, cols, :], ((1,), (1,))).astype(bf16).astype(f32)
                sig = sigmoid(gate)
                silu = gate * sig
                product(0, rows, cols)[...] = (silu * up).astype(bf16)
                product(1, rows, cols)[...] = (by_act * up * (sig + silu * (1.0 - sig))).astype(bf16)
                product(2, rows, cols)[...] = (by_act * silu).astype(bf16)

        if first:
            loop(0, T // TC, chunk)
        else:
            loop(0, T // TS, piece)
            load_act(j).wait()
            start(loads(j)[:2])
        start(spills(j))
        stage, slot, m = reduce.stage, odd(j + base), D // 2

        def rows_of(i):
            halfway(i, 2, at_2, at_3)
            rows = at(i * m, m)
            gates = dot(a_t[rows, :], work[pl.ds(T, T), :]).astype(bf16)
            ups = dot(a_t[rows, :], work[pl.ds(2 * T, T), :]).astype(bf16)
            downs = dot(dh_t[rows, :], work[pl.ds(0, T), :]).astype(bf16)
            for y in range(Y):
                lanes = slice(y * LANES, (y + 1) * LANES)
                for x in range(X // 2):
                    for c in range(CORES):
                        part = slice((x * CORES + c) * z.h, (x * CORES + c + 1) * z.h)
                        stage[slot, i * (X // 2) + x, c, y, 0] = gates[part, lanes]
                        stage[slot, i * (X // 2) + x, c, y, 1] = ups[part, lanes]
                for x in range(X):
                    stage[slot, x, i, y, 2] = downs[y * z.h : (y + 1) * z.h, x * LANES : (x + 1) * LANES]

        loop(0, 2, rows_of)
        if first:
            step("late_p", j)
        else:
            pl.when(j + 1 < NB)(lambda: reduce.start_late_p(j + base))

            @pl.when(j + 1 == NB)
            def _():
                for m in range(3):
                    reduce.start_p(NB + base - 1, m)

    loop(0, NB, block)
    if first:
        left = pltpu.make_async_copy(reduce.stage.at[(NB - 1) % 2], left_out, left_sem)
        left.start()
    spilled(NB - 1)

    def load_3(i):
        slot, rows = odd(i), at(i * T3, T3)
        out = [load_h(i)]
        for k in range(2):
            for j in range(NB):
                out.append(pltpu.make_async_copy(spill.at[k, j, rows, :], work.at[at(((slot * 2 + k) * NB + j) * T3, T3), :], s3_sem.at[slot]))
        return out

    def store_3(i):
        return pltpu.make_async_copy(dx_buf.at[odd(i)], dx_out.at[at(i * T3, T3), :], o_sem.at[odd(i)])

    def store_turned(i):
        return pltpu.make_async_copy(dx_t_buf.at[odd(i)], dx_t_out.at[:, at(i * T3, T3, LANES)], dx_t_sem.at[odd(i)])

    start(load_3(0))
    u = NB + base - 1
    if first:
        todo = ("x2:1", "z:2,ay:3", "", "az:2,y:1", "", "ay:2,z:1", "", "")
    else:
        todo = (
            "x2:1,ay:3",
            "x1.0,x1.1,z:2",
            "x1.2",
            "x2.0,az:2,y:1,x2.1",
            "x2.2,ay:2",
            "z:1,y.0,y.1",
            "y.2,az:1,z.0,z.1",
            "z.2,ay:1,az.0",
            "az.1,az.2,ay.0,ay.1,ay.2",
        )

    def steps(text):
        for item in filter(None, text.split(",")):
            name, _, behind = item.partition(":")
            if behind:
                step(name, u - int(behind))
            else:
                name, _, m = item.partition(".")
                step(name, u, int(m))

    done = units - 2 if first else units - 4

    def rows_back(i):
        slot, rows = odd(i), at(i * T3, T3)
        pl.when(i + 1 < n3)(lambda: start(load_3(i + 1)))
        for when, text in enumerate(todo[:n3]):
            pl.when(i == when)(lambda text=text: steps(text))

        @pl.when(i == n3 - 2)
        def _():
            loop(0, done, reduce.start_f)

        @pl.when(i == n3 - 1)
        def _():
            loop(0, done, reduce.finish)

        if not first:

            @pl.when(i == 0)
            def _():
                for j in range(NB):
                    for copy in loads(j)[:2]:
                        copy.wait()

        load_h(i).wait()
        wait(work.at[at(slot * 2 * NB * T3, 2 * NB * T3), :], s3_sem.at[slot])
        pl.when(i > 1)(lambda: store_3(i - 2).wait())
        if first:
            pl.when(i > 2)(lambda: store_turned(i - 3).wait())
            dx_t_buf[1 - slot] = dx_buf[1 - slot].T
        back = []
        for k, w in ((0, wg), (1, wu)):
            total = None
            for j in range(NB):
                part = dot(work[at(((slot * 2 + k) * NB + j) * T3, T3), :], w[j], ((1,), (1,)))
                total = part if total is None else total + part
            back.append(total.astype(bf16))
        by_a = (back[0] + back[1]).astype(f32)
        wide = h_buf[slot].astype(f32)
        square = jnp.mean(wide * wide, -1, keepdims=True) + 1e-6
        scale = lax.rsqrt(square)
        by_scale = jnp.sum(by_a * wide, -1, keepdims=True)
        by_square = by_scale * (-0.5 * scale / square) * (2.0 / D)
        dx_buf[slot] = dh[rows, :] + (by_a * scale + by_square * wide).astype(bf16)
        store_3(i).start()
        if first:
            pl.when(i > 0)(lambda: store_turned(i - 1).start())

    loop(0, n3, rows_back)
    if first:
        store_turned(n3 - 3).wait()
        dx_t_buf[odd(n3 - 1)] = dx_buf[odd(n3 - 1)].T
        store_turned(n3 - 1).start()
    assert n3 == 8
    for text in todo[n3:]:
        steps(text)
    if first:
        reduce.hand_on(units - 1, piece_out)
    back = units - 1 if first else units
    for v in range(done, back):
        if first or v + 1 < back:
            reduce.start_f(v)
        else:
            for m in range(3):
                reduce.start_f(v, m)
    for v in range(done, back):
        reduce.finish(v)
    reduce.end(back, 0 if first else 1)
    if first:
        fetch.end()
        left.wait()
    for i in range(max(0, n3 - 2), n3):
        store_3(i).wait()
        if first:
            store_turned(i).wait()


def call(body, out, n_in, scratch, number, aliases=()):
    return pl.pallas_call(
        body,
        out_shape=out,
        in_specs=[pl.BlockSpec(memory_space=HBM)] * n_in,
        out_specs=[pl.BlockSpec(memory_space=HBM)] * len(out),
        scratch_shapes=scratch,
        input_output_aliases=dict(aliases),
        compiler_params=pltpu.CompilerParams(
            collective_id=number,
            has_side_effects=True,
            vmem_limit_bytes=66_900_000,
        ),
    )


def forward(z, x, dy, shards):
    S = jax.ShapeDtypeStruct
    wide, tall, tokens, hidden, piece = (z.NB, z.D, z.FB), (z.NB, z.FB, z.D), (z.T, z.D), (z.NB, z.T, z.FB), (2, z.TC, z.FB)
    scratch = [VMEM(tokens, bf16), VMEM(tokens, f32), VMEM(tokens, bf16), VMEM((2, z.T3, z.D), bf16), VMEM(tokens[::-1], bf16), VMEM(tokens[::-1], bf16)]
    scratch += [VMEM(piece, bf16), VMEM(piece, f32), VMEM(piece, f32)]
    early = [(z.early, *shape[1:]) for shape in (wide, wide, tall)]
    scratch += [VMEM(shape, bf16) for shape in (wide, wide, tall, *early)]
    scratch += [DMA, DMA((3,)), DMA((3,)), DMA, DMA((3, 2)), DMA((2,)), DMA((2,))] + Fetch.scratch(z) + Fetch.scratch(z)
    out = [S(tokens, bf16), S(wide, bf16), S(wide, bf16), S(tall, bf16), S(hidden, bf16), S(hidden, f32), S(hidden, f32)]
    out += [S(shape, bf16) for shape in (*early, tokens[::-1], tokens[::-1])]
    h, *out = call(functools.partial(forward_kernel, z), out, 5, scratch, 0)(x, dy, *shards)
    return h, out[:3], out[3:6], out[6:9], out[9:]


def backward(z, h, dh, dh_t, w, more, first):
    S = jax.ShapeDtypeStruct
    wide, tall, tokens = (z.NB, z.D, z.FB), (z.NB, z.FB, z.D), (z.T, z.D)
    units = z.NB - 1 if first else z.NB + 2
    scratch = [VMEM((2, z.T3, z.D), bf16), VMEM((2, z.T3, z.D), bf16)]
    scratch += [VMEM(tokens[::-1], bf16), VMEM(tokens, bf16), VMEM(tokens[::-1], bf16)]
    scratch += [VMEM(wide, bf16), VMEM(wide, bf16), VMEM(tall, bf16), VMEM((max(3 * z.T, 4 * z.NB * z.T3), z.FB), bf16)]
    scratch += [DMA((2,)), DMA, DMA((3, z.NB)), DMA((2,)), DMA((2,)), DMA((2,)), DMA, DMA((2,))]
    if first:
        scratch += [VMEM(tokens, bf16), VMEM((2, z.D, z.T3), bf16), DMA((2,))] + Fetch.scratch(z)
    else:
        scratch += [VMEM((z.slots, 2, z.TS, z.FB), f32), DMA((2, z.slots)), DMA]
    scratch += Reduce.scratch(z, units)
    grads = [S((2, z.h, z.F), bf16), S((2, z.h, z.F), bf16), S((2, z.F // (X * CORES), z.D), bf16)]
    out = [S(tokens, bf16), *grads, S((2, z.NB, z.T, z.FB), bf16)]
    if first:
        out += [S((X, CORES, *z.unit), bf16), S((3, 16, LANES), bf16), S(tokens[::-1], bf16)]
    args = (h, dh, dh_t, *w, *more)
    aliases = {} if first else {len(args) - 3 + i: 1 + i for i in range(3)}
    dx, g, u, d, _, *left = call(functools.partial(backward_kernel, z, first), out, len(args), scratch, 1 if first else 2, aliases)(*args)
    return dx, (g, u, d), left


def solution(mesh):
    def step(x, dy, *weights):
        z = Sizes(mesh, x.shape[1], x.shape[2], weights[0].shape[2])
        h, w, (act, by_up, by_gate), early, (a_t, dy_t) = forward(z, x[0], dy[0], weights)
        dh, grads, (left, piece, dh_t) = backward(z, h, dy[0], dy_t, weights, early, True)
        dx, grads, _ = backward(z, x[0], dh, dh_t, w, (left, piece, by_up, by_gate, act, a_t, *grads), False)
        return dx[None], *grads

    states, cut = P(("rep", "r", "s"), None, None), P(None, "s", None)
    return jax.shard_map(
        step,
        mesh=mesh,
        in_specs=(states, states) + (cut,) * 3,
        out_specs=(states,) + (P("rep", "s", None),) * 3,
        check_vma=False,
    )
```
